32 devices in a mesh: slab: 8 (over z, x), yz: 4 (over y, core).
Axes of the slice: x: 2, y: 2, z: 4, core: 2. Of those that a mesh axis runs over, the one named last changes fastest.
Arguments:
- embeddings: bfloat16 [512, 25, 128], P(('slab', 'yz')), may hold values from -6 to 6
- neighbours: int32 [16384], P(('slab', 'yz')), may hold values from 0 to 127
- valid: int32 [16384], P(('slab', 'yz')), may hold values 0 or 1
- azimuth: float32 [16384], P(('slab', 'yz')), may hold values from -3.140625 to 3.140625
- polar: float32 [16384], P(('slab', 'yz')), may hold values from 0 to 3.14159
- distance: float32 [16384], P(('slab', 'yz')), may hold values from 0.9 to 5
- send_low: int32 [256], P(('slab', 'yz')), may hold values from 0 to 15
- send_high: int32 [256], P(('slab', 'yz')), may hold values from 0 to 15
- w_zero: bfloat16 [2, 640, 640], replicated, may hold values from -0.25 to 0.25
- w_one_re: bfloat16 [2, 512, 512], replicated, may hold values from -0.25 to 0.25
- w_one_im: bfloat16 [2, 512, 512], replicated, may hold values from -0.25 to 0.25
- w_two_re: bfloat16 [2, 384, 384], replicated, may hold values from -0.3125 to 0.3125
- w_two_im: bfloat16 [2, 384, 384], replicated, may hold values from -0.3125 to 0.3125
- radial_weight: float32 [2, 8, 128], replicated, may hold values from -2 to 2
- readout: float32 [128], replicated, may hold values from -0.5 to 0.5
Outputs:
- updated: bfloat16 [512, 25, 128], P(('slab', 'yz'))
- forces: float32 [3, 512], P(None, ('slab', 'yz'))
The draws below stay inside these ranges and needn't reach their ends.
All inputs are finite; a program needn't handle non-finite values. No bound on the sum of `valid` on one device may be relied on, other than what follows from the above.
Results may differ from the reference program's by a relative error of at most 0.0043.
Values may be sent and summed in bfloat16 or wider, within the bound.
No kernel may reach another device: no remote copies, remote signals or barrier semaphores. Data moves between devices by JAX's collectives and lax.ppermute only.
A program may use at most 64 MiB of HBM per device.

```python
import math
import jax
import jax.numpy as jnp
from jax import lax

CHANNELS = 128
COEFFS = 25
NEIGHB = 32
LAYERS = 2
ATOM_DEV = 16
GHOSTS = 8
ATOMS = 512
EDGES = 16384
GHOST_ALL = 256
N_SLAB = 8
N_YZ = 4


def with_ends(entries, stream_key, smallest, high):
    spot = [jax.random.randint(jax.random.fold_in(stream_key, axis), (), 0, length) for axis, length in enumerate(entries.shape)]
    widest = entries.shape.index(max(entries.shape))
    neighbour = spot[:widest] + [(spot[widest] + 1) % entries.shape[widest]] + spot[widest + 1:]
    return entries.at[tuple(spot)].set(smallest).at[tuple(neighbour)].set(high)


def block_scale(rng, shape, pieces, smallest, largest):
    level, own = 1.0, jax.random.fold_in(rng, 6)
    for axis_at, parts in pieces:
        heights = jnp.exp(jax.random.uniform(jax.random.fold_in(own, axis_at), (parts,), jnp.float32, smallest / len(pieces), largest / len(pieces)))
        level = level * jnp.repeat(heights, shape[axis_at] // parts).reshape([-1 if axis == axis_at else 1 for axis in range(len(shape))])
    return level


def noise(key, dims, scale, limit, cuts=(), kind=jnp.bfloat16):
    factor_of = block_scale(key, dims, cuts, -0.22, 0.18) if cuts else 1.0
    entries = jax.random.normal(key, dims, jnp.float32) * scale * factor_of
    return jnp.minimum(jnp.maximum(entries, -limit), limit).astype(kind)


def setup_inputs(seed: int = 0) -> dict:
    keys = jax.random.split(jax.random.key(seed), 16)
    return {
        "embeddings": noise(keys[0], (ATOMS, COEFFS, CHANNELS), 1.0, 6.0, ((0, 32),)),
        "neighbours": with_ends(jax.random.randint(keys[1], (EDGES,), 0, N_YZ * (ATOM_DEV + 2 * GHOSTS)), jax.random.fold_in(keys[1], 1), 0, (N_YZ * (ATOM_DEV + 2 * GHOSTS)) - 1).astype(jnp.int32),
        "valid": with_ends((jax.random.randint(keys[2], (EDGES,), 0, 8) < 7).astype(jnp.int32), jax.random.fold_in(keys[2], 1), 0, 1),
        "azimuth": jnp.clip(jax.random.uniform(keys[3], (EDGES,), jnp.float32, -3.140625, 3.140625), -3.140625, 3.140625),
        "polar": jnp.clip(3.14159 * jax.random.uniform(keys[4], (EDGES,), jnp.float32) ** block_scale(keys[4], (EDGES,), ((0, 32),), -0.2, 0.2), 0.0, 3.14159),
        "distance": jnp.clip(0.9 + 4.1 * jax.random.uniform(keys[5], (EDGES,), jnp.float32) ** block_scale(keys[5], (EDGES,), ((0, 32),), -0.2, 0.2), 0.9, 5.0),
        "send_low": with_ends(jax.random.randint(keys[6], (GHOST_ALL,), 0, ATOM_DEV), jax.random.fold_in(keys[6], 1), 0, ATOM_DEV - 1).astype(jnp.int32),
        "send_high": with_ends(jax.random.randint(keys[7], (GHOST_ALL,), 0, ATOM_DEV), jax.random.fold_in(keys[7], 1), 0, ATOM_DEV - 1).astype(jnp.int32),
        "w_zero": noise(keys[8], (LAYERS, 5 * CHANNELS, 5 * CHANNELS), (5 * CHANNELS) ** -0.5, 0.25),
        "w_one_re": noise(keys[9], (LAYERS, 4 * CHANNELS, 4 * CHANNELS), (4 * CHANNELS) ** -0.5, 0.25),
        "w_one_im": noise(keys[10], (LAYERS, 4 * CHANNELS, 4 * CHANNELS), (4 * CHANNELS) ** -0.5, 0.25),
        "w_two_re": noise(keys[11], (LAYERS, 3 * CHANNELS, 3 * CHANNELS), (3 * CHANNELS) ** -0.5, 0.3125),
        "w_two_im": noise(keys[12], (LAYERS, 3 * CHANNELS, 3 * CHANNELS), (3 * CHANNELS) ** -0.5, 0.3125),
        "radial_weight": noise(keys[13], (LAYERS, 8, CHANNELS), 8 ** -0.5, 2.0, (), jnp.float32),
        "readout": noise(keys[14], (CHANNELS,), CHANNELS ** -0.5, 0.5, (), jnp.float32),
    }


HIGHEST = lax.Precision.HIGHEST

def slot_index(degree, azimuth_order):
    return degree * degree + degree + azimuth_order

def radial_scale(distance, radial_weight):
    centers = 1.0 + 0.5 * jnp.arange(8, dtype=jnp.float32)
    basis_values = jnp.exp(-jnp.square((distance[:, None] - centers[None, :]) / 0.5))
    return jax.nn.silu(jnp.dot(basis_values, radial_weight, precision=HIGHEST))

def stacked(values, slots):
    return jnp.stack([values[:, coeff_slot] for coeff_slot in slots], axis=1)

def convolve(features, azimuth, distance, valid, w_zero, w_one_re, w_one_im, w_two_re, w_two_im, radial_weight):
    values = features.astype(jnp.float32)
    edge_count = values.shape[0]
    channel_count = values.shape[2]
    degrees = math.isqrt(values.shape[1])
    radial_rows = (radial_scale(distance, radial_weight) * valid.astype(jnp.float32)[:, None])[:, None, :]
    results = [None] * values.shape[1]
    zero_slots = [slot_index(degree, 0) for degree in range(degrees)]
    zero_in = stacked(values, zero_slots).reshape(edge_count, -1).astype(jnp.bfloat16)
    zero_out = jnp.dot(zero_in, w_zero, preferred_element_type=jnp.float32).reshape(edge_count, degrees, channel_count) * radial_rows
    for position, coeff_slot in enumerate(zero_slots):
        results[coeff_slot] = zero_out[:, position]
    for azimuth_order, real_part, imag_part in ((1, w_one_re, w_one_im), (2, w_two_re, w_two_im)):
        plus_slots = [slot_index(degree, azimuth_order) for degree in range(azimuth_order, degrees)]
        minus_slots = [slot_index(degree, -azimuth_order) for degree in range(azimuth_order, degrees)]
        plus_part = stacked(values, plus_slots)
        minus_part = stacked(values, minus_slots)
        cosine = jnp.cos(azimuth_order * azimuth)[:, None, None]
        sine = jnp.sin(azimuth_order * azimuth)[:, None, None]
        turned_plus = (cosine * plus_part + sine * minus_part).reshape(edge_count, -1).astype(jnp.bfloat16)
        turned_minus = (cosine * minus_part - sine * plus_part).reshape(edge_count, -1).astype(jnp.bfloat16)
        out_plus = (jnp.dot(turned_plus, real_part, preferred_element_type=jnp.float32) - jnp.dot(turned_minus, imag_part, preferred_element_type=jnp.float32)).reshape(edge_count, -1, channel_count) * radial_rows
        out_minus = (jnp.dot(turned_plus, imag_part, preferred_element_type=jnp.float32) + jnp.dot(turned_minus, real_part, preferred_element_type=jnp.float32)).reshape(edge_count, -1, channel_count) * radial_rows
        back_plus = cosine * out_plus - sine * out_minus
        back_minus = sine * out_plus + cosine * out_minus
        for position, coeff_slot in enumerate(plus_slots):
            results[coeff_slot] = back_plus[:, position]
        for position, coeff_slot in enumerate(minus_slots):
            results[coeff_slot] = back_minus[:, position]
    blank = jnp.zeros((edge_count, channel_count), jnp.float32)
    full = jnp.stack([blank if entry_value is None else entry_value for entry_value in results], axis=1)
    return (full, zero_out[:, 0])

def reference(embeddings, neighbours, valid, azimuth, polar, distance, send_low, send_high, w_zero, w_one_re, w_one_im, w_two_re, w_two_im, radial_weight, readout):
    slabs = N_SLAB
    devices = N_SLAB * N_YZ
    coeffs = embeddings.shape[1]
    channel_count = embeddings.shape[2]
    table_rows = N_YZ * (ATOM_DEV + 2 * GHOSTS)
    low_lists = send_low.reshape(devices, GHOSTS)
    high_lists = send_high.reshape(devices, GHOSTS)
    slab_neighbours = neighbours.reshape(slabs, -1)
    slab_azimuth = azimuth.reshape(slabs, -1)
    slab_polar = polar.reshape(slabs, -1)
    slab_distance = distance.reshape(slabs, -1)
    slab_valid = valid.reshape(slabs, -1)
    current = embeddings
    strength = None
    for layer_index in range(LAYERS):
        device_rows = current.reshape(devices, ATOM_DEV, coeffs, channel_count)
        low_rows = jax.vmap(lambda rows, picks: rows[picks])(device_rows, low_lists).reshape(slabs, N_YZ * GHOSTS, coeffs, channel_count)
        high_rows = jax.vmap(lambda rows, picks: rows[picks])(device_rows, high_lists).reshape(slabs, N_YZ * GHOSTS, coeffs, channel_count)
        own_rows = current.reshape(slabs, N_YZ * ATOM_DEV, coeffs, channel_count)
        tables = jnp.concatenate([own_rows, jnp.roll(high_rows, 1, axis=0), jnp.roll(low_rows, -1, axis=0)], axis=1)
        weights = (w_zero[layer_index], w_one_re[layer_index], w_one_im[layer_index], w_two_re[layer_index], w_two_im[layer_index], radial_weight[layer_index])

        def per_slab(items):
            table, picks, angle, length, usable = items
            message, scalar_out = convolve(table[picks], angle, length, usable, *weights)
            summed = message.reshape(-1, NEIGHB, coeffs, channel_count).sum(axis=1)
            return (summed, 0.125 * jnp.dot(scalar_out, readout, precision=HIGHEST))
        summed, strength = lax.map(per_slab, (tables, slab_neighbours, slab_azimuth, slab_distance, slab_valid))
        current = (current.astype(jnp.float32) + 0.18 * summed.reshape(-1, coeffs, channel_count)).astype(jnp.bfloat16)
    direction = jnp.stack([jnp.sin(slab_polar) * jnp.cos(slab_azimuth), jnp.sin(slab_polar) * jnp.sin(slab_azimuth), jnp.cos(slab_polar)], axis=0)
    pull = direction * strength[None]
    own_force = pull.reshape(3, -1, NEIGHB).sum(axis=-1)

    def table_pull(items):
        slab_pull, picks = items
        onehot = (picks[:, None] == jnp.arange(table_rows, dtype=jnp.int32)[None, :]).astype(jnp.float32)
        return -jnp.dot(slab_pull, onehot, precision=HIGHEST)
    table_force = lax.map(table_pull, (jnp.transpose(pull, (1, 0, 2)), slab_neighbours))
    own_rows_count = N_YZ * ATOM_DEV
    own_part = jnp.transpose(table_force[:, :, :own_rows_count], (1, 0, 2)).reshape(3, -1)
    below_part = jnp.roll(table_force[:, :, own_rows_count:own_rows_count + N_YZ * GHOSTS], -1, axis=0)
    above_part = jnp.roll(table_force[:, :, own_rows_count + N_YZ * GHOSTS:], 1, axis=0)
    below_dev = jnp.transpose(below_part.reshape(slabs, 3, N_YZ, GHOSTS), (0, 2, 1, 3)).reshape(devices, 3, GHOSTS)
    above_dev = jnp.transpose(above_part.reshape(slabs, 3, N_YZ, GHOSTS), (0, 2, 1, 3)).reshape(devices, 3, GHOSTS)
    atom_ids = jnp.arange(ATOM_DEV, dtype=jnp.int32)
    high_hot = (high_lists[:, :, None] == atom_ids[None, None, :]).astype(jnp.float32)
    low_hot = (low_lists[:, :, None] == atom_ids[None, None, :]).astype(jnp.float32)
    ghost_force = jnp.einsum('dcg,dga->dca', below_dev, high_hot, precision=HIGHEST) + jnp.einsum('dcg,dga->dca', above_dev, low_hot, precision=HIGHEST)
    forces = own_force + own_part + jnp.transpose(ghost_force, (1, 0, 2)).reshape(3, -1)
    return (current, forces)
```

```python
import functools
import math

import jax
import jax.numpy as jnp
from jax import lax
from jax.experimental import pallas as pl
from jax.experimental.pallas import tpu as pltpu
from jax.sharding import PartitionSpec as P

HIGHEST = lax.Precision.HIGHEST
BF16 = jnp.bfloat16
F32 = jnp.float32
ORDERS = (1, 2)
VMEM = pl.BlockSpec(memory_space=pltpu.VMEM)


def slot_index(degree, azimuth_order):
    return degree * degree + degree + azimuth_order


def slot_groups(degrees):
    groups = [[slot_index(degree, 0) for degree in range(degrees)]]
    for order in ORDERS:
        groups.append([slot_index(degree, order) for degree in range(order, degrees)])
        groups.append([slot_index(degree, -order) for degree in range(order, degrees)])
    return groups


def slot_order(degrees):
    return [slot for group in slot_groups(degrees) for slot in group]


def odd_slab():
    return lax.axis_index("slab") % 2 == 1


def dot(left, right, contract=((1,), (0,)), precision=None):
    return lax.dot_general(
        left, right, (contract, ((), ())), precision=precision, preferred_element_type=F32
    )


def lent_hot(low_ref, high_ref, atoms):
    odd = odd_slab()
    low, high = low_ref[...], high_ref[...]
    picks = jnp.concatenate([jnp.where(odd, low, high), jnp.where(odd, high, low)], axis=1)
    rows = lax.broadcasted_iota(jnp.int32, (atoms, picks.shape[1]), 0)
    return (rows == picks).astype(F32)


def lent_rows(hot, rows):
    return dot(hot.astype(BF16), rows, ((0,), (0,))).astype(BF16)


def pack_kernel(emb_ref, low_ref, high_ref, own_ref, pair_ref, other_ref, wide):
    atoms, coeffs, channels = emb_ref.shape
    ghosts = low_ref.shape[1]
    wide[...] = emb_ref[...].astype(F32)
    for place, slot in enumerate(slot_order(math.isqrt(coeffs))):
        own_ref[:, place * channels : (place + 1) * channels] = wide[:, slot, :].astype(BF16)
    lent = lent_rows(lent_hot(low_ref, high_ref, atoms), own_ref[...])
    pair_ref[...] = lent[:ghosts]
    other_ref[...] = lent[ghosts:]


def static_kernel(
    atoms, ghosts, slab_devices,
    nbr_ref, valid_ref, azi_ref, pol_ref, dist_ref, rw_ref,
    hot_ref, radial_ref, dirs_ref, pulls_ref,
):
    layers, centers = rw_ref.shape[0], rw_ref.shape[1]
    nbr = nbr_ref[...]
    edges = nbr.shape[1]
    own_count, ghost_count = slab_devices * atoms, slab_devices * ghosts
    block = atoms + 2 * ghosts
    me = lax.axis_index("yz")
    odd = odd_slab()
    is_own = nbr < own_count
    ghost = nbr - own_count
    below = ghost < ghost_count
    ghost = jnp.where(below, ghost, ghost - ghost_count)
    paired = jnp.where(odd, below.astype(jnp.int32), 1 - below.astype(jnp.int32))
    device = jnp.where(is_own, nbr // atoms, ghost // ghosts)
    inner = jnp.where(
        is_own, nbr % atoms, atoms + (1 - paired) * ghosts + ghost % ghosts
    )
    place = (device ^ me) * block + inner
    rows = lax.broadcasted_iota(jnp.int32, (slab_devices * block, edges), 0)
    hot = jnp.where((rows == place) & (valid_ref[...] != 0), 1.0, 0.0).astype(F32)
    hot_cols = jnp.transpose(hot).astype(BF16)
    hot_ref[...] = jnp.concatenate([hot_cols, hot_cols], axis=1)
    middle = 1.0 + 0.5 * lax.broadcasted_iota(jnp.int32, (centers, edges), 0).astype(F32)
    basis = jnp.exp(-jnp.square((dist_ref[...] - middle) / 0.5))
    for layer in range(layers):
        scale = dot(basis, rw_ref[layer], ((0,), (0,)), HIGHEST)
        radial = scale / (1.0 + jnp.exp(-scale))
        radial_ref[layer] = radial
    azimuth, polar = azi_ref[...], pol_ref[...]
    sin_polar = jnp.sin(polar)
    dirs = [sin_polar * jnp.cos(azimuth), sin_polar * jnp.sin(azimuth), jnp.cos(polar)]
    dirs_ref[...] = jnp.concatenate(dirs, axis=0)
    channels = rw_ref.shape[2]
    for axis, along in enumerate(dirs):
        pulls_ref[:, axis * channels : (axis + 1) * channels] = dot(
            hot * along, radial, precision=HIGHEST
        ).astype(BF16)


def layer_sums(layer, degrees, channels, tables, weights, hot_ref, radial_ref, scratch):
    joined, mixed = scratch
    groups = slot_groups(degrees)
    w_zero, w_one_re, w_one_im, w_two_re, w_two_im = (ref[layer] for ref in weights)
    width = joined.shape[1]
    start = 0
    for ref in tables:
        count = ref.shape[0]
        joined[start : start + count] = ref[:, :width].astype(F32)
        start += count
    rows = start

    def put(column, value):
        high = value.astype(BF16)
        low = (value - high.astype(F32)).astype(BF16)
        mixed[:rows, column : column + value.shape[1]] = high
        mixed[rows:, column : column + value.shape[1]] = low

    span = len(groups[0]) * channels
    zero = dot(joined[:, :span].astype(BF16), w_zero)
    put(0, zero)
    column = span
    for index, (real, imag) in enumerate(((w_one_re, w_one_im), (w_two_re, w_two_im))):
        span = len(groups[2 * index + 1]) * channels
        both = jnp.concatenate(
            [joined[:, column : column + span], joined[:, column + span : column + 2 * span]], axis=0
        ).astype(BF16)
        by_real = dot(both, real)
        by_imag = dot(both, imag)
        put(column, by_real[:rows] - by_imag[rows:])
        put(column + span, by_imag[:rows] + by_real[rows:])
        column += 2 * span
    radial = radial_ref[layer]
    edges = radial.shape[0]
    hot = hot_ref[...]
    atoms = tables[0].shape[0]
    sums = []
    first = None
    step = 2 * channels
    for begin in range(0, width, step):
        got = dot(hot, mixed[:, begin : min(begin + step, width)])
        for inner in range(0, got.shape[1], channels):
            message = got[:, inner : inner + channels] * radial
            if first is None:
                first = message
            sums.append(message.reshape(atoms, edges // atoms, channels).sum(axis=1))
    return sums, first, zero


def first_kernel(
    layer, last, degrees, channels, count,
    low_ref, high_ref, hot_ref, radial_ref, pulls_ref, *refs,
):
    tables, weights = refs[:count], refs[count : count + 5]
    own_ref, pair_ref, other_ref = refs[count + 5 : count + 8]
    scratch = refs[count + 8 :]
    sums, _, _ = layer_sums(
        layer, degrees, channels, tables, weights, hot_ref, radial_ref, scratch
    )
    atoms = tables[0].shape[0]
    ghosts = low_ref.shape[1]
    width = len(sums) * channels
    for place, total in enumerate(sums):
        cols = slice(place * channels, (place + 1) * channels)
        own_ref[:, cols] = (tables[0][:, cols].astype(F32) + 0.18 * total).astype(BF16)
    lent = lent_rows(lent_hot(low_ref, high_ref, atoms), own_ref[:, :width])
    pair_ref[:, :width] = lent[:ghosts]
    other_ref[:, :width] = lent[ghosts:]
    if last:
        block = atoms + 2 * ghosts
        part = pulls_ref.shape[1]
        for slot in range(pulls_ref.shape[0] // block):
            cols = slice(width + slot * part, width + (slot + 1) * part)
            at = slot * block
            own_ref[:, cols] = pulls_ref[at : at + atoms]
            pair_ref[:, cols] = pulls_ref[at + atoms : at + atoms + ghosts]
            other_ref[:, cols] = pulls_ref[at + atoms + ghosts : at + block]


def last_kernel(
    layer, degrees, channels, count,
    emb_ref, low_ref, high_ref, hot_ref, radial_ref, dirs_ref, readout_ref, *refs,
):
    tables, weights = refs[:count], refs[count : count + 5]
    out_ref, force_ref = refs[count + 5 : count + 7]
    joined, mixed, wide = refs[count + 7 :]
    sums, first, zero = layer_sums(
        layer, degrees, channels, tables, weights, hot_ref, radial_ref, (joined, mixed)
    )
    atoms = tables[0].shape[0]
    ghosts = low_ref.shape[1]
    wide[...] = emb_ref[...].astype(F32)
    for place, slot in enumerate(slot_order(degrees)):
        cols = slice(place * channels, (place + 1) * channels)
        wide[:, slot, :] = tables[0][:, cols].astype(F32) + 0.18 * sums[place]
    out_ref[...] = wide[...].astype(BF16)

    readout = 0.125 * readout_ref[...]
    strength = dot(readout, first, ((1,), (1,)), HIGHEST)
    pull = dirs_ref[...] * strength
    edges = pull.shape[1]
    edge = lax.broadcasted_iota(jnp.int32, (atoms, edges), 1)
    atom = lax.broadcasted_iota(jnp.int32, (atoms, edges), 0)
    owner = (edge // (edges // atoms) == atom).astype(F32)
    own_force = dot(pull, owner, ((1,), (1,)), HIGHEST)

    width = len(sums) * channels
    part = 3 * channels
    kinds = [0.0, 0.0, 0.0]
    for slot in range(count // 3):
        for kind in range(3):
            ref = tables[3 * slot + kind]
            kinds[kind] += ref[:, width + slot * part : width + (slot + 1) * part].astype(F32)
    lent = jnp.concatenate(kinds[1:], axis=0)
    pulls = kinds[0] + dot(lent_hot(low_ref, high_ref, atoms), lent, precision=HIGHEST)
    mine = zero[:atoms, :channels] * readout
    ones = jnp.ones((1, channels), F32)
    for axis in range(3):
        back = dot(
            ones, mine * pulls[:, axis * channels : (axis + 1) * channels], ((1,), (1,)), HIGHEST
        )
        force_ref[axis : axis + 1, :] = own_force[axis : axis + 1] - back


def exchange(own, pair, other, slabs, slab_devices):
    def toward(block, step):
        route = []
        for slab in range(slabs):
            to = slab + 1 if (slab % 2 == 0) == (step > 0) else slab - 1
            route.append((slab, to % slabs))
        return lax.ppermute(block, "slab", route)

    got_other = toward(other, -1)
    got_pair = toward(pair, 1)
    held = {0: (own, got_pair, got_other)}
    bit = slab_devices // 2
    while bit:
        route = [(q, q ^ bit) for q in range(slab_devices)]
        for slot in sorted(held):
            held[slot | bit] = tuple(lax.ppermute(block, "yz", route) for block in held[slot])
        bit //= 2
    return [block for slot in range(slab_devices) for block in held[slot]]


def body(
    embeddings, neighbours, valid, azimuth, polar, distance, send_low, send_high,
    w_zero, w_one_re, w_one_im, w_two_re, w_two_im, radial_weight, readout,
):
    atoms, coeffs, channels = embeddings.shape
    degrees = math.isqrt(coeffs)
    ghosts = send_low.shape[0]
    edges = neighbours.shape[0]
    layers = w_zero.shape[0]
    slabs, slab_devices = lax.axis_size("slab"), lax.axis_size("yz")
    rows = slab_devices * (atoms + 2 * ghosts)
    width = len(slot_order(degrees)) * channels
    low, high = send_low.reshape(1, -1), send_high.reshape(1, -1)
    shape = jax.ShapeDtypeStruct

    own, pair, other = pl.pallas_call(
        pack_kernel,
        out_shape=[
            shape((atoms, width), BF16), shape((ghosts, width), BF16), shape((ghosts, width), BF16)
        ],
        in_specs=[VMEM] * 3,
        out_specs=[VMEM] * 3,
        scratch_shapes=[pltpu.VMEM((atoms, coeffs, channels), F32)],
        name="pack",
    )(embeddings, low, high)

    row = lambda value: value.reshape(1, -1)
    hot, radial, dirs, pulls = pl.pallas_call(
        functools.partial(static_kernel, atoms, ghosts, slab_devices),
        out_shape=[
            shape((edges, 2 * rows), BF16), shape((layers, edges, channels), F32),
            shape((3, edges), F32), shape((rows, 3 * channels), BF16),
        ],
        in_specs=[VMEM] * 6,
        out_specs=[VMEM] * 4,
        name="geometry",
    )(row(neighbours), row(valid), row(azimuth), row(polar), row(distance), radial_weight)

    weights = (w_zero, w_one_re, w_one_im, w_two_re, w_two_im)
    scratch = [pltpu.VMEM((rows, width), F32), pltpu.VMEM((2 * rows, width), BF16)]
    for layer in range(layers):
        tables = exchange(own, pair, other, slabs, slab_devices)
        if layer < layers - 1:
            last = layer == layers - 2
            wide = width + (slab_devices * 3 * channels if last else 0)
            own, pair, other = pl.pallas_call(
                functools.partial(first_kernel, layer, last, degrees, channels, len(tables)),
                out_shape=[
                    shape((atoms, wide), BF16), shape((ghosts, wide), BF16),
                    shape((ghosts, wide), BF16),
                ],
                in_specs=[VMEM] * (5 + len(tables) + len(weights)),
                out_specs=[VMEM] * 3,
                scratch_shapes=scratch,
                name="layer",
            )(low, high, hot, radial, pulls, *tables, *weights)
        else:
            updated, forces = pl.pallas_call(
                functools.partial(last_kernel, layer, degrees, channels, len(tables)),
                out_shape=[shape((atoms, coeffs, channels), BF16), shape((3, atoms), F32)],
                in_specs=[VMEM] * (7 + len(tables) + len(weights)),
                out_specs=[VMEM] * 2,
                scratch_shapes=scratch + [pltpu.VMEM((atoms, coeffs, channels), F32)],
                name="last_layer",
            )(embeddings, low, high, hot, radial, dirs, readout.reshape(1, -1), *tables, *weights)
    return (updated, forces)


def solution(mesh):
    both = ("slab", "yz")
    in_specs = (P(both, None, None), *([P(both)] * 7), *([P()] * 7))
    out_specs = (P(both, None, None), P(None, both))
    return jax.shard_map(body, mesh=mesh, in_specs=in_specs, out_specs=out_specs, check_vma=False)
```

```python
import functools
import math

import jax
import jax.numpy as jnp
from jax import lax
from jax.experimental import pallas as pl
from jax.experimental.pallas import tpu as pltpu
from jax.sharding import PartitionSpec as P

HIGHEST = lax.Precision.HIGHEST
BF16 = jnp.bfloat16
F32 = jnp.float32
ORDERS = (1, 2)
VMEM = pl.BlockSpec(memory_space=pltpu.VMEM)


def near(*arrays):
    return [pltpu.with_memory_space_constraint(array, pltpu.VMEM) for array in arrays]


def away(*arrays):
    return [pltpu.with_memory_space_constraint(array, pltpu.HBM) for array in arrays]


def slot_index(degree, azimuth_order):
    return degree * degree + degree + azimuth_order


def slot_groups(degrees):
    groups = [[slot_index(degree, 0) for degree in range(degrees)]]
    for order in ORDERS:
        groups.append([slot_index(degree, order) for degree in range(order, degrees)])
        groups.append([slot_index(degree, -order) for degree in range(order, degrees)])
    return groups


def slot_order(degrees):
    return [slot for group in slot_groups(degrees) for slot in group]


def unused_slots(coeffs):
    order = slot_order(math.isqrt(coeffs))
    return [slot for slot in range(coeffs) if slot not in order]


def odd_slab():
    return lax.axis_index("slab") % 2 == 1


def dot(left, right, contract=((1,), (0,)), precision=None):
    return lax.dot_general(
        left, right, (contract, ((), ())), precision=precision, preferred_element_type=F32
    )


def lent_hot(low_ref, high_ref, atoms):
    odd = odd_slab()
    low, high = low_ref[...], high_ref[...]
    picks = jnp.concatenate([jnp.where(odd, low, high), jnp.where(odd, high, low)], axis=1)
    rows = lax.broadcasted_iota(jnp.int32, (atoms, picks.shape[1]), 0)
    return (rows == picks).astype(F32)


def lent_rows(hot, rows):
    return dot(hot.astype(BF16), rows, ((0,), (0,))).astype(BF16)


def pack_kernel(emb_ref, low_ref, high_ref, own_ref, pair_ref, other_ref, rest_ref, lent_ref):
    coeffs, atoms, channels = emb_ref.shape
    ghosts = low_ref.shape[1]
    order = slot_order(math.isqrt(coeffs))
    for place, slot in enumerate(order):
        own_ref[:, place * channels : (place + 1) * channels] = emb_ref[slot]
    for place, slot in enumerate(unused_slots(coeffs)):
        rest_ref[place] = emb_ref[slot]
    hot = lent_hot(low_ref, high_ref, atoms)
    lent_ref[...] = hot
    lent = lent_rows(hot, own_ref[...])
    pair_ref[...] = lent[:ghosts]
    other_ref[...] = lent[ghosts:]


def scale_kernel(
    atoms, ghosts, slab_devices,
    nbr_ref, valid_ref, dist_ref, rw_ref, readout_ref, *refs,
):
    count = (len(refs) - 5) // 2
    far, (hot_ref, radial_ref, flags_ref, vector_ref), held = refs[:count], refs[count : count + 4], refs[count + 4 : -1]
    sems = refs[-1]
    copies = [pltpu.make_async_copy(far[i], held[i], sems.at[i]) for i in range(count)]
    for copy in copies:
        copy.start()
    layers, centers = rw_ref.shape[0], rw_ref.shape[1]
    nbr = nbr_ref[...]
    edges = nbr.shape[1]
    own_count, ghost_count = slab_devices * atoms, slab_devices * ghosts
    block = atoms + 2 * ghosts
    me = lax.axis_index("yz")
    odd = odd_slab()
    is_own = nbr < own_count
    ghost = nbr - own_count
    below = ghost < ghost_count
    ghost = jnp.where(below, ghost, ghost - ghost_count)
    paired = jnp.where(odd, below.astype(jnp.int32), 1 - below.astype(jnp.int32))
    device = jnp.where(is_own, nbr // atoms, ghost // ghosts)
    inner = jnp.where(
        is_own, nbr % atoms, atoms + (1 - paired) * ghosts + ghost % ghosts
    )
    place = (device ^ me) * block + inner
    rows = lax.broadcasted_iota(jnp.int32, (slab_devices * block, edges), 0)
    hot = jnp.where((rows == place) & (valid_ref[...] != 0), 1.0, 0.0).astype(F32)
    flags_ref[...] = hot
    hot_cols = jnp.transpose(hot).astype(BF16)
    hot_ref[...] = jnp.concatenate([hot_cols, hot_cols], axis=1)
    middle = 1.0 + 0.5 * lax.broadcasted_iota(jnp.int32, (centers, edges), 0).astype(F32)
    basis = jnp.exp(-jnp.square((dist_ref[...] - middle) / 0.5))
    for layer in range(layers):
        scale = dot(basis, rw_ref[layer], ((0,), (0,)), HIGHEST)
        radial_ref[layer] = scale / (1.0 + jnp.exp(-scale))
    vector_ref[...] = 0.125 * readout_ref[...]
    for copy in copies:
        copy.wait()


def pull_kernel(azi_ref, pol_ref, radial_ref, flags_ref, dirs_ref, pulls_ref):
    azimuth, polar = azi_ref[...], pol_ref[...]
    sin_polar = jnp.sin(polar)
    dirs = [sin_polar * jnp.cos(azimuth), sin_polar * jnp.sin(azimuth), jnp.cos(polar)]
    dirs_ref[...] = jnp.concatenate(dirs, axis=0)
    radial = radial_ref[radial_ref.shape[0] - 1]
    channels = radial.shape[1]
    for axis, along in enumerate(dirs):
        pulls_ref[:, axis * channels : (axis + 1) * channels] = dot(
            flags_ref[...] * along, radial, precision=HIGHEST
        ).astype(BF16)


def layer_sums(layer, degrees, channels, tables, weights, hot_ref, radial_ref, scratch):
    joined, mixed = scratch
    groups = slot_groups(degrees)
    w_zero, w_one_re, w_one_im, w_two_re, w_two_im = (ref[layer] for ref in weights)
    width = joined.shape[1]
    start = 0
    for ref in tables:
        count = ref.shape[0]
        joined[start : start + count] = ref[:, :width].astype(F32)
        start += count
    rows = start

    def put(column, value):
        high = value.astype(BF16)
        low = (value - high.astype(F32)).astype(BF16)
        mixed[:rows, column : column + value.shape[1]] = high
        mixed[rows:, column : column + value.shape[1]] = low

    span = len(groups[0]) * channels
    zero = dot(joined[:, :span].astype(BF16), w_zero)
    put(0, zero)
    column = span
    for index, (real, imag) in enumerate(((w_one_re, w_one_im), (w_two_re, w_two_im))):
        span = len(groups[2 * index + 1]) * channels
        both = jnp.concatenate(
            [joined[:, column : column + span], joined[:, column + span : column + 2 * span]], axis=0
        ).astype(BF16)
        by_real = dot(both, real)
        by_imag = dot(both, imag)
        put(column, by_real[:rows] - by_imag[rows:])
        put(column + span, by_imag[:rows] + by_real[rows:])
        column += 2 * span
    radial = radial_ref[layer]
    edges = radial.shape[0]
    hot = hot_ref[...]
    atoms = tables[0].shape[0]
    sums = []
    first = None
    step = 2 * channels
    for begin in range(0, width, step):
        got = dot(hot, mixed[:, begin : min(begin + step, width)])
        for inner in range(0, got.shape[1], channels):
            message = got[:, inner : inner + channels] * radial
            if first is None:
                first = message
            sums.append(message.reshape(atoms, edges // atoms, channels).sum(axis=1))
    return sums, first, zero


def first_kernel(
    layer, last, degrees, channels, count,
    lent_ref, hot_ref, radial_ref, pulls_ref, *refs,
):
    tables, weights = refs[:count], refs[count : count + 5]
    own_ref, pair_ref, other_ref = refs[count + 5 : count + 8]
    scratch = refs[count + 8 :]
    sums, _, _ = layer_sums(
        layer, degrees, channels, tables, weights, hot_ref, radial_ref, scratch
    )
    atoms = tables[0].shape[0]
    ghosts = lent_ref.shape[1] // 2
    width = len(sums) * channels
    for place, total in enumerate(sums):
        cols = slice(place * channels, (place + 1) * channels)
        own_ref[:, cols] = (tables[0][:, cols].astype(F32) + 0.18 * total).astype(BF16)
    lent = lent_rows(lent_ref[...], own_ref[:, :width])
    pair_ref[:, :width] = lent[:ghosts]
    other_ref[:, :width] = lent[ghosts:]
    if last:
        block = atoms + 2 * ghosts
        part = pulls_ref.shape[1]
        for slot in range(pulls_ref.shape[0] // block):
            cols = slice(width + slot * part, width + (slot + 1) * part)
            at = slot * block
            own_ref[:, cols] = pulls_ref[at : at + atoms]
            pair_ref[:, cols] = pulls_ref[at + atoms : at + atoms + ghosts]
            other_ref[:, cols] = pulls_ref[at + atoms + ghosts : at + block]


def last_kernel(
    layer, degrees, channels, count,
    rest_ref, lent_ref, hot_ref, radial_ref, dirs_ref, readout_ref, *refs,
):
    tables, weights = refs[:count], refs[count : count + 5]
    out_ref, force_ref = refs[count + 5 : count + 7]
    scratch = refs[count + 7 :]
    sums, first, zero = layer_sums(
        layer, degrees, channels, tables, weights, hot_ref, radial_ref, scratch
    )
    atoms = tables[0].shape[0]
    order = slot_order(degrees)
    for place, slot in enumerate(order):
        cols = slice(place * channels, (place + 1) * channels)
        out_ref[slot] = (tables[0][:, cols].astype(F32) + 0.18 * sums[place]).astype(BF16)
    for place, slot in enumerate(unused_slots(degrees * degrees)):
        out_ref[slot] = rest_ref[place]

    readout = readout_ref[...]
    strength = dot(readout, first, ((1,), (1,)), HIGHEST)
    pull = dirs_ref[...] * strength
    edges = pull.shape[1]
    edge = lax.broadcasted_iota(jnp.int32, (atoms, edges), 1)
    atom = lax.broadcasted_iota(jnp.int32, (atoms, edges), 0)
    owner = (edge // (edges // atoms) == atom).astype(F32)
    own_force = dot(pull, owner, ((1,), (1,)), HIGHEST)

    width = len(sums) * channels
    part = 3 * channels
    kinds = [0.0, 0.0, 0.0]
    for slot in range(count // 3):
        for kind in range(3):
            ref = tables[3 * slot + kind]
            kinds[kind] += ref[:, width + slot * part : width + (slot + 1) * part].astype(F32)
    lent = jnp.concatenate(kinds[1:], axis=0)
    pulls = kinds[0] + dot(lent_ref[...], lent, precision=HIGHEST)
    mine = zero[:atoms, :channels] * readout
    ones = jnp.ones((1, channels), F32)
    for axis in range(3):
        back = dot(
            ones, mine * pulls[:, axis * channels : (axis + 1) * channels], ((1,), (1,)), HIGHEST
        )
        force_ref[axis : axis + 1, :] = own_force[axis : axis + 1] - back


def exchange(own, pair, other, slabs, slab_devices, between=()):
    def toward(block, step):
        route = []
        for slab in range(slabs):
            to = slab + 1 if (slab % 2 == 0) == (step > 0) else slab - 1
            route.append((slab, to % slabs))
        return lax.ppermute(block, "slab", route)

    got_other = toward(other, -1)
    got_pair = toward(pair, 1)
    if between:
        got_pair, *between = lax.optimization_barrier((got_pair, *between))
    held = {0: (own, got_pair, got_other)}
    bit = slab_devices // 2
    while bit:
        route = [(q, q ^ bit) for q in range(slab_devices)]
        for slot in sorted(held):
            held[slot | bit] = tuple(lax.ppermute(block, "yz", route) for block in held[slot])
        bit //= 2
    return [block for slot in range(slab_devices) for block in held[slot]], between


def body(
    embeddings, neighbours, valid, azimuth, polar, distance, send_low, send_high,
    w_zero, w_one_re, w_one_im, w_two_re, w_two_im, radial_weight, readout,
):
    atoms, coeffs, channels = embeddings.shape
    degrees = math.isqrt(coeffs)
    ghosts = send_low.shape[0]
    edges = neighbours.shape[0]
    layers = w_zero.shape[0]
    slabs, slab_devices = lax.axis_size("slab"), lax.axis_size("yz")
    rows = slab_devices * (atoms + 2 * ghosts)
    width = len(slot_order(degrees)) * channels
    low, high = send_low.reshape(1, -1), send_high.reshape(1, -1)
    held, shape = pltpu.VMEM, jax.ShapeDtypeStruct
    embeddings = embeddings.transpose(1, 0, 2)
    params = pltpu.CompilerParams(vmem_limit_bytes=20 * 2**20)
    row = lambda value: value.reshape(1, -1)
    far = pl.BlockSpec(memory_space=pl.ANY)

    own, pair, other, rest, lent = pl.pallas_call(
        pack_kernel,
        out_shape=[
            held((atoms, width), BF16), held((ghosts, width), BF16), held((ghosts, width), BF16),
            held((len(unused_slots(coeffs)), atoms, channels), BF16), held((atoms, 2 * ghosts), F32),
        ],
        in_specs=[VMEM] * 3,
        out_specs=[VMEM] * 5,
        compiler_params=params,
        name="pack",
    )(*away(embeddings, low, high))

    weights = (w_zero, w_one_re, w_one_im, w_two_re, w_two_im)
    hot, radial, flags, vector, *weights = pl.pallas_call(
        functools.partial(scale_kernel, atoms, ghosts, slab_devices),
        out_shape=[
            held((edges, 2 * rows), BF16), held((layers, edges, channels), F32),
            held((rows, edges), F32), held((1, channels), F32),
            *(held(array.shape, array.dtype) for array in weights),
        ],
        in_specs=[VMEM] * 5 + [far] * len(weights),
        out_specs=[VMEM] * (4 + len(weights)),
        scratch_shapes=[pltpu.SemaphoreType.DMA((len(weights),))],
        compiler_params=params,
        name="scales",
    )(*away(*map(row, (neighbours, valid, distance)), radial_weight, row(readout), *weights))
    dirs, pulls = pl.pallas_call(
        pull_kernel,
        out_shape=[held((3, edges), F32), held((rows, 3 * channels), BF16)],
        in_specs=[VMEM] * 4,
        out_specs=[VMEM] * 2,
        compiler_params=params,
        name="pulls",
    )(*away(row(azimuth), row(polar)), *near(radial, flags))

    scratch = [pltpu.VMEM((rows, width), F32), pltpu.VMEM((2 * rows, width), BF16)]
    between = (hot, radial)
    for layer in range(layers):
        tables, between = exchange(own, pair, other, slabs, slab_devices, between)
        if layer == 0:
            hot, radial = between
            between = ()
        if layer < layers - 1:
            last = layer == layers - 2
            wide = width + (slab_devices * 3 * channels if last else 0)
            own, pair, other = pl.pallas_call(
                functools.partial(first_kernel, layer, last, degrees, channels, len(tables)),
                out_shape=[
                    held((atoms, wide), BF16), held((ghosts, wide), BF16), held((ghosts, wide), BF16)
                ],
                in_specs=[VMEM] * (4 + len(tables) + len(weights)),
                out_specs=[VMEM] * 3,
                scratch_shapes=scratch,
                compiler_params=params,
                name="layer",
            )(*near(lent, hot, radial, pulls, *tables, *weights))
        else:
            updated, forces = pl.pallas_call(
                functools.partial(last_kernel, layer, degrees, channels, len(tables)),
                out_shape=[shape((coeffs, atoms, channels), BF16), shape((3, atoms), F32)],
                in_specs=[VMEM] * (6 + len(tables) + len(weights)),
                out_specs=[VMEM] * 2,
                scratch_shapes=scratch,
                compiler_params=params,
                name="last_layer",
            )(*near(rest, lent, hot, radial, dirs, vector, *tables, *weights))
    return (updated.transpose(1, 0, 2), forces)


def solution(mesh):
    both = ("slab", "yz")
    in_specs = (P(both, None, None), *([P(both)] * 7), *([P()] * 7))
    out_specs = (P(both, None, None), P(None, both))
    return jax.shard_map(body, mesh=mesh, in_specs=in_specs, out_specs=out_specs, check_vma=False)
```

```python
import functools
import math

import jax
import jax.numpy as jnp
from jax import lax
from jax.experimental import pallas as pl
from jax.experimental.pallas import tpu as pltpu
from jax.sharding import PartitionSpec as P


HIGHEST = lax.Precision.HIGHEST
BF16 = jnp.bfloat16
F32 = jnp.float32
ORDERS = (1, 2)
VMEM = pl.BlockSpec(memory_space=pltpu.VMEM)


def near(*arrays):
    return [pltpu.with_memory_space_constraint(array, pltpu.VMEM) for array in arrays]


def away(*arrays):
    return [pltpu.with_memory_space_constraint(array, pltpu.HBM) for array in arrays]


def slot_index(degree, azimuth_order):
    return degree * degree + degree + azimuth_order


def slot_groups(degrees):
    groups = [[slot_index(degree, 0) for degree in range(degrees)]]
    for order in ORDERS:
        groups.append([slot_index(degree, order) for degree in range(order, degrees)])
        groups.append([slot_index(degree, -order) for degree in range(order, degrees)])
    return groups


def slot_order(degrees):
    return [slot for group in slot_groups(degrees) for slot in group]


def unused_slots(coeffs):
    order = slot_order(math.isqrt(coeffs))
    return [slot for slot in range(coeffs) if slot not in order]


def odd_slab():
    return lax.axis_index("slab") % 2 == 1


def dot(left, right, contract=((1,), (0,)), precision=None):
    return lax.dot_general(
        left, right, (contract, ((), ())), precision=precision, preferred_element_type=F32
    )


def lent_picks(low_ref, high_ref):
    odd = odd_slab()
    low, high = low_ref[...], high_ref[...]
    return jnp.concatenate([jnp.where(odd, low, high), jnp.where(odd, high, low)], axis=1)


def lent_hot(picks, atoms):
    rows = lax.broadcasted_iota(jnp.int32, (atoms, picks.shape[1]), 0)
    return (rows == picks).astype(F32)


def lent_rows(hot, rows):
    return dot(hot.astype(BF16), rows, ((0,), (0,))).astype(BF16)


def pack_kernel(
    emb_ref, low_ref, high_ref, nbr_ref, valid_ref, dist_ref, azi_ref, pol_ref,
    own_ref, pair_ref, other_ref, rest_ref, facts_ref,
):
    coeffs, atoms, channels = emb_ref.shape
    ghosts = low_ref.shape[1]
    edges = nbr_ref.shape[1]
    order = slot_order(math.isqrt(coeffs))
    for place, slot in enumerate(order):
        own_ref[:, place * channels : (place + 1) * channels] = emb_ref[slot]
    for place, slot in enumerate(unused_slots(coeffs)):
        rest_ref[place] = emb_ref[slot]
    picks = lent_picks(low_ref, high_ref)
    lent = lent_rows(lent_hot(picks, atoms), own_ref[...])
    pair_ref[...] = lent[:ghosts]
    other_ref[...] = lent[ghosts:]
    facts_ref[...] = jnp.zeros(facts_ref.shape, F32)
    facts_ref[0:1, :edges] = nbr_ref[...].astype(F32)
    facts_ref[1:2, :edges] = valid_ref[...].astype(F32)
    facts_ref[2:3, :edges] = dist_ref[...]
    facts_ref[3:4, :edges] = azi_ref[...]
    facts_ref[4:5, :edges] = pol_ref[...]
    facts_ref[5:6, : 2 * ghosts] = picks.astype(F32)


def scale_kernel(
    atoms, ghosts, slab_devices,
    facts_ref, partner_ref, rw_ref, readout_ref, *refs,
):
    count = (len(refs) - 6) // 2
    far, held = refs[:count], refs[count + 5 : -1]
    hot_ref, radial_ref, flags_ref, vector_ref, lent_ref = refs[count : count + 5]
    sems = refs[-1]
    copies = [pltpu.make_async_copy(far[i], held[i], sems.at[i]) for i in range(count)]
    for copy in copies:
        copy.start()
    layers, centers = rw_ref.shape[0], rw_ref.shape[1]
    own_count, ghost_count = slab_devices * atoms, slab_devices * ghosts
    half = slab_devices // 2
    me = lax.axis_index("yz")
    odd = odd_slab()
    vector_ref[...] = 0.125 * readout_ref[...]
    for side, ref in enumerate((facts_ref, partner_ref)):
        edges = hot_ref.shape[0] // 2
        nbr = ref[0:1, :edges].astype(jnp.int32)
        is_own = nbr < own_count
        ghost = nbr - own_count
        below = ghost < ghost_count
        ghost = jnp.where(below, ghost, ghost - ghost_count)
        paired = jnp.where(odd, below.astype(jnp.int32), 1 - below.astype(jnp.int32))
        slot = jnp.where(is_own, nbr // atoms, ghost // ghosts) ^ me
        upper = slot // half
        inner = jnp.where(
            is_own,
            upper * atoms + nbr % atoms,
            2 * atoms + (1 - paired) * (2 * ghosts) + upper * ghosts + ghost % ghosts,
        )
        place = (slot % half) * (2 * atoms + 4 * ghosts) + inner
        rows = lax.broadcasted_iota(jnp.int32, (flags_ref.shape[0], edges), 0)
        hot = jnp.where((rows == place) & (ref[1:2, :edges] != 0.0), 1.0, 0.0).astype(F32)
        span = slice(side * edges, (side + 1) * edges)
        flags_ref[:, span] = hot
        hot_cols = jnp.transpose(hot).astype(BF16)
        hot_ref[span, :] = jnp.concatenate([hot_cols, hot_cols], axis=1)
        middle = 1.0 + 0.5 * lax.broadcasted_iota(jnp.int32, (centers, edges), 0).astype(F32)
        basis = jnp.exp(-jnp.square((ref[2:3, :edges] - middle) / 0.5))
        for layer in range(layers):
            scale = dot(basis, rw_ref[layer], ((0,), (0,)), HIGHEST)
            radial_ref[layer, span, :] = scale / (1.0 + jnp.exp(-scale))
        picks = ref[5:6, : 2 * ghosts].astype(jnp.int32)
        lent_ref[side] = lent_hot(picks, atoms)
    for copy in copies:
        copy.wait()


def pull_kernel(facts_ref, partner_ref, radial_ref, flags_ref, dirs_ref, pulls_ref):
    edges = flags_ref.shape[1] // 2
    channels = radial_ref.shape[2]
    for side, ref in enumerate((facts_ref, partner_ref)):
        azimuth, polar = ref[3:4, :edges], ref[4:5, :edges]
        sin_polar = jnp.sin(polar)
        dirs = [sin_polar * jnp.cos(azimuth), sin_polar * jnp.sin(azimuth), jnp.cos(polar)]
        dirs_ref[:, side * edges : (side + 1) * edges] = jnp.concatenate(dirs, axis=0)
    radial = radial_ref[radial_ref.shape[0] - 1]
    high = radial.astype(BF16)
    both = jnp.concatenate([high, (radial - high.astype(F32)).astype(BF16)], axis=1)
    for axis in range(3):
        along = flags_ref[...] * dirs_ref[axis : axis + 1, :]
        high = along.astype(BF16)
        low = (along - high.astype(F32)).astype(BF16)
        got = dot(jnp.concatenate([high, low], axis=0), both)
        rows = flags_ref.shape[0]
        got = got[:rows, :channels] + got[:rows, channels:] + got[rows:, :channels]
        pulls_ref[:, axis * channels : (axis + 1) * channels] = got.astype(BF16)


def layer_sums(layer, degrees, channels, atoms, per_atom, tables, weights, hot_ref, radial_ref, scratch):
    joined, mixed = scratch
    groups = slot_groups(degrees)
    w_zero, w_one_re, w_one_im, w_two_re, w_two_im = (ref[layer] for ref in weights)
    width = joined.shape[1]
    start = 0
    for ref in tables:
        count = ref.shape[0]
        joined[start : start + count] = ref[:, :width].astype(F32)
        start += count
    rows = start

    def put(column, value):
        high = value.astype(BF16)
        low = (value - high.astype(F32)).astype(BF16)
        mixed[:rows, column : column + value.shape[1]] = high
        mixed[rows:, column : column + value.shape[1]] = low

    span = len(groups[0]) * channels
    zero = dot(joined[:, :span].astype(BF16), w_zero)
    put(0, zero)
    column = span
    for index, (real, imag) in enumerate(((w_one_re, w_one_im), (w_two_re, w_two_im))):
        span = len(groups[2 * index + 1]) * channels
        both = jnp.concatenate(
            [joined[:, column : column + span], joined[:, column + span : column + 2 * span]], axis=0
        ).astype(BF16)
        by_real = dot(both, real)
        by_imag = dot(both, imag)
        put(column, by_real[:rows] - by_imag[rows:])
        put(column + span, by_imag[:rows] + by_real[rows:])
        column += 2 * span
    edges = atoms * per_atom
    radial = radial_ref[layer, :edges, :]
    hot = hot_ref[:edges, :]
    sums = []
    first = None
    step = 2 * channels
    for begin in range(0, width, step):
        got = dot(hot, mixed[:, begin : min(begin + step, width)])
        for inner in range(0, got.shape[1], channels):
            message = got[:, inner : inner + channels] * radial
            if first is None:
                first = message
            sums.append(message.reshape(atoms, per_atom, channels).sum(axis=1))
    return sums, first, zero


def first_kernel(
    layer, last, degrees, channels, per_atom, count,
    lent_ref, hot_ref, radial_ref, pulls_ref, *refs,
):
    tables, weights = refs[:count], refs[count : count + 5]
    own_ref, pair_ref, other_ref = refs[count + 5 : count + 8]
    scratch = refs[count + 8 :]
    joined = scratch[0]
    both = own_ref.shape[0]
    atoms, ghosts = both // 2, lent_ref.shape[2] // 2
    sums, _, _ = layer_sums(
        layer, degrees, channels, both, per_atom, tables, weights, hot_ref, radial_ref, scratch
    )
    width = len(sums) * channels
    for place, total in enumerate(sums):
        cols = slice(place * channels, (place + 1) * channels)
        own_ref[:, cols] = (joined[:both, cols] + 0.18 * total).astype(BF16)
    for side in range(2):
        lent = lent_rows(lent_ref[side], own_ref[side * atoms : (side + 1) * atoms, :width])
        pair_ref[side * ghosts : (side + 1) * ghosts, :width] = lent[:ghosts]
        other_ref[side * ghosts : (side + 1) * ghosts, :width] = lent[ghosts:]
    if last:
        part = pulls_ref.shape[1]
        block = 2 * atoms + 4 * ghosts
        for slot in range(pulls_ref.shape[0] // block):
            cols = slice(width + slot // 2 * part, width + (slot // 2 + 1) * part)
            at = slot * block
            for ref, size in ((own_ref, atoms), (pair_ref, ghosts), (other_ref, ghosts)):
                to = slot % 2 * size
                ref[to : to + size, cols] = pulls_ref[at : at + size]
                at += 2 * size


def last_kernel(
    layer, degrees, channels, atoms, per_atom, count,
    rest_ref, lent_ref, hot_ref, radial_ref, dirs_ref, readout_ref, *refs,
):
    tables, weights = refs[:count], refs[count : count + 5]
    out_ref, force_ref = refs[count + 5 : count + 7]
    scratch = refs[count + 7 :]
    joined = scratch[0]
    sums, first, zero = layer_sums(
        layer, degrees, channels, atoms, per_atom, tables, weights, hot_ref, radial_ref, scratch
    )
    order = slot_order(degrees)
    for place, slot in enumerate(order):
        cols = slice(place * channels, (place + 1) * channels)
        out_ref[slot] = (joined[:atoms, cols] + 0.18 * sums[place]).astype(BF16)
    for place, slot in enumerate(unused_slots(degrees * degrees)):
        out_ref[slot] = rest_ref[place]

    readout = readout_ref[...]
    strength = dot(readout, first, ((1,), (1,)), HIGHEST)
    edges = atoms * per_atom
    pull = dirs_ref[:, :edges] * strength
    edge = lax.broadcasted_iota(jnp.int32, (atoms, edges), 1)
    atom = lax.broadcasted_iota(jnp.int32, (atoms, edges), 0)
    owner = (edge // per_atom == atom).astype(F32)
    own_force = dot(pull, owner, ((1,), (1,)), HIGHEST)

    width = len(sums) * channels
    part = 3 * channels
    ghosts = lent_ref.shape[2] // 2
    kinds = [0.0, 0.0, 0.0]
    for slot in range(count // 3):
        cols = slice(width + slot // 2 * part, width + (slot // 2 + 1) * part)
        for kind, size in enumerate((atoms, ghosts, ghosts)):
            at = slot % 2 * size
            kinds[kind] += tables[3 * slot + kind][at : at + size, cols].astype(F32)
    lent = jnp.concatenate(kinds[1:], axis=0)
    pulls = kinds[0] + dot(lent_ref[0], lent, precision=HIGHEST)
    mine = zero[:atoms, :channels] * readout
    ones = jnp.ones((1, channels), F32)
    for axis in range(3):
        back = dot(
            ones, mine * pulls[:, axis * channels : (axis + 1) * channels], ((1,), (1,)), HIGHEST
        )
        force_ref[axis : axis + 1, :] = own_force[axis : axis + 1] - back


def across(block, bit, slab_devices):
    return lax.ppermute(block, "yz", [(q, q ^ bit) for q in range(slab_devices)])


def toward(block, step, slabs):
    route = []
    for slab in range(slabs):
        to = slab + 1 if (slab % 2 == 0) == (step > 0) else slab - 1
        route.append((slab, to % slabs))
    return lax.ppermute(block, "slab", route)


def spread(held, bits, slab_devices):
    for bit in bits:
        for slot in sorted(held):
            held[slot | bit] = tuple(across(block, bit, slab_devices) for block in held[slot])
    return held


def order_bits(slab_devices):
    bits, bit = [], slab_devices // 2
    while bit:
        bits.append(bit)
        bit //= 2
    return bits


def body(
    embeddings, neighbours, valid, azimuth, polar, distance, send_low, send_high,
    w_zero, w_one_re, w_one_im, w_two_re, w_two_im, radial_weight, readout,
):
    atoms, coeffs, channels = embeddings.shape
    degrees = math.isqrt(coeffs)
    ghosts = send_low.shape[0]
    edges = neighbours.shape[0]
    layers = w_zero.shape[0]
    slabs, slab_devices = lax.axis_size("slab"), lax.axis_size("yz")
    rows = slab_devices * (atoms + 2 * ghosts)
    width = len(slot_order(degrees)) * channels
    low, high = send_low.reshape(1, -1), send_high.reshape(1, -1)
    held, shape = pltpu.VMEM, jax.ShapeDtypeStruct
    embeddings = embeddings.transpose(1, 0, 2)
    params = pltpu.CompilerParams(vmem_limit_bytes=24 * 2**20)
    row = lambda value: value.reshape(1, -1)
    far = pl.BlockSpec(memory_space=pl.ANY)

    half = slab_devices // 2
    own, pair, other, rest, facts = pl.pallas_call(
        pack_kernel,
        out_shape=[
            held((atoms, width), BF16), held((ghosts, width), BF16), held((ghosts, width), BF16),
            held((len(unused_slots(coeffs)), atoms, channels), BF16),
            held((8, max(edges, 2 * ghosts)), F32),
        ],
        in_specs=[VMEM] * 8,
        out_specs=[VMEM] * 5,
        compiler_params=params,
        name="pack",
    )(*away(embeddings, low, high, *map(row, (neighbours, valid, distance, azimuth, polar))))

    partner = across(facts, half, slab_devices)
    got_other = toward(other, -1, slabs)
    got_pair = toward(pair, 1, slabs)
    got_own = across(own, half, slab_devices)
    weights = (w_zero, w_one_re, w_one_im, w_two_re, w_two_im)
    hot, radial, flags, vector, lent, *weights = pl.pallas_call(
        functools.partial(scale_kernel, atoms, ghosts, slab_devices),
        out_shape=[
            held((2 * edges, 2 * rows), BF16), held((layers, 2 * edges, channels), F32),
            held((rows, 2 * edges), F32), held((1, channels), F32), held((2, atoms, 2 * ghosts), F32),
            *(held(array.shape, array.dtype) for array in weights),
        ],
        in_specs=[VMEM] * 4 + [far] * len(weights),
        out_specs=[VMEM] * (5 + len(weights)),
        scratch_shapes=[pltpu.SemaphoreType.DMA((len(weights),))],
        compiler_params=params,
        name="scales",
    )(*near(facts, partner), *away(radial_weight, row(readout), *weights))
    dirs, pulls = pl.pallas_call(
        pull_kernel,
        out_shape=[held((3, 2 * edges), F32), held((rows, 3 * channels), BF16)],
        in_specs=[VMEM] * 4,
        out_specs=[VMEM] * 2,
        compiler_params=params,
        name="pulls",
    )(*near(facts, partner, radial, flags))

    bits = order_bits(slab_devices)
    got_pair, hot, radial = lax.optimization_barrier((got_pair, hot, radial))
    blocks = {0: (own, got_pair, got_other)}
    pair_y = across(got_pair, half, slab_devices)
    other_y = across(got_other, half, slab_devices)
    blocks[half] = (got_own, pair_y, other_y)
    blocks = spread(blocks, bits[1:], slab_devices)
    tables = [
        blocks[slot + upper][kind]
        for slot in range(half) for kind in range(3) for upper in (0, half)
    ]
    scratch = [pltpu.VMEM((rows, width), F32), pltpu.VMEM((2 * rows, width), BF16)]
    per_atom = edges // atoms
    for layer in range(layers):
        if layer < layers - 1:
            last = layer == layers - 2
            wide = width + ((half + 1) // 2 * 3 * channels if last else 0)
            own, pair, other = pl.pallas_call(
                functools.partial(first_kernel, layer, last, degrees, channels, per_atom, len(tables)),
                out_shape=[
                    held((2 * atoms, wide), BF16), held((2 * ghosts, wide), BF16),
                    held((2 * ghosts, wide), BF16),
                ],
                in_specs=[VMEM] * (4 + len(tables) + len(weights)),
                out_specs=[VMEM] * 3,
                scratch_shapes=scratch,
                compiler_params=params,
                name="layer",
            )(*near(lent, hot, radial, pulls, *tables, *weights))
            got_other = toward(other, -1, slabs)
            got_pair = toward(pair, 1, slabs)
            blocks = spread({0: (own, got_pair, got_other)}, bits[1:], slab_devices)
            tables = [block for slot in range(half) for block in blocks[slot]]
        else:
            updated, forces = pl.pallas_call(
                functools.partial(
                    last_kernel, layer, degrees, channels, atoms, per_atom, len(tables)
                ),
                out_shape=[shape((coeffs, atoms, channels), BF16), shape((3, atoms), F32)],
                in_specs=[VMEM] * (6 + len(tables) + len(weights)),
                out_specs=[VMEM] * 2,
                scratch_shapes=scratch,
                compiler_params=params,
                name="last_layer",
            )(*near(rest, lent, hot, radial, dirs, vector, *tables, *weights))
    return (updated.transpose(1, 0, 2), forces)


def solution(mesh):
    both = ("slab", "yz")
    in_specs = (P(both, None, None), *([P(both)] * 7), *([P()] * 7))
    out_specs = (P(both, None, None), P(None, both))
    return jax.shard_map(body, mesh=mesh, in_specs=in_specs, out_specs=out_specs, check_vma=False)
```

```python
import functools
import math

import jax
import jax.numpy as jnp
from jax import lax
from jax.experimental import pallas as pl
from jax.experimental.pallas import tpu as pltpu
from jax.sharding import PartitionSpec as P


HIGHEST = lax.Precision.HIGHEST
BF16 = jnp.bfloat16
F32 = jnp.float32
ORDERS = (1, 2)
VMEM = pl.BlockSpec(memory_space=pltpu.VMEM)


def near(*arrays):
    return [pltpu.with_memory_space_constraint(array, pltpu.VMEM) for array in arrays]


def away(*arrays):
    return [pltpu.with_memory_space_constraint(array, pltpu.HBM) for array in arrays]


def slot_index(degree, azimuth_order):
    return degree * degree + degree + azimuth_order


def slot_groups(degrees):
    groups = [[slot_index(degree, 0) for degree in range(degrees)]]
    for order in ORDERS:
        groups.append([slot_index(degree, order) for degree in range(order, degrees)])
        groups.append([slot_index(degree, -order) for degree in range(order, degrees)])
    return groups


def slot_order(degrees):
    return [slot for group in slot_groups(degrees) for slot in group]


def unused_slots(coeffs):
    order = slot_order(math.isqrt(coeffs))
    return [slot for slot in range(coeffs) if slot not in order]


def odd_slab():
    return lax.axis_index("slab") % 2 == 1


def dot(left, right, contract=((1,), (0,)), precision=None):
    return lax.dot_general(
        left, right, (contract, ((), ())), precision=precision, preferred_element_type=F32
    )


def lent_picks(low_ref, high_ref):
    odd = odd_slab()
    low, high = low_ref[...], high_ref[...]
    return jnp.concatenate([jnp.where(odd, low, high), jnp.where(odd, high, low)], axis=1)


def lent_hot(picks, atoms):
    rows = lax.broadcasted_iota(jnp.int32, (atoms, picks.shape[1]), 0)
    return (rows == picks).astype(F32)


def lent_rows(hot, rows):
    return dot(hot.astype(BF16), rows, ((0,), (0,))).astype(BF16)


def pack_kernel(
    emb_ref, low_ref, high_ref, nbr_ref, valid_ref, dist_ref, azi_ref, pol_ref,
    own_ref, pair_ref, other_ref, rest_ref, facts_ref,
):
    coeffs, atoms, channels = emb_ref.shape
    ghosts = low_ref.shape[1]
    edges = nbr_ref.shape[1]
    order = slot_order(math.isqrt(coeffs))
    for place, slot in enumerate(order):
        own_ref[:, place * channels : (place + 1) * channels] = emb_ref[slot]
    for place, slot in enumerate(unused_slots(coeffs)):
        rest_ref[place] = emb_ref[slot]
    picks = lent_picks(low_ref, high_ref)
    lent = lent_rows(lent_hot(picks, atoms), own_ref[...])
    pair_ref[...] = lent[:ghosts]
    other_ref[...] = lent[ghosts:]
    facts_ref[...] = jnp.zeros(facts_ref.shape, F32)
    facts_ref[0:1, :edges] = nbr_ref[...].astype(F32)
    facts_ref[1:2, :edges] = valid_ref[...].astype(F32)
    facts_ref[2:3, :edges] = dist_ref[...]
    facts_ref[3:4, :edges] = azi_ref[...]
    facts_ref[4:5, :edges] = pol_ref[...]
    facts_ref[5:6, : 2 * ghosts] = picks.astype(F32)


def start_fetch(refs, layer):
    count = len(refs) // 2
    copies = [
        pltpu.make_async_copy(refs[i].at[layer], refs[count + i], refs[-1].at[i])
        for i in range(count)
    ]
    for copy in copies:
        copy.start()
    return copies


def edge_scales(
    atoms, ghosts, slab_devices, facts_ref, rw_ref, hot_ref, radial_ref, flags_ref, lent_ref
):
    layers, centers = rw_ref.shape[0], rw_ref.shape[1]
    own_count, ghost_count = slab_devices * atoms, slab_devices * ghosts
    half = slab_devices // 2
    me = lax.axis_index("yz")
    odd = odd_slab()
    edges = hot_ref.shape[0]
    nbr = facts_ref[0:1, :edges].astype(jnp.int32)
    is_own = nbr < own_count
    ghost = nbr - own_count
    below = ghost < ghost_count
    ghost = jnp.where(below, ghost, ghost - ghost_count)
    paired = jnp.where(odd, below.astype(jnp.int32), 1 - below.astype(jnp.int32))
    slot = jnp.where(is_own, nbr // atoms, ghost // ghosts) ^ me
    upper = slot // half
    inner = jnp.where(
        is_own,
        upper * atoms + nbr % atoms,
        2 * atoms + (1 - paired) * (2 * ghosts) + upper * ghosts + ghost % ghosts,
    )
    place = (slot % half) * (2 * atoms + 4 * ghosts) + inner
    rows = lax.broadcasted_iota(jnp.int32, (flags_ref.shape[0], edges), 0)
    hot = jnp.where((rows == place) & (facts_ref[1:2, :edges] != 0.0), 1.0, 0.0).astype(F32)
    flags_ref[...] = hot
    hot_cols = jnp.transpose(hot).astype(BF16)
    hot_ref[...] = jnp.concatenate([hot_cols, hot_cols], axis=1)
    middle = 1.0 + 0.5 * lax.broadcasted_iota(jnp.int32, (centers, edges), 0).astype(F32)
    basis = jnp.exp(-jnp.square((facts_ref[2:3, :edges] - middle) / 0.5))
    for layer in range(layers):
        scale = dot(basis, rw_ref[layer], ((0,), (0,)), HIGHEST)
        radial_ref[layer] = scale / (1.0 + jnp.exp(-scale))
    lent_ref[...] = lent_hot(facts_ref[5:6, : 2 * ghosts].astype(jnp.int32), atoms)


def own_scale_kernel(
    atoms, ghosts, slab_devices, count,
    facts_ref, rw_ref, readout_ref, *refs,
):
    far, refs = refs[:count], refs[count:]
    hot_ref, radial_ref, flags_ref, lent_ref, vector_ref, scales_ref = refs[:6]
    copies = start_fetch((*far, *refs[6:]), 0)
    vector_ref[...] = 0.125 * readout_ref[...]
    scales_ref[...] = rw_ref[...]
    edge_scales(
        atoms, ghosts, slab_devices, facts_ref, rw_ref, hot_ref, radial_ref, flags_ref, lent_ref
    )
    for copy in copies:
        copy.wait()


def partner_scale_kernel(
    atoms, ghosts, slab_devices, count, fetched,
    facts_ref, rw_ref, *refs,
):
    far, refs = refs[:count], refs[count:]
    copies = [start_fetch((*far, *refs[4 + count * i : 4 + count * (i + 1)], refs[-1].at[i]), layer)
              for i, layer in enumerate(fetched)]
    edge_scales(atoms, ghosts, slab_devices, facts_ref, rw_ref, *refs[:4])
    for group in copies:
        for copy in group:
            copy.wait()


def pull_kernel(
    facts_ref, radial_ref, flags_ref, partner_ref, radial_y_ref, flags_y_ref, dirs_ref, pulls_ref
):
    edges, channels = radial_ref.shape[1:]
    last = radial_ref.shape[0] - 1
    rows = flags_ref.shape[0]
    totals = [0.0, 0.0, 0.0]
    for ref, scale_ref, hot_ref in (
        (facts_ref, radial_ref, flags_ref), (partner_ref, radial_y_ref, flags_y_ref)
    ):
        azimuth, polar = ref[3:4, :edges], ref[4:5, :edges]
        sin_polar = jnp.sin(polar)
        dirs = [sin_polar * jnp.cos(azimuth), sin_polar * jnp.sin(azimuth), jnp.cos(polar)]
        if ref is facts_ref:
            dirs_ref[...] = jnp.concatenate(dirs, axis=0)
        radial = scale_ref[last]
        high = radial.astype(BF16)
        both = jnp.concatenate([high, (radial - high.astype(F32)).astype(BF16)], axis=1)
        for axis in range(3):
            along = hot_ref[...] * dirs[axis]
            high = along.astype(BF16)
            low = (along - high.astype(F32)).astype(BF16)
            got = dot(jnp.concatenate([high, low], axis=0), both)
            totals[axis] += (
                got[:rows, :channels] + got[:rows, channels:] + got[rows:, :channels]
            )
    pulls_ref[...] = jnp.concatenate(totals, axis=1).astype(BF16)


def layer_sums(layer, degrees, channels, atoms, per_atom, tables, weights, hots, radials, scratch):
    joined, mixed = scratch
    groups = slot_groups(degrees)
    w_zero, w_one_re, w_one_im, w_two_re, w_two_im = (ref[...] for ref in weights)
    width = joined.shape[1]
    start = 0
    for ref in tables:
        count = ref.shape[0]
        joined[start : start + count] = ref[:, :width].astype(F32)
        start += count
    rows = start

    def put(column, value):
        high = value.astype(BF16)
        low = (value - high.astype(F32)).astype(BF16)
        mixed[:rows, column : column + value.shape[1]] = high
        mixed[rows:, column : column + value.shape[1]] = low

    span = len(groups[0]) * channels
    zero = dot(joined[:, :span].astype(BF16), w_zero)
    put(0, zero)
    column = span
    for index, (real, imag) in enumerate(((w_one_re, w_one_im), (w_two_re, w_two_im))):
        span = len(groups[2 * index + 1]) * channels
        both = jnp.concatenate(
            [joined[:, column : column + span], joined[:, column + span : column + 2 * span]], axis=0
        ).astype(BF16)
        by_real = dot(both, real)
        by_imag = dot(both, imag)
        put(column, by_real[:rows] - by_imag[rows:])
        put(column + span, by_imag[:rows] + by_real[rows:])
        column += 2 * span
    part = atoms // len(hots)
    sums = []
    first = None
    step = 2 * channels
    for begin in range(0, width, step):
        end = min(begin + step, width)
        pieces = []
        for hot_ref, radial_ref in zip(hots, radials):
            got = dot(hot_ref[...], mixed[:, begin:end])
            for inner in range(0, end - begin, channels):
                message = got[:, inner : inner + channels] * radial_ref[layer]
                if first is None:
                    first = message
                pieces.append(message.reshape(part, per_atom, channels).sum(axis=1))
        count = (end - begin) // channels
        for inner in range(count):
            sums.append(jnp.concatenate(pieces[inner::count], axis=0))
    return sums, first, zero


def first_kernel(
    layer, last, degrees, channels, per_atom, count,
    lent_ref, hot_ref, radial_ref, lent_y_ref, hot_y_ref, radial_y_ref, pulls_ref, *refs,
):
    tables, weights = refs[:count], refs[count : count + 5]
    own_ref, pair_ref, other_ref = refs[count + 5 : count + 8]
    scratch = refs[count + 8 :]
    joined = scratch[0]
    both = own_ref.shape[0]
    atoms, ghosts = both // 2, lent_ref.shape[1] // 2
    sums, _, _ = layer_sums(
        layer, degrees, channels, both, per_atom, tables, weights,
        (hot_ref, hot_y_ref), (radial_ref, radial_y_ref), scratch,
    )
    width = len(sums) * channels
    for place, total in enumerate(sums):
        cols = slice(place * channels, (place + 1) * channels)
        own_ref[:, cols] = (joined[:both, cols] + 0.18 * total).astype(BF16)
    for side, hot in enumerate((lent_ref, lent_y_ref)):
        lent = lent_rows(hot[...], own_ref[side * atoms : (side + 1) * atoms, :width])
        pair_ref[side * ghosts : (side + 1) * ghosts, :width] = lent[:ghosts]
        other_ref[side * ghosts : (side + 1) * ghosts, :width] = lent[ghosts:]
    if last:
        part = pulls_ref.shape[1]
        block = 2 * atoms + 4 * ghosts
        for slot in range(pulls_ref.shape[0] // block):
            cols = slice(width + slot // 2 * part, width + (slot // 2 + 1) * part)
            at = slot * block
            for ref, size in ((own_ref, atoms), (pair_ref, ghosts), (other_ref, ghosts)):
                to = slot % 2 * size
                ref[to : to + size, cols] = pulls_ref[at : at + size]
                at += 2 * size


def last_kernel(
    layer, degrees, channels, atoms, per_atom, count,
    rest_ref, lent_ref, hot_ref, radial_ref, dirs_ref, readout_ref, *refs,
):
    tables, weights = refs[:count], refs[count : count + 5]
    out_ref, force_ref = refs[count + 5 : count + 7]
    scratch = refs[count + 7 :]
    joined = scratch[0]
    sums, first, zero = layer_sums(
        layer, degrees, channels, atoms, per_atom, tables, weights, (hot_ref,), (radial_ref,), scratch
    )
    order = slot_order(degrees)
    for place, slot in enumerate(order):
        cols = slice(place * channels, (place + 1) * channels)
        out_ref[slot] = (joined[:atoms, cols] + 0.18 * sums[place]).astype(BF16)
    for place, slot in enumerate(unused_slots(degrees * degrees)):
        out_ref[slot] = rest_ref[place]

    readout = readout_ref[...]
    strength = dot(readout, first, ((1,), (1,)), HIGHEST)
    edges = atoms * per_atom
    pull = dirs_ref[...] * strength
    edge = lax.broadcasted_iota(jnp.int32, (atoms, edges), 1)
    atom = lax.broadcasted_iota(jnp.int32, (atoms, edges), 0)
    owner = (edge // per_atom == atom).astype(F32)
    own_force = dot(pull, owner, ((1,), (1,)), HIGHEST)

    width = len(sums) * channels
    part = 3 * channels
    ghosts = lent_ref.shape[1] // 2
    kinds = [0.0, 0.0, 0.0]
    for slot in range(count // 3):
        cols = slice(width + slot // 2 * part, width + (slot // 2 + 1) * part)
        for kind, size in enumerate((atoms, ghosts, ghosts)):
            at = slot % 2 * size
            kinds[kind] += tables[3 * slot + kind][at : at + size, cols].astype(F32)
    lent = jnp.concatenate(kinds[1:], axis=0)
    pulls = kinds[0] + dot(lent_ref[...], lent, precision=HIGHEST)
    mine = zero[:atoms, :channels] * readout
    ones = jnp.ones((1, channels), F32)
    for axis in range(3):
        back = dot(
            ones, mine * pulls[:, axis * channels : (axis + 1) * channels], ((1,), (1,)), HIGHEST
        )
        force_ref[axis : axis + 1, :] = own_force[axis : axis + 1] - back


def across(block, bit, slab_devices):
    return lax.ppermute(block, "yz", [(q, q ^ bit) for q in range(slab_devices)])


def toward(block, step, slabs):
    route = []
    for slab in range(slabs):
        to = slab + 1 if (slab % 2 == 0) == (step > 0) else slab - 1
        route.append((slab, to % slabs))
    return lax.ppermute(block, "slab", route)


def spread(held, bits, slab_devices):
    for bit in bits:
        for slot in sorted(held):
            held[slot | bit] = tuple(across(block, bit, slab_devices) for block in held[slot])
    return held


def order_bits(slab_devices):
    bits, bit = [], slab_devices // 2
    while bit:
        bits.append(bit)
        bit //= 2
    return bits


def body(
    embeddings, neighbours, valid, azimuth, polar, distance, send_low, send_high,
    w_zero, w_one_re, w_one_im, w_two_re, w_two_im, radial_weight, readout,
):
    atoms, coeffs, channels = embeddings.shape
    degrees = math.isqrt(coeffs)
    ghosts = send_low.shape[0]
    edges = neighbours.shape[0]
    layers = w_zero.shape[0]
    slabs, slab_devices = lax.axis_size("slab"), lax.axis_size("yz")
    rows = slab_devices * (atoms + 2 * ghosts)
    width = len(slot_order(degrees)) * channels
    low, high = send_low.reshape(1, -1), send_high.reshape(1, -1)
    held, shape = pltpu.VMEM, jax.ShapeDtypeStruct
    embeddings = embeddings.transpose(1, 0, 2)
    params = pltpu.CompilerParams(vmem_limit_bytes=24 * 2**20)
    row = lambda value: value.reshape(1, -1)
    far = pl.BlockSpec(memory_space=pl.ANY)

    half = slab_devices // 2
    own, pair, other, rest, facts = pl.pallas_call(
        pack_kernel,
        out_shape=[
            held((atoms, width), BF16), held((ghosts, width), BF16), held((ghosts, width), BF16),
            held((len(unused_slots(coeffs)), atoms, channels), BF16),
            held((8, max(edges, 2 * ghosts)), F32),
        ],
        in_specs=[VMEM] * 8,
        out_specs=[VMEM] * 5,
        compiler_params=params,
        name="pack",
    )(*away(embeddings, low, high, *map(row, (neighbours, valid, distance, azimuth, polar))))

    partner = across(facts, half, slab_devices)
    got_other = toward(other, -1, slabs)
    got_pair = toward(pair, 1, slabs)
    got_own = across(own, half, slab_devices)
    weights = (w_zero, w_one_re, w_one_im, w_two_re, w_two_im)
    count = len(weights)
    near_weights = [held(array.shape[1:], array.dtype) for array in weights]
    side_shapes = [
        held((edges, 2 * rows), BF16), held((layers, edges, channels), F32),
        held((rows, edges), F32), held((atoms, 2 * ghosts), F32),
    ]
    hot, radial, flags, lent, vector, radial_weight, *first_weights = pl.pallas_call(
        functools.partial(own_scale_kernel, atoms, ghosts, slab_devices, count),
        out_shape=[
            *side_shapes, held((1, channels), F32), held(radial_weight.shape, F32),
            *near_weights,
        ],
        in_specs=[VMEM] * 3 + [far] * count,
        out_specs=[VMEM] * (6 + count),
        scratch_shapes=[pltpu.SemaphoreType.DMA((count,))],
        compiler_params=params,
        name="scales",
    )(*near(facts), *away(radial_weight, row(readout), *weights))
    got_pair, facts, radial_weight = lax.optimization_barrier((got_pair, facts, radial_weight))
    pair_y = across(got_pair, half, slab_devices)
    other_y = across(got_other, half, slab_devices)
    fetched = tuple(range(1, layers))
    hot_y, radial_y, flags_y, lent_y, *later_weights = pl.pallas_call(
        functools.partial(partner_scale_kernel, atoms, ghosts, slab_devices, count, fetched),
        out_shape=[*side_shapes, *(near_weights * len(fetched))],
        in_specs=[VMEM] * 2 + [far] * count,
        out_specs=[VMEM] * (4 + count * len(fetched)),
        scratch_shapes=[pltpu.SemaphoreType.DMA((len(fetched), count))],
        compiler_params=params,
        name="scales_y",
    )(*near(partner, radial_weight), *away(*weights))
    dirs, pulls = pl.pallas_call(
        pull_kernel,
        out_shape=[held((3, edges), F32), held((rows, 3 * channels), BF16)],
        in_specs=[VMEM] * 6,
        out_specs=[VMEM] * 2,
        compiler_params=params,
        name="pulls",
    )(*near(facts, radial, flags, partner, radial_y, flags_y))
    weights = (*first_weights, *later_weights)

    bits = order_bits(slab_devices)
    blocks = {0: (own, got_pair, got_other)}
    blocks[half] = (got_own, pair_y, other_y)
    blocks = spread(blocks, bits[1:], slab_devices)
    tables = [
        blocks[slot + upper][kind]
        for slot in range(half) for kind in range(3) for upper in (0, half)
    ]
    scratch = [pltpu.VMEM((rows, width), F32), pltpu.VMEM((2 * rows, width), BF16)]
    per_atom = edges // atoms
    for layer in range(layers):
        now = weights[layer * count : (layer + 1) * count]
        if layer < layers - 1:
            last = layer == layers - 2
            wide = width + ((half + 1) // 2 * 3 * channels if last else 0)
            own, pair, other = pl.pallas_call(
                functools.partial(first_kernel, layer, last, degrees, channels, per_atom, len(tables)),
                out_shape=[
                    held((2 * atoms, wide), BF16), held((2 * ghosts, wide), BF16),
                    held((2 * ghosts, wide), BF16),
                ],
                in_specs=[VMEM] * (7 + len(tables) + count),
                out_specs=[VMEM] * 3,
                scratch_shapes=scratch,
                compiler_params=params,
                name="layer",
            )(*near(lent, hot, radial, lent_y, hot_y, radial_y, pulls, *tables, *now))
            got_other = toward(other, -1, slabs)
            got_pair = toward(pair, 1, slabs)
            blocks = spread({0: (own, got_pair, got_other)}, bits[1:], slab_devices)
            tables = [block for slot in range(half) for block in blocks[slot]]
        else:
            updated, forces = pl.pallas_call(
                functools.partial(
                    last_kernel, layer, degrees, channels, atoms, per_atom, len(tables)
                ),
                out_shape=[shape((coeffs, atoms, channels), BF16), shape((3, atoms), F32)],
                in_specs=[VMEM] * (6 + len(tables) + count),
                out_specs=[VMEM] * 2,
                scratch_shapes=scratch,
                compiler_params=params,
                name="last_layer",
            )(*near(rest, lent, hot, radial, dirs, vector, *tables, *now))
    return (updated.transpose(1, 0, 2), forces)


def solution(mesh):
    both = ("slab", "yz")
    in_specs = (P(both, None, None), *([P(both)] * 7), *([P()] * 7))
    out_specs = (P(both, None, None), P(None, both))
    return jax.shard_map(body, mesh=mesh, in_specs=in_specs, out_specs=out_specs, check_vma=False)
```

```python
import functools
import math

import jax
import jax.numpy as jnp
from jax import lax
from jax.experimental import pallas as pl
from jax.experimental.pallas import tpu as pltpu
from jax.sharding import PartitionSpec as P


HIGHEST = lax.Precision.HIGHEST
BF16 = jnp.bfloat16
F32 = jnp.float32
ORDERS = (1, 2)
DIGIT = 128
VMEM = pl.BlockSpec(memory_space=pltpu.VMEM)


def near(*arrays):
    return [pltpu.with_memory_space_constraint(array, pltpu.VMEM) for array in arrays]


def away(*arrays):
    return [pltpu.with_memory_space_constraint(array, pltpu.HBM) for array in arrays]


def slot_index(degree, azimuth_order):
    return degree * degree + degree + azimuth_order


def slot_groups(degrees):
    groups = [[slot_index(degree, 0) for degree in range(degrees)]]
    for order in ORDERS:
        groups.append([slot_index(degree, order) for degree in range(order, degrees)])
        groups.append([slot_index(degree, -order) for degree in range(order, degrees)])
    return groups


def slot_order(degrees):
    return [slot for group in slot_groups(degrees) for slot in group]


def unused_slots(coeffs):
    order = slot_order(math.isqrt(coeffs))
    return [slot for slot in range(coeffs) if slot not in order]


def odd_slab():
    return lax.axis_index("slab") % 2 == 1


def dot(left, right, contract=((1,), (0,)), precision=None):
    return lax.dot_general(
        left, right, (contract, ((), ())), precision=precision, preferred_element_type=F32
    )


def lent_picks(low_ref, high_ref):
    odd = odd_slab()
    low, high = low_ref[...], high_ref[...]
    return jnp.concatenate([jnp.where(odd, low, high), jnp.where(odd, high, low)], axis=1)


def lent_hot(picks, atoms):
    rows = lax.broadcasted_iota(jnp.int32, (atoms, picks.shape[1]), 0)
    return (rows == picks).astype(F32)


def lent_rows(hot, rows):
    return dot(hot.astype(BF16), rows, ((0,), (0,))).astype(BF16)


def thirds(value):
    parts = []
    for _ in range(3):
        part = value.astype(BF16).astype(F32)
        parts.append(part)
        value = value - part
    return parts


def pack_kernel(
    emb_ref, low_ref, high_ref, nbr_ref, valid_ref, dist_ref, azi_ref, pol_ref, rw_ref, readout_ref,
    own_ref, pair_ref, other_ref, rest_ref, scales_ref, vector_ref,
):
    coeffs, atoms, channels = emb_ref.shape
    ghosts = low_ref.shape[1]
    edges = nbr_ref.shape[1]
    order = slot_order(math.isqrt(coeffs))
    width = len(order) * channels
    for place, slot in enumerate(order):
        own_ref[:, place * channels : (place + 1) * channels] = emb_ref[slot]
    for place, slot in enumerate(unused_slots(coeffs)):
        rest_ref[place] = emb_ref[slot]
    picks = lent_picks(low_ref, high_ref)
    lent = lent_rows(lent_hot(picks, atoms), own_ref[:, :width])
    pair_ref[...] = lent[:ghosts]
    other_ref[...] = lent[ghosts:]
    nbr = nbr_ref[...]
    picks = jnp.concatenate(
        [picks, jnp.zeros((1, edges - 2 * ghosts), jnp.int32)], axis=1
    ).astype(F32)
    facts = [
        (nbr // DIGIT).astype(F32), (nbr % DIGIT).astype(F32), valid_ref[...].astype(F32), picks,
        *thirds(dist_ref[...]), *thirds(azi_ref[...]), *thirds(pol_ref[...]),
    ]
    facts.append(jnp.zeros((atoms - len(facts), edges), F32))
    own_ref[:, width:] = jnp.concatenate(facts, axis=0).astype(BF16)
    scales_ref[...] = rw_ref[...]
    vector_ref[...] = 0.125 * readout_ref[...]


def edge_facts(ref, edges):
    rows = ref[:, ref.shape[1] - edges :].astype(F32)
    row = lambda at: rows[at : at + 1]
    whole = lambda at: row(at) + row(at + 1) + row(at + 2)
    nbr = (row(0) * DIGIT + row(1)).astype(jnp.int32)
    return nbr, row(2), row(3).astype(jnp.int32), whole(4), whole(7), whole(10)


def start_fetch(refs, layer):
    count = len(refs) // 2
    copies = [
        pltpu.make_async_copy(refs[i].at[layer], refs[count + i], refs[-1].at[i])
        for i in range(count)
    ]
    for copy in copies:
        copy.start()
    return copies


def edge_scales(
    atoms, ghosts, slab_devices, facts_ref, rw_ref, hot_ref, radial_ref, flags_ref, lent_ref
):
    layers, centers = rw_ref.shape[0], rw_ref.shape[1]
    own_count, ghost_count = slab_devices * atoms, slab_devices * ghosts
    half = slab_devices // 2
    me = lax.axis_index("yz")
    odd = odd_slab()
    edges = hot_ref.shape[0]
    nbr, valid, picks, distance, _, _ = edge_facts(facts_ref, edges)
    is_own = nbr < own_count
    ghost = nbr - own_count
    below = ghost < ghost_count
    ghost = jnp.where(below, ghost, ghost - ghost_count)
    paired = jnp.where(odd, below.astype(jnp.int32), 1 - below.astype(jnp.int32))
    slot = jnp.where(is_own, nbr // atoms, ghost // ghosts) ^ me
    upper = slot // half
    inner = jnp.where(
        is_own,
        upper * atoms + nbr % atoms,
        2 * atoms + (1 - paired) * (2 * ghosts) + upper * ghosts + ghost % ghosts,
    )
    place = (slot % half) * (2 * atoms + 4 * ghosts) + inner
    rows = lax.broadcasted_iota(jnp.int32, (flags_ref.shape[0], edges), 0)
    hot = jnp.where((rows == place) & (valid != 0.0), 1.0, 0.0).astype(F32)
    flags_ref[...] = hot
    hot_cols = jnp.transpose(hot).astype(BF16)
    hot_ref[...] = jnp.concatenate([hot_cols, hot_cols], axis=1)
    middle = 1.0 + 0.5 * lax.broadcasted_iota(jnp.int32, (centers, edges), 0).astype(F32)
    basis = jnp.exp(-jnp.square((distance - middle) / 0.5))
    for layer in range(layers):
        scale = dot(basis, rw_ref[layer], ((0,), (0,)), HIGHEST)
        radial_ref[layer] = scale / (1.0 + jnp.exp(-scale))
    lent_ref[...] = lent_hot(picks[:, : 2 * ghosts], atoms)


def scale_kernel(atoms, ghosts, slab_devices, count, facts_ref, rw_ref, *refs):
    far, refs = refs[:count], refs[count:]
    copies = start_fetch((*far, *refs[4:]), 0) if count else ()
    edge_scales(atoms, ghosts, slab_devices, facts_ref, rw_ref, *refs[:4])
    for copy in copies:
        copy.wait()


def pull_kernel(
    facts_ref, radial_ref, flags_ref, partner_ref, radial_y_ref, flags_y_ref, dirs_ref, pulls_ref
):
    edges, channels = radial_ref.shape[1:]
    last = radial_ref.shape[0] - 1
    rows = flags_ref.shape[0]
    totals = [0.0, 0.0, 0.0]
    for ref, scale_ref, hot_ref in (
        (facts_ref, radial_ref, flags_ref), (partner_ref, radial_y_ref, flags_y_ref)
    ):
        _, _, _, _, azimuth, polar = edge_facts(ref, edges)
        sin_polar = jnp.sin(polar)
        dirs = [sin_polar * jnp.cos(azimuth), sin_polar * jnp.sin(azimuth), jnp.cos(polar)]
        if ref is facts_ref:
            columns = jnp.transpose(jnp.concatenate([*dirs, *dirs, *dirs[:2]], axis=0))
            for axis in range(3):
                dirs_ref[axis] = jnp.broadcast_to(columns[:, axis : axis + 1], (edges, channels))
        radial = scale_ref[last]
        high = radial.astype(BF16)
        both = jnp.concatenate([high, (radial - high.astype(F32)).astype(BF16)], axis=1)
        for axis in range(3):
            along = hot_ref[...] * dirs[axis]
            high = along.astype(BF16)
            low = (along - high.astype(F32)).astype(BF16)
            got = dot(jnp.concatenate([high, low], axis=0), both)
            totals[axis] += (
                got[:rows, :channels] + got[:rows, channels:] + got[rows:, :channels]
            )
    pulls_ref[...] = jnp.concatenate(totals, axis=1).astype(BF16)


def layer_sums(layer, degrees, channels, atoms, per_atom, tables, weights, hots, radials, scratch):
    joined, mixed = scratch
    groups = slot_groups(degrees)
    w_zero, w_one_re, w_one_im, w_two_re, w_two_im = (ref[...] for ref in weights)
    width = joined.shape[1]
    start = 0
    for ref in tables:
        count = ref.shape[0]
        joined[start : start + count] = ref[:, :width].astype(F32)
        start += count
    rows = start

    def put(column, value):
        high = value.astype(BF16)
        low = (value - high.astype(F32)).astype(BF16)
        mixed[:rows, column : column + value.shape[1]] = high
        mixed[rows:, column : column + value.shape[1]] = low

    span = len(groups[0]) * channels
    zero = dot(joined[:, :span].astype(BF16), w_zero)
    put(0, zero)
    column = span
    for index, (real, imag) in enumerate(((w_one_re, w_one_im), (w_two_re, w_two_im))):
        span = len(groups[2 * index + 1]) * channels
        both = jnp.concatenate(
            [joined[:, column : column + span], joined[:, column + span : column + 2 * span]], axis=0
        ).astype(BF16)
        by_real = dot(both, real)
        by_imag = dot(both, imag)
        put(column, by_real[:rows] - by_imag[rows:])
        put(column + span, by_imag[:rows] + by_real[rows:])
        column += 2 * span
    part = atoms // len(hots)
    sums = []
    first = None
    step = 2 * channels
    for begin in range(0, width, step):
        end = min(begin + step, width)
        pieces = []
        for hot_ref, radial_ref in zip(hots, radials):
            got = dot(hot_ref[...], mixed[:, begin:end])
            for inner in range(0, end - begin, channels):
                message = got[:, inner : inner + channels] * radial_ref[layer]
                if first is None:
                    first = message
                pieces.append(message.reshape(part, per_atom, channels).sum(axis=1))
        count = (end - begin) // channels
        for inner in range(count):
            sums.append(jnp.concatenate(pieces[inner::count], axis=0))
    return sums, first, zero


def first_kernel(
    layer, last, degrees, channels, per_atom, count,
    lent_ref, hot_ref, radial_ref, lent_y_ref, hot_y_ref, radial_y_ref, pulls_ref, *refs,
):
    tables, weights, far = refs[:count], refs[count : count + 5], refs[count + 5 : count + 10]
    own_ref, pair_ref, other_ref = refs[count + 10 : count + 13]
    scratch = refs[count + 18 : count + 20]
    copies = start_fetch((*far, *refs[count + 13 : count + 18], refs[-1]), layer + 1)
    joined = scratch[0]
    both = own_ref.shape[0]
    atoms, ghosts = both // 2, lent_ref.shape[1] // 2
    sums, _, _ = layer_sums(
        layer, degrees, channels, both, per_atom, tables, weights,
        (hot_ref, hot_y_ref), (radial_ref, radial_y_ref), scratch,
    )
    width = len(sums) * channels
    for place, total in enumerate(sums):
        cols = slice(place * channels, (place + 1) * channels)
        own_ref[:, cols] = (joined[:both, cols] + 0.18 * total).astype(BF16)
    for side, hot in enumerate((lent_ref, lent_y_ref)):
        lent = lent_rows(hot[...], own_ref[side * atoms : (side + 1) * atoms, :width])
        pair_ref[side * ghosts : (side + 1) * ghosts, :width] = lent[:ghosts]
        other_ref[side * ghosts : (side + 1) * ghosts, :width] = lent[ghosts:]
    if last:
        part = pulls_ref.shape[1]
        block = 2 * atoms + 4 * ghosts
        for slot in range(pulls_ref.shape[0] // block):
            cols = slice(width + slot // 2 * part, width + (slot // 2 + 1) * part)
            at = slot * block
            for ref, size in ((own_ref, atoms), (pair_ref, ghosts), (other_ref, ghosts)):
                to = slot % 2 * size
                ref[to : to + size, cols] = pulls_ref[at : at + size]
                at += 2 * size
    for copy in copies:
        copy.wait()


def last_kernel(
    layer, degrees, channels, atoms, per_atom, count,
    rest_ref, lent_ref, hot_ref, radial_ref, dirs_ref, readout_ref, *refs,
):
    tables, weights = refs[:count], refs[count : count + 5]
    out_ref, force_ref = refs[count + 5 : count + 7]
    scratch = refs[count + 7 :]
    joined = scratch[0]
    sums, first, zero = layer_sums(
        layer, degrees, channels, atoms, per_atom, tables, weights, (hot_ref,), (radial_ref,), scratch
    )
    order = slot_order(degrees)
    for place, slot in enumerate(order):
        cols = slice(place * channels, (place + 1) * channels)
        out_ref[slot] = (joined[:atoms, cols] + 0.18 * sums[place]).astype(BF16)
    for place, slot in enumerate(unused_slots(degrees * degrees)):
        out_ref[slot] = rest_ref[place]

    width = len(sums) * channels
    part = 3 * channels
    ghosts = lent_ref.shape[1] // 2
    own, lent = 0.0, []
    for slot in range(count // 3):
        cols = slice(width + slot // 2 * part, width + (slot // 2 + 1) * part)
        own_rows, *lent_blocks = (
            tables[3 * slot + kind][slot % 2 * size : (slot % 2 + 1) * size, cols].astype(F32)
            for kind, size in enumerate((atoms, ghosts, ghosts))
        )
        own += own_rows
        lent += lent_blocks
    hot = jnp.concatenate([lent_ref[...]] * (count // 3), axis=1).astype(BF16)
    pulls = own + dot(hot, jnp.concatenate(lent, axis=0).astype(BF16))
    readout = readout_ref[...]
    parts = []
    for axis in range(3):
        pull = (first * dirs_ref[axis]).reshape(atoms, per_atom, channels).sum(axis=1)
        back = zero[:atoms, :channels] * pulls[:, axis * channels : (axis + 1) * channels]
        parts.append((pull - back) * readout)
    ones = jnp.ones((8, channels), F32)
    total = dot(ones, jnp.concatenate(parts, axis=0), ((1,), (1,)), HIGHEST)
    for axis in range(3):
        force_ref[axis : axis + 1, :] = total[:1, axis * atoms : (axis + 1) * atoms]


def across(block, bit, slab_devices):
    return lax.ppermute(block, "yz", [(q, q ^ bit) for q in range(slab_devices)])


def toward(block, step, slabs):
    route = []
    for slab in range(slabs):
        to = slab + 1 if (slab % 2 == 0) == (step > 0) else slab - 1
        route.append((slab, to % slabs))
    return lax.ppermute(block, "slab", route)


def spread(held, bits, slab_devices):
    for bit in bits:
        for slot in sorted(held):
            held[slot | bit] = tuple(across(block, bit, slab_devices) for block in held[slot])
    return held


def order_bits(slab_devices):
    bits, bit = [], slab_devices // 2
    while bit:
        bits.append(bit)
        bit //= 2
    return bits


def body(
    embeddings, neighbours, valid, azimuth, polar, distance, send_low, send_high,
    w_zero, w_one_re, w_one_im, w_two_re, w_two_im, radial_weight, readout,
):
    atoms, coeffs, channels = embeddings.shape
    degrees = math.isqrt(coeffs)
    ghosts = send_low.shape[0]
    edges = neighbours.shape[0]
    layers = w_zero.shape[0]
    slabs, slab_devices = lax.axis_size("slab"), lax.axis_size("yz")
    rows = slab_devices * (atoms + 2 * ghosts)
    width = len(slot_order(degrees)) * channels
    low, high = send_low.reshape(1, -1), send_high.reshape(1, -1)
    held, shape = pltpu.VMEM, jax.ShapeDtypeStruct
    embeddings = embeddings.transpose(1, 0, 2)
    params = pltpu.CompilerParams(vmem_limit_bytes=24 * 2**20)
    row = lambda value: value.reshape(1, -1)
    far = pl.BlockSpec(memory_space=pl.ANY)

    half = slab_devices // 2
    own, pair, other, rest, radial_weight, vector = pl.pallas_call(
        pack_kernel,
        out_shape=[
            held((atoms, width + edges), BF16), held((ghosts, width), BF16),
            held((ghosts, width), BF16), held((len(unused_slots(coeffs)), atoms, channels), BF16),
            held(radial_weight.shape, F32), held((1, channels), F32),
        ],
        in_specs=[VMEM] * 10,
        out_specs=[VMEM] * 6,
        compiler_params=params,
        name="pack",
    )(*away(
        embeddings, low, high, *map(row, (neighbours, valid, distance, azimuth, polar)),
        radial_weight, row(readout),
    ))

    got_other = toward(other, -1, slabs)
    got_pair = toward(pair, 1, slabs)
    got_own = across(own, half, slab_devices)
    weights = (w_zero, w_one_re, w_one_im, w_two_re, w_two_im)
    count = len(weights)
    near_weights = [held(array.shape[1:], array.dtype) for array in weights]
    side_shapes = [
        held((edges, 2 * rows), BF16), held((layers, edges, channels), F32),
        held((rows, edges), F32), held((atoms, 2 * ghosts), F32),
    ]
    hot, radial, flags, lent = pl.pallas_call(
        functools.partial(scale_kernel, atoms, ghosts, slab_devices, 0),
        out_shape=side_shapes,
        in_specs=[VMEM] * 2,
        out_specs=[VMEM] * 4,
        compiler_params=params,
        name="scales",
    )(*near(own, radial_weight))
    got_pair, flags = lax.optimization_barrier((got_pair, flags))
    pair_y = across(got_pair, half, slab_devices)
    other_y = across(got_other, half, slab_devices)
    hot_y, radial_y, flags_y, lent_y, *now = pl.pallas_call(
        functools.partial(scale_kernel, atoms, ghosts, slab_devices, count),
        out_shape=[*side_shapes, *near_weights],
        in_specs=[VMEM] * 2 + [far] * count,
        out_specs=[VMEM] * (4 + count),
        scratch_shapes=[pltpu.SemaphoreType.DMA((count,))],
        compiler_params=params,
        name="scales_y",
    )(*near(got_own, radial_weight), *away(*weights))
    dirs, pulls = pl.pallas_call(
        pull_kernel,
        out_shape=[held((3, edges, channels), F32), held((rows, 3 * channels), BF16)],
        in_specs=[VMEM] * 6,
        out_specs=[VMEM] * 2,
        compiler_params=params,
        name="pulls",
    )(*near(own, radial, flags, got_own, radial_y, flags_y))

    bits = order_bits(slab_devices)
    blocks = {0: (own, got_pair, got_other)}
    blocks[half] = (got_own, pair_y, other_y)
    blocks = spread(blocks, bits[1:], slab_devices)
    tables = [
        blocks[slot + upper][kind]
        for slot in range(half) for kind in range(3) for upper in (0, half)
    ]
    scratch = [pltpu.VMEM((rows, width), F32), pltpu.VMEM((2 * rows, width), BF16)]
    per_atom = edges // atoms
    for layer in range(layers):
        if layer < layers - 1:
            last = layer == layers - 2
            wide = width + ((half + 1) // 2 * 3 * channels if last else 0)
            own, pair, other, *now = pl.pallas_call(
                functools.partial(first_kernel, layer, last, degrees, channels, per_atom, len(tables)),
                out_shape=[
                    held((2 * atoms, wide), BF16), held((2 * ghosts, wide), BF16),
                    held((2 * ghosts, wide), BF16), *near_weights,
                ],
                in_specs=[VMEM] * (7 + len(tables) + count) + [far] * count,
                out_specs=[VMEM] * (3 + count),
                scratch_shapes=[*scratch, pltpu.SemaphoreType.DMA((count,))],
                compiler_params=params,
                name="layer",
            )(*near(lent, hot, radial, lent_y, hot_y, radial_y, pulls, *tables, *now), *away(*weights))
            got_other = toward(other, -1, slabs)
            got_pair = toward(pair, 1, slabs)
            blocks = spread({0: (own, got_pair, got_other)}, bits[1:], slab_devices)
            tables = [block for slot in range(half) for block in blocks[slot]]
        else:
            updated, forces = pl.pallas_call(
                functools.partial(
                    last_kernel, layer, degrees, channels, atoms, per_atom, len(tables)
                ),
                out_shape=[shape((coeffs, atoms, channels), BF16), shape((3, atoms), F32)],
                in_specs=[VMEM] * (6 + len(tables) + count),
                out_specs=[VMEM] * 2,
                scratch_shapes=scratch,
                compiler_params=params,
                name="last_layer",
            )(*near(rest, lent, hot, radial, dirs, vector, *tables, *now))
    return (updated.transpose(1, 0, 2), forces)


def solution(mesh):
    both = ("slab", "yz")
    in_specs = (P(both, None, None), *([P(both)] * 7), *([P()] * 7))
    out_specs = (P(both, None, None), P(None, both))
    return jax.shard_map(body, mesh=mesh, in_specs=in_specs, out_specs=out_specs, check_vma=False)
```

```python
import functools
import math

import jax
import jax.numpy as jnp
from jax import lax
from jax.experimental import pallas as pl
from jax.experimental.pallas import tpu as pltpu
from jax.sharding import PartitionSpec as P


HIGHEST = lax.Precision.HIGHEST
BF16 = jnp.bfloat16
F32 = jnp.float32
ORDERS = (1, 2)
DIGIT = 128
VMEM = pl.BlockSpec(memory_space=pltpu.VMEM)


def near(*arrays):
    return [pltpu.with_memory_space_constraint(array, pltpu.VMEM) for array in arrays]


def away(*arrays):
    return [pltpu.with_memory_space_constraint(array, pltpu.HBM) for array in arrays]


def slot_index(degree, azimuth_order):
    return degree * degree + degree + azimuth_order


def slot_groups(degrees):
    groups = [[slot_index(degree, 0) for degree in range(degrees)]]
    for order in ORDERS:
        groups.append([slot_index(degree, order) for degree in range(order, degrees)])
        groups.append([slot_index(degree, -order) for degree in range(order, degrees)])
    return groups


def slot_order(degrees):
    return [slot for group in slot_groups(degrees) for slot in group]


def unused_slots(coeffs):
    order = slot_order(math.isqrt(coeffs))
    return [slot for slot in range(coeffs) if slot not in order]


def odd_slab():
    return lax.axis_index("slab") % 2 == 1


def dot(left, right, contract=((1,), (0,)), precision=None):
    return lax.dot_general(
        left, right, (contract, ((), ())), precision=precision, preferred_element_type=F32
    )


def lent_picks(low_ref, high_ref):
    odd = odd_slab()
    low, high = low_ref[...], high_ref[...]
    return jnp.concatenate([jnp.where(odd, low, high), jnp.where(odd, high, low)], axis=1)


def lent_hot(picks, atoms):
    rows = lax.broadcasted_iota(jnp.int32, (atoms, picks.shape[1]), 0)
    return (rows == picks).astype(F32)


def lent_rows(hot, rows):
    return dot(hot.astype(BF16), rows, ((0,), (0,))).astype(BF16)


def thirds(value):
    parts = []
    for _ in range(3):
        part = value.astype(BF16).astype(F32)
        parts.append(part)
        value = value - part
    return parts


def pack_kernel(
    emb_ref, low_ref, high_ref, nbr_ref, valid_ref, dist_ref, azi_ref, pol_ref, rw_ref, readout_ref,
    own_ref, pair_ref, other_ref, rest_ref, scales_ref, vector_ref,
):
    coeffs, atoms, channels = emb_ref.shape
    ghosts = low_ref.shape[1]
    edges = nbr_ref.shape[1]
    order = slot_order(math.isqrt(coeffs))
    width = len(order) * channels
    for place, slot in enumerate(order):
        own_ref[:, place * channels : (place + 1) * channels] = emb_ref[slot]
    for place, slot in enumerate(unused_slots(coeffs)):
        rest_ref[place] = emb_ref[slot]
    picks = lent_picks(low_ref, high_ref)
    lent = lent_rows(lent_hot(picks, atoms), own_ref[:, :width])
    pair_ref[...] = lent[:ghosts]
    other_ref[...] = lent[ghosts:]
    nbr = nbr_ref[...]
    picks = jnp.concatenate(
        [picks, jnp.zeros((1, edges - 2 * ghosts), jnp.int32)], axis=1
    ).astype(F32)
    facts = [
        (nbr // DIGIT).astype(F32), (nbr % DIGIT).astype(F32), valid_ref[...].astype(F32), picks,
        *thirds(dist_ref[...]), *thirds(azi_ref[...]), *thirds(pol_ref[...]),
    ]
    facts.append(jnp.zeros((atoms - len(facts), edges), F32))
    own_ref[:, width:] = jnp.concatenate(facts, axis=0).astype(BF16)
    scales_ref[...] = rw_ref[...]
    vector_ref[...] = 0.125 * readout_ref[...]


def edge_facts(ref, edges):
    rows = ref[:, ref.shape[1] - edges :].astype(F32)
    row = lambda at: rows[at : at + 1]
    whole = lambda at: row(at) + row(at + 1) + row(at + 2)
    nbr = (row(0) * DIGIT + row(1)).astype(jnp.int32)
    return nbr, row(2), row(3).astype(jnp.int32), whole(4), whole(7), whole(10)


def start_fetch(refs, layer):
    count = len(refs) // 2
    copies = [
        pltpu.make_async_copy(refs[i].at[layer], refs[count + i], refs[-1].at[i])
        for i in range(count)
    ]
    for copy in copies:
        copy.start()
    return copies


def edge_scales(
    atoms, ghosts, slab_devices, facts_ref, rw_ref, hot_ref, radial_ref, flags_ref, lent_ref
):
    layers, centers = rw_ref.shape[0], rw_ref.shape[1]
    own_count, ghost_count = slab_devices * atoms, slab_devices * ghosts
    half = slab_devices // 2
    me = lax.axis_index("yz")
    odd = odd_slab()
    edges = hot_ref.shape[0]
    nbr, valid, picks, distance, _, _ = edge_facts(facts_ref, edges)
    is_own = nbr < own_count
    ghost = nbr - own_count
    below = ghost < ghost_count
    ghost = jnp.where(below, ghost, ghost - ghost_count)
    paired = jnp.where(odd, below.astype(jnp.int32), 1 - below.astype(jnp.int32))
    slot = jnp.where(is_own, nbr // atoms, ghost // ghosts) ^ me
    upper = slot // half
    inner = jnp.where(
        is_own,
        upper * atoms + nbr % atoms,
        2 * atoms + (1 - paired) * (2 * ghosts) + upper * ghosts + ghost % ghosts,
    )
    place = (slot % half) * (2 * atoms + 4 * ghosts) + inner
    rows = lax.broadcasted_iota(jnp.int32, (flags_ref.shape[0], edges), 0)
    hot = jnp.where((rows == place) & (valid != 0.0), 1.0, 0.0).astype(F32)
    flags_ref[...] = hot
    hot_cols = jnp.transpose(hot).astype(BF16)
    hot_ref[...] = jnp.concatenate([hot_cols, hot_cols], axis=1)
    middle = 1.0 + 0.5 * lax.broadcasted_iota(jnp.int32, (centers, edges), 0).astype(F32)
    basis = jnp.exp(-jnp.square((distance - middle) / 0.5))
    for layer in range(layers):
        scale = dot(basis, rw_ref[layer], ((0,), (0,)), HIGHEST)
        radial_ref[layer] = scale / (1.0 + jnp.exp(-scale))
    lent_ref[...] = lent_hot(picks[:, : 2 * ghosts], atoms)


def scale_kernel(atoms, ghosts, slab_devices, count, fetched, facts_ref, rw_ref, *refs):
    far, refs = refs[:count], refs[count:]
    copies = []
    for i, layer in enumerate(fetched):
        near_refs = refs[4 + count * i : 4 + count * (i + 1)]
        copies += start_fetch((*far, *near_refs, refs[-1].at[i]), layer)
    edge_scales(atoms, ghosts, slab_devices, facts_ref, rw_ref, *refs[:4])
    for copy in copies:
        copy.wait()


def pull_kernel(
    facts_ref, radial_ref, flags_ref, partner_ref, radial_y_ref, flags_y_ref, dirs_ref, pulls_ref
):
    edges, channels = radial_ref.shape[1:]
    last = radial_ref.shape[0] - 1
    rows = flags_ref.shape[0]
    totals = [0.0, 0.0, 0.0]
    for ref, scale_ref, hot_ref in (
        (facts_ref, radial_ref, flags_ref), (partner_ref, radial_y_ref, flags_y_ref)
    ):
        _, _, _, _, azimuth, polar = edge_facts(ref, edges)
        sin_polar = jnp.sin(polar)
        dirs = [sin_polar * jnp.cos(azimuth), sin_polar * jnp.sin(azimuth), jnp.cos(polar)]
        if ref is facts_ref:
            columns = jnp.transpose(jnp.concatenate([*dirs, *dirs, *dirs[:2]], axis=0))
            for axis in range(3):
                dirs_ref[axis] = jnp.broadcast_to(columns[:, axis : axis + 1], (edges, channels))
        radial = scale_ref[last]
        high = radial.astype(BF16)
        both = jnp.concatenate([high, (radial - high.astype(F32)).astype(BF16)], axis=1)
        for axis in range(3):
            along = hot_ref[...] * dirs[axis]
            high = along.astype(BF16)
            low = (along - high.astype(F32)).astype(BF16)
            got = dot(jnp.concatenate([high, low], axis=0), both)
            totals[axis] += (
                got[:rows, :channels] + got[:rows, channels:] + got[rows:, :channels]
            )
    pulls_ref[...] = jnp.concatenate(totals, axis=1).astype(BF16)


def layer_sums(layer, degrees, channels, atoms, per_atom, tables, weights, hots, radials, scratch):
    joined, mixed = scratch
    groups = slot_groups(degrees)
    w_zero, w_one_re, w_one_im, w_two_re, w_two_im = (ref[...] for ref in weights)
    width = joined.shape[1]
    start = 0
    for ref in tables:
        count = ref.shape[0]
        joined[start : start + count] = ref[:, :width].astype(F32)
        start += count
    rows = start

    def put(column, value):
        high = value.astype(BF16)
        low = (value - high.astype(F32)).astype(BF16)
        mixed[:rows, column : column + value.shape[1]] = high
        mixed[rows:, column : column + value.shape[1]] = low

    span = len(groups[0]) * channels
    zero = dot(joined[:, :span].astype(BF16), w_zero)
    put(0, zero)
    column = span
    for index, (real, imag) in enumerate(((w_one_re, w_one_im), (w_two_re, w_two_im))):
        span = len(groups[2 * index + 1]) * channels
        both = jnp.concatenate(
            [joined[:, column : column + span], joined[:, column + span : column + 2 * span]], axis=0
        ).astype(BF16)
        by_real = dot(both, real)
        by_imag = dot(both, imag)
        put(column, by_real[:rows] - by_imag[rows:])
        put(column + span, by_imag[:rows] + by_real[rows:])
        column += 2 * span
    part = atoms // len(hots)
    sums = []
    first = None
    step = 2 * channels
    for begin in range(0, width, step):
        end = min(begin + step, width)
        pieces = []
        for hot_ref, radial_ref in zip(hots, radials):
            got = dot(hot_ref[...], mixed[:, begin:end])
            for inner in range(0, end - begin, channels):
                message = got[:, inner : inner + channels] * radial_ref[layer]
                if first is None:
                    first = message
                pieces.append(message.reshape(part, per_atom, channels).sum(axis=1))
        count = (end - begin) // channels
        for inner in range(count):
            sums.append(jnp.concatenate(pieces[inner::count], axis=0))
    return sums, first, zero


def first_kernel(
    layer, last, degrees, channels, per_atom, count,
    lent_ref, hot_ref, radial_ref, lent_y_ref, hot_y_ref, radial_y_ref, pulls_ref, *refs,
):
    tables, weights = refs[:count], refs[count : count + 5]
    own_ref, pair_ref, other_ref = refs[count + 5 : count + 8]
    scratch = refs[count + 8 :]
    joined = scratch[0]
    both = own_ref.shape[0]
    atoms, ghosts = both // 2, lent_ref.shape[1] // 2
    sums, _, _ = layer_sums(
        layer, degrees, channels, both, per_atom, tables, weights,
        (hot_ref, hot_y_ref), (radial_ref, radial_y_ref), scratch,
    )
    width = len(sums) * channels
    for place, total in enumerate(sums):
        cols = slice(place * channels, (place + 1) * channels)
        own_ref[:, cols] = (joined[:both, cols] + 0.18 * total).astype(BF16)
    for side, hot in enumerate((lent_ref, lent_y_ref)):
        lent = lent_rows(hot[...], own_ref[side * atoms : (side + 1) * atoms, :width])
        pair_ref[side * ghosts : (side + 1) * ghosts, :width] = lent[:ghosts]
        other_ref[side * ghosts : (side + 1) * ghosts, :width] = lent[ghosts:]
    if last:
        part = pulls_ref.shape[1]
        block = 2 * atoms + 4 * ghosts
        for slot in range(pulls_ref.shape[0] // block):
            cols = slice(width + slot // 2 * part, width + (slot // 2 + 1) * part)
            at = slot * block
            for ref, size in ((own_ref, atoms), (pair_ref, ghosts), (other_ref, ghosts)):
                to = slot % 2 * size
                ref[to : to + size, cols] = pulls_ref[at : at + size]
                at += 2 * size


def last_kernel(
    layer, degrees, channels, atoms, per_atom, count,
    rest_ref, lent_ref, hot_ref, radial_ref, dirs_ref, readout_ref, *refs,
):
    tables, weights = refs[:count], refs[count : count + 5]
    out_ref, force_ref = refs[count + 5 : count + 7]
    scratch = refs[count + 7 :]
    joined = scratch[0]
    sums, first, zero = layer_sums(
        layer, degrees, channels, atoms, per_atom, tables, weights, (hot_ref,), (radial_ref,), scratch
    )
    order = slot_order(degrees)
    for place, slot in enumerate(order):
        cols = slice(place * channels, (place + 1) * channels)
        out_ref[slot] = (joined[:atoms, cols] + 0.18 * sums[place]).astype(BF16)
    for place, slot in enumerate(unused_slots(degrees * degrees)):
        out_ref[slot] = rest_ref[place]

    width = len(sums) * channels
    part = 3 * channels
    ghosts = lent_ref.shape[1] // 2
    own, lent = 0.0, []
    for slot in range(count // 3):
        cols = slice(width + slot // 2 * part, width + (slot // 2 + 1) * part)
        own_rows, *lent_blocks = (
            tables[3 * slot + kind][slot % 2 * size : (slot % 2 + 1) * size, cols].astype(F32)
            for kind, size in enumerate((atoms, ghosts, ghosts))
        )
        own += own_rows
        lent += lent_blocks
    hot = jnp.concatenate([lent_ref[...]] * (count // 3), axis=1).astype(BF16)
    pulls = own + dot(hot, jnp.concatenate(lent, axis=0).astype(BF16))
    readout = readout_ref[...]
    parts = []
    for axis in range(3):
        pull = (first * dirs_ref[axis]).reshape(atoms, per_atom, channels).sum(axis=1)
        back = zero[:atoms, :channels] * pulls[:, axis * channels : (axis + 1) * channels]
        parts.append((pull - back) * readout)
    ones = jnp.ones((8, channels), F32)
    total = dot(ones, jnp.concatenate(parts, axis=0), ((1,), (1,)), HIGHEST)
    for axis in range(3):
        force_ref[axis : axis + 1, :] = total[:1, axis * atoms : (axis + 1) * atoms]


def across(block, bit, slab_devices):
    return lax.ppermute(block, "yz", [(q, q ^ bit) for q in range(slab_devices)])


def toward(block, step, slabs):
    route = []
    for slab in range(slabs):
        to = slab + 1 if (slab % 2 == 0) == (step > 0) else slab - 1
        route.append((slab, to % slabs))
    return lax.ppermute(block, "slab", route)


def spread(held, bits, slab_devices):
    for bit in bits:
        for slot in sorted(held):
            got = []
            for block in held[slot]:
                got.append(across(block, bit, slab_devices))
            held[slot | bit] = tuple(got)
    return held


def order_bits(slab_devices):
    bits, bit = [], slab_devices // 2
    while bit:
        bits.append(bit)
        bit //= 2
    return bits


def body(
    embeddings, neighbours, valid, azimuth, polar, distance, send_low, send_high,
    w_zero, w_one_re, w_one_im, w_two_re, w_two_im, radial_weight, readout,
):
    atoms, coeffs, channels = embeddings.shape
    degrees = math.isqrt(coeffs)
    ghosts = send_low.shape[0]
    edges = neighbours.shape[0]
    layers = w_zero.shape[0]
    slabs, slab_devices = lax.axis_size("slab"), lax.axis_size("yz")
    rows = slab_devices * (atoms + 2 * ghosts)
    width = len(slot_order(degrees)) * channels
    low, high = send_low.reshape(1, -1), send_high.reshape(1, -1)
    held, shape = pltpu.VMEM, jax.ShapeDtypeStruct
    embeddings = embeddings.transpose(1, 0, 2)
    params = pltpu.CompilerParams(vmem_limit_bytes=24 * 2**20)
    row = lambda value: value.reshape(1, -1)
    far = pl.BlockSpec(memory_space=pl.ANY)

    half = slab_devices // 2
    own, pair, other, rest, radial_weight, vector = pl.pallas_call(
        pack_kernel,
        out_shape=[
            held((atoms, width + edges), BF16), held((ghosts, width), BF16),
            held((ghosts, width), BF16), held((len(unused_slots(coeffs)), atoms, channels), BF16),
            held(radial_weight.shape, F32), held((1, channels), F32),
        ],
        in_specs=[VMEM] * 10,
        out_specs=[VMEM] * 6,
        compiler_params=params,
        name="pack",
    )(*away(
        embeddings, low, high, *map(row, (neighbours, valid, distance, azimuth, polar)),
        radial_weight, row(readout),
    ))

    got_other = toward(other, -1, slabs)
    got_pair = toward(pair, 1, slabs)
    got_own = across(own, half, slab_devices)
    weights = (w_zero, w_one_re, w_one_im, w_two_re, w_two_im)
    count = len(weights)
    near_weights = [held(array.shape[1:], array.dtype) for array in weights]
    side_shapes = [
        held((edges, 2 * rows), BF16), held((layers, edges, channels), F32),
        held((rows, edges), F32), held((atoms, 2 * ghosts), F32),
    ]

    def scales(facts, fetched):
        return pl.pallas_call(
            functools.partial(scale_kernel, atoms, ghosts, slab_devices, count, fetched),
            out_shape=[*side_shapes, *(near_weights * len(fetched))],
            in_specs=[VMEM] * 2 + [far] * count,
            out_specs=[VMEM] * (4 + count * len(fetched)),
            scratch_shapes=[pltpu.SemaphoreType.DMA((len(fetched), count))],
            compiler_params=params,
        )(*near(facts, radial_weight), *away(*weights))

    hot, radial, flags, lent, *first_weights = scales(own, (0,))
    got_pair, flags = lax.optimization_barrier((got_pair, flags))
    pair_y = across(got_pair, half, slab_devices)
    other_y = across(got_other, half, slab_devices)
    hot_y, radial_y, flags_y, lent_y, *later_weights = scales(got_own, tuple(range(1, layers)))
    dirs, pulls = pl.pallas_call(
        pull_kernel,
        out_shape=[held((3, edges, channels), F32), held((rows, 3 * channels), BF16)],
        in_specs=[VMEM] * 6,
        out_specs=[VMEM] * 2,
        compiler_params=params,
        name="pulls",
    )(*near(own, radial, flags, got_own, radial_y, flags_y))

    bits = order_bits(slab_devices)
    blocks = {0: (own, got_pair, got_other)}
    blocks[half] = (got_own, pair_y, other_y)
    blocks = spread(blocks, bits[1:], slab_devices)
    tables = [
        blocks[slot + upper][kind]
        for slot in range(half) for kind in range(3) for upper in (0, half)
    ]
    scratch = [pltpu.VMEM((rows, width), F32), pltpu.VMEM((2 * rows, width), BF16)]
    per_atom = edges // atoms
    weights = (*first_weights, *later_weights)
    for layer in range(layers):
        now = weights[layer * count : (layer + 1) * count]
        if layer < layers - 1:
            last = layer == layers - 2
            wide = width + ((half + 1) // 2 * 3 * channels if last else 0)
            own, pair, other = pl.pallas_call(
                functools.partial(first_kernel, layer, last, degrees, channels, per_atom, len(tables)),
                out_shape=[
                    held((2 * atoms, wide), BF16), held((2 * ghosts, wide), BF16),
                    held((2 * ghosts, wide), BF16),
                ],
                in_specs=[VMEM] * (7 + len(tables) + count),
                out_specs=[VMEM] * 3,
                scratch_shapes=scratch,
                compiler_params=params,
                name="layer",
            )(*near(lent, hot, radial, lent_y, hot_y, radial_y, pulls, *tables, *now))
            got_other = toward(other, -1, slabs)
            got_pair = toward(pair, 1, slabs)
            blocks = spread({0: (own, got_pair, got_other)}, bits[1:], slab_devices)
            tables = [block for slot in range(half) for block in blocks[slot]]
        else:
            updated, forces = pl.pallas_call(
                functools.partial(
                    last_kernel, layer, degrees, channels, atoms, per_atom, len(tables)
                ),
                out_shape=[shape((coeffs, atoms, channels), BF16), shape((3, atoms), F32)],
                in_specs=[VMEM] * (6 + len(tables) + count),
                out_specs=[VMEM] * 2,
                scratch_shapes=scratch,
                compiler_params=params,
                name="last_layer",
            )(*near(rest, lent, hot, radial, dirs, vector, *tables, *now))
    return (updated.transpose(1, 0, 2), forces)


def solution(mesh):
    both = ("slab", "yz")
    in_specs = (P(both, None, None), *([P(both)] * 7), *([P()] * 7))
    out_specs = (P(both, None, None), P(None, both))
    return jax.shard_map(body, mesh=mesh, in_specs=in_specs, out_specs=out_specs, check_vma=False)
```

```python
import functools
import math

import jax
import jax.numpy as jnp
from jax import lax
from jax.experimental import pallas as pl
from jax.experimental.pallas import tpu as pltpu
from jax.sharding import PartitionSpec as P


HIGHEST = lax.Precision.HIGHEST
BF16 = jnp.bfloat16
F32 = jnp.float32
ORDERS = (1, 2)
DIGIT = 128
VMEM = pl.BlockSpec(memory_space=pltpu.VMEM)


def near(*arrays):
    return [pltpu.with_memory_space_constraint(array, pltpu.VMEM) for array in arrays]


def away(*arrays):
    return [pltpu.with_memory_space_constraint(array, pltpu.HBM) for array in arrays]


def slot_index(degree, azimuth_order):
    return degree * degree + degree + azimuth_order


def slot_groups(degrees):
    groups = [[slot_index(degree, 0) for degree in range(degrees)]]
    for order in ORDERS:
        groups.append([slot_index(degree, order) for degree in range(order, degrees)])
        groups.append([slot_index(degree, -order) for degree in range(order, degrees)])
    return groups


def slot_order(degrees):
    return [slot for group in slot_groups(degrees) for slot in group]


def unused_slots(coeffs):
    order = slot_order(math.isqrt(coeffs))
    return [slot for slot in range(coeffs) if slot not in order]


def odd_slab():
    return lax.axis_index("slab") % 2 == 1


def dot(left, right, contract=((1,), (0,)), precision=None):
    return lax.dot_general(
        left, right, (contract, ((), ())), precision=precision, preferred_element_type=F32
    )


def lent_picks(low_ref, high_ref):
    odd = odd_slab()
    low, high = low_ref[...], high_ref[...]
    return jnp.concatenate([jnp.where(odd, low, high), jnp.where(odd, high, low)], axis=1)


def lent_hot(picks, atoms):
    rows = lax.broadcasted_iota(jnp.int32, (atoms, picks.shape[1]), 0)
    return (rows == picks).astype(F32)


def lent_rows(hot, rows):
    return dot(hot.astype(BF16), rows, ((0,), (0,))).astype(BF16)


def thirds(value):
    parts = []
    for _ in range(3):
        part = value.astype(BF16).astype(F32)
        parts.append(part)
        value = value - part
    return parts


def pack_kernel(
    emb_ref, low_ref, high_ref, nbr_ref, valid_ref, dist_ref, azi_ref, pol_ref, rw_ref, readout_ref,
    own_ref, pair_ref, other_ref, rest_ref, scales_ref, vector_ref,
):
    coeffs, atoms, channels = emb_ref.shape
    ghosts = low_ref.shape[1]
    edges = nbr_ref.shape[1]
    order = slot_order(math.isqrt(coeffs))
    width = len(order) * channels
    for place, slot in enumerate(order):
        own_ref[:, place * channels : (place + 1) * channels] = emb_ref[slot]
    for place, slot in enumerate(unused_slots(coeffs)):
        rest_ref[place] = emb_ref[slot]
    picks = lent_picks(low_ref, high_ref)
    lent = lent_rows(lent_hot(picks, atoms), own_ref[:, :width])
    pair_ref[...] = lent[:ghosts]
    other_ref[...] = lent[ghosts:]
    nbr = nbr_ref[...]
    picks = jnp.concatenate(
        [picks, jnp.zeros((1, edges - 2 * ghosts), jnp.int32)], axis=1
    ).astype(F32)
    facts = [
        (nbr // DIGIT).astype(F32), (nbr % DIGIT).astype(F32), valid_ref[...].astype(F32), picks,
        *thirds(dist_ref[...]), *thirds(azi_ref[...]), *thirds(pol_ref[...]),
    ]
    facts.append(jnp.zeros((atoms - len(facts), edges), F32))
    own_ref[:, width:] = jnp.concatenate(facts, axis=0).astype(BF16)
    scales_ref[...] = rw_ref[...]
    vector_ref[...] = 0.125 * readout_ref[...]


def edge_facts(ref, edges):
    rows = ref[:, ref.shape[1] - edges :].astype(F32)
    row = lambda at: rows[at : at + 1]
    whole = lambda at: row(at) + row(at + 1) + row(at + 2)
    nbr = (row(0) * DIGIT + row(1)).astype(jnp.int32)
    return nbr, row(2), row(3).astype(jnp.int32), whole(4), whole(7), whole(10)


def start_fetch(far, near_refs, sems, plan):
    copies = [
        pltpu.make_async_copy(far[which].at[layer], near_refs[i], sems.at[i])
        for i, (layer, which) in enumerate(plan)
    ]
    for copy in copies:
        copy.start()
    return copies


def edge_scales(
    atoms, ghosts, slab_devices, facts_ref, rw_ref, hot_ref, radial_ref, lent_ref
):
    layers, centers = rw_ref.shape[0], rw_ref.shape[1]
    own_count, ghost_count = slab_devices * atoms, slab_devices * ghosts
    half = slab_devices // 2
    me = lax.axis_index("yz")
    odd = odd_slab()
    edges = hot_ref.shape[0]
    count = hot_ref.shape[1] // 2
    nbr, valid, picks, distance, azimuth, polar = edge_facts(facts_ref, edges)
    is_own = nbr < own_count
    ghost = nbr - own_count
    below = ghost < ghost_count
    ghost = jnp.where(below, ghost, ghost - ghost_count)
    paired = jnp.where(odd, below.astype(jnp.int32), 1 - below.astype(jnp.int32))
    slot = jnp.where(is_own, nbr // atoms, ghost // ghosts) ^ me
    upper = slot // half
    inner = jnp.where(
        is_own,
        upper * atoms + nbr % atoms,
        2 * atoms + upper * (2 * ghosts) + (1 - paired) * ghosts + ghost % ghosts,
    )
    place = (slot % half) * (2 * atoms + 4 * ghosts) + inner
    rows = lax.broadcasted_iota(jnp.int32, (count, edges), 0)
    hot = jnp.where((rows == place) & (valid != 0.0), 1.0, 0.0).astype(F32)
    hot_cols = jnp.transpose(hot).astype(BF16)
    hot_ref[...] = jnp.concatenate([hot_cols, hot_cols], axis=1)
    middle = 1.0 + 0.5 * lax.broadcasted_iota(jnp.int32, (centers, edges), 0).astype(F32)
    basis = jnp.exp(-jnp.square((distance - middle) / 0.5))
    for layer in range(layers):
        scale = dot(basis, rw_ref[layer], ((0,), (0,)), HIGHEST)
        radial = scale / (1.0 + jnp.exp(-scale))
        radial_ref[layer] = radial
    lent_ref[...] = lent_hot(picks[:, : 2 * ghosts], atoms)
    sin_polar = jnp.sin(polar)
    dirs = [sin_polar * jnp.cos(azimuth), sin_polar * jnp.sin(azimuth), jnp.cos(polar)]
    channels = radial.shape[1]
    high = radial.astype(BF16)
    both = jnp.concatenate([high, (radial - high.astype(F32)).astype(BF16)], axis=1)
    pulls = []
    for axis in range(3):
        along = hot * dirs[axis]
        high = along.astype(BF16)
        low = (along - high.astype(F32)).astype(BF16)
        got = dot(jnp.concatenate([high, low], axis=0), both)
        pulls.append(got[:count, :channels] + got[:count, channels:] + got[count:, :channels])
    return dirs, pulls


def own_scale_kernel(atoms, ghosts, slab_devices, count, plan, facts_ref, rw_ref, *refs):
    far, (hot_ref, radial_ref, lent_ref, dirs_ref, part_ref), refs = (
        refs[:count], refs[count : count + 5], refs[count + 5 :]
    )
    copies = start_fetch(far, refs[:-1], refs[-1], plan)
    dirs, pulls = edge_scales(
        atoms, ghosts, slab_devices, facts_ref, rw_ref, hot_ref, radial_ref, lent_ref
    )
    columns = jnp.transpose(jnp.concatenate([*dirs, *dirs, *dirs[:2]], axis=0))
    for axis in range(3):
        dirs_ref[axis] = jnp.broadcast_to(columns[:, axis : axis + 1], dirs_ref.shape[1:])
    part_ref[...] = jnp.concatenate(pulls, axis=1)
    for copy in copies:
        copy.wait()


def partner_scale_kernel(
    atoms, ghosts, slab_devices, count, plan, facts_ref, rw_ref, part_ref, *refs
):
    far, (hot_ref, radial_ref, lent_ref, pulls_ref), refs = (
        refs[:count], refs[count : count + 4], refs[count + 4 :]
    )
    copies = start_fetch(far, refs[:-1], refs[-1], plan)
    _, pulls = edge_scales(
        atoms, ghosts, slab_devices, facts_ref, rw_ref, hot_ref, radial_ref, lent_ref
    )
    pulls_ref[...] = (part_ref[...] + jnp.concatenate(pulls, axis=1)).astype(BF16)
    for copy in copies:
        copy.wait()


def join_kernel(pair_ref, other_ref, both_ref):
    ghosts = pair_ref.shape[0]
    both_ref[:ghosts] = pair_ref[...]
    both_ref[ghosts:] = other_ref[...]


def layer_sums(layer, degrees, channels, atoms, per_atom, tables, weights, hots, radials, scratch):
    joined, mixed = scratch
    groups = slot_groups(degrees)
    w_zero, w_one_re, w_one_im, w_two_re, w_two_im = (ref[...] for ref in weights)
    width = joined.shape[1]
    start = 0
    for ref, begin, end in tables:
        joined[start : start + end - begin] = ref[begin:end, :width].astype(F32)
        start += end - begin
    rows = start

    def put(column, value):
        high = value.astype(BF16)
        low = (value - high.astype(F32)).astype(BF16)
        mixed[:rows, column : column + value.shape[1]] = high
        mixed[rows:, column : column + value.shape[1]] = low

    span = len(groups[0]) * channels
    zero = dot(joined[:, :span].astype(BF16), w_zero)
    put(0, zero)
    column = span
    for index, (real, imag) in enumerate(((w_one_re, w_one_im), (w_two_re, w_two_im))):
        span = len(groups[2 * index + 1]) * channels
        both = jnp.concatenate(
            [joined[:, column : column + span], joined[:, column + span : column + 2 * span]], axis=0
        ).astype(BF16)
        by_real = dot(both, real)
        by_imag = dot(both, imag)
        put(column, by_real[:rows] - by_imag[rows:])
        put(column + span, by_imag[:rows] + by_real[rows:])
        column += 2 * span
    part = atoms // len(hots)
    sums = []
    first = None
    step = 2 * channels
    for begin in range(0, width, step):
        end = min(begin + step, width)
        pieces = []
        for hot_ref, radial_ref in zip(hots, radials):
            got = dot(hot_ref[...], mixed[:, begin:end])
            for inner in range(0, end - begin, channels):
                message = got[:, inner : inner + channels] * radial_ref[layer]
                if first is None:
                    first = message
                pieces.append(message.reshape(part, per_atom, channels).sum(axis=1))
        count = (end - begin) // channels
        for inner in range(count):
            sums.append(jnp.concatenate(pieces[inner::count], axis=0))
    return sums, first, zero


def first_kernel(
    layer, last, degrees, channels, per_atom, count,
    lent_ref, hot_ref, radial_ref, lent_y_ref, hot_y_ref, radial_y_ref, pulls_ref, *refs,
):
    tables, weights = refs[:count], refs[count : count + 5]
    own_ref, pair_ref, other_ref = refs[count + 5 : count + 8]
    scratch = refs[count + 8 :]
    joined = scratch[0]
    both = own_ref.shape[0]
    atoms, ghosts = both // 2, lent_ref.shape[1] // 2
    sums, _, _ = layer_sums(
        layer, degrees, channels, both, per_atom, [(ref, 0, ref.shape[0]) for ref in tables], weights,
        (hot_ref, hot_y_ref), (radial_ref, radial_y_ref), scratch,
    )
    width = len(sums) * channels
    for place, total in enumerate(sums):
        cols = slice(place * channels, (place + 1) * channels)
        own_ref[:, cols] = (joined[:both, cols] + 0.18 * total).astype(BF16)
    for side, hot in enumerate((lent_ref, lent_y_ref)):
        lent = lent_rows(hot[...], own_ref[side * atoms : (side + 1) * atoms, :width])
        pair_ref[side * ghosts : (side + 1) * ghosts, :width] = lent[:ghosts]
        other_ref[side * ghosts : (side + 1) * ghosts, :width] = lent[ghosts:]
    if last:
        part = pulls_ref.shape[1]
        block = 2 * atoms + 4 * ghosts
        for slot in range(pulls_ref.shape[0] // block):
            cols = slice(width + slot // 2 * part, width + (slot // 2 + 1) * part)
            at = slot * block
            for ref, size, gap in (
                (own_ref, atoms, 2 * atoms), (pair_ref, ghosts, ghosts), (other_ref, ghosts, 0)
            ):
                to = slot % 2 * size
                ref[to : to + size, cols] = pulls_ref[at : at + size]
                at += gap


def last_kernel(
    layer, degrees, channels, atoms, per_atom, count,
    rest_ref, lent_ref, hot_ref, radial_ref, dirs_ref, readout_ref, *refs,
):
    tables, weights = refs[:count], refs[count : count + 5]
    out_ref, force_ref = refs[count + 5 : count + 7]
    scratch = refs[count + 7 :]
    joined = scratch[0]
    ghosts = lent_ref.shape[1] // 2
    pieces = []
    for slot in range(count // 3):
        own_rows, pair_rows, other_rows = tables[3 * slot : 3 * slot + 3]
        pieces.append((own_rows, 0, 2 * atoms))
        for upper in range(2):
            span = (upper * ghosts, (upper + 1) * ghosts)
            pieces += [(pair_rows, *span), (other_rows, *span)]
    sums, first, zero = layer_sums(
        layer, degrees, channels, atoms, per_atom, pieces, weights, (hot_ref,), (radial_ref,), scratch
    )
    order = slot_order(degrees)
    for place, slot in enumerate(order):
        cols = slice(place * channels, (place + 1) * channels)
        out_ref[slot] = (joined[:atoms, cols] + 0.18 * sums[place]).astype(BF16)
    for place, slot in enumerate(unused_slots(degrees * degrees)):
        out_ref[slot] = rest_ref[place]

    width = len(sums) * channels
    part = 3 * channels
    own, lent = 0.0, []
    for slot in range(count // 3):
        cols = slice(width + slot // 2 * part, width + (slot // 2 + 1) * part)
        own_rows, *lent_blocks = (
            tables[3 * slot + kind][slot % 2 * size : (slot % 2 + 1) * size, cols].astype(F32)
            for kind, size in enumerate((atoms, ghosts, ghosts))
        )
        own += own_rows
        lent += lent_blocks
    hot = jnp.concatenate([lent_ref[...]] * (count // 3), axis=1).astype(BF16)
    pulls = own + dot(hot, jnp.concatenate(lent, axis=0).astype(BF16))
    readout = readout_ref[...]
    parts = []
    for axis in range(3):
        pull = (first * dirs_ref[axis]).reshape(atoms, per_atom, channels).sum(axis=1)
        back = zero[:atoms, :channels] * pulls[:, axis * channels : (axis + 1) * channels]
        parts.append((pull - back) * readout)
    ones = jnp.ones((8, channels), F32)
    total = dot(ones, jnp.concatenate(parts, axis=0), ((1,), (1,)), HIGHEST)
    for axis in range(3):
        force_ref[axis : axis + 1, :] = total[:1, axis * atoms : (axis + 1) * atoms]


def across(block, bit, slab_devices):
    return lax.ppermute(block, "yz", [(q, q ^ bit) for q in range(slab_devices)])


def toward(block, step, slabs):
    route = []
    for slab in range(slabs):
        to = slab + 1 if (slab % 2 == 0) == (step > 0) else slab - 1
        route.append((slab, to % slabs))
    return lax.ppermute(block, "slab", route)


def spread(held, bits, slab_devices):
    for bit in bits:
        for slot in sorted(held):
            got = []
            for block in held[slot]:
                got.append(across(block, bit, slab_devices))
            held[slot | bit] = tuple(got)
    return held


def order_bits(slab_devices):
    bits, bit = [], slab_devices // 2
    while bit:
        bits.append(bit)
        bit //= 2
    return bits


def body(
    embeddings, neighbours, valid, azimuth, polar, distance, send_low, send_high,
    w_zero, w_one_re, w_one_im, w_two_re, w_two_im, radial_weight, readout,
):
    atoms, coeffs, channels = embeddings.shape
    degrees = math.isqrt(coeffs)
    ghosts = send_low.shape[0]
    edges = neighbours.shape[0]
    layers = w_zero.shape[0]
    slabs, slab_devices = lax.axis_size("slab"), lax.axis_size("yz")
    rows = slab_devices * (atoms + 2 * ghosts)
    width = len(slot_order(degrees)) * channels
    low, high = send_low.reshape(1, -1), send_high.reshape(1, -1)
    held, shape = pltpu.VMEM, jax.ShapeDtypeStruct
    embeddings = embeddings.transpose(1, 0, 2)
    params = pltpu.CompilerParams(vmem_limit_bytes=24 * 2**20)
    row = lambda value: value.reshape(1, -1)
    far = pl.BlockSpec(memory_space=pl.ANY)

    half = slab_devices // 2
    bits = order_bits(slab_devices)
    own, pair, other, rest, radial_weight, vector = pl.pallas_call(
        pack_kernel,
        out_shape=[
            held((atoms, width + edges), BF16), held((ghosts, width), BF16),
            held((ghosts, width), BF16), held((len(unused_slots(coeffs)), atoms, channels), BF16),
            held(radial_weight.shape, F32), held((1, channels), F32),
        ],
        in_specs=[VMEM] * 10,
        out_specs=[VMEM] * 6,
        compiler_params=params,
        name="pack",
    )(*away(
        embeddings, low, high, *map(row, (neighbours, valid, distance, azimuth, polar)),
        radial_weight, row(readout),
    ))

    got_other = toward(other, -1, slabs)
    got_pair = toward(pair, 1, slabs)
    got_own = across(own, half, slab_devices)
    weights = (w_zero, w_one_re, w_one_im, w_two_re, w_two_im)
    count = len(weights)
    near_weights = [held(array.shape[1:], array.dtype) for array in weights]
    side_shapes = [
        held((edges, 2 * rows), BF16), held((layers, edges, channels), F32),
        held((atoms, 2 * ghosts), F32),
    ]
    later = [(layer, which) for layer in range(1, layers) for which in range(count)]
    plans = (
        [(0, which) for which in range(count)] + [entry for entry in later if entry[1] < 2],
        [entry for entry in later if entry[1] >= 2],
    )

    def scales(kernel, plan, more, *arrays):
        return pl.pallas_call(
            functools.partial(kernel, atoms, ghosts, slab_devices, count, plan),
            out_shape=[*side_shapes, *more, *(near_weights[which] for _, which in plan)],
            in_specs=[VMEM] * len(arrays) + [far] * count,
            out_specs=[VMEM] * (3 + len(more) + len(plan)),
            scratch_shapes=[pltpu.SemaphoreType.DMA((len(plan),))],
            compiler_params=params,
        )(*near(*arrays), *away(*weights))

    hot, radial, lent, dirs, part, *first_weights = scales(
        own_scale_kernel, plans[0],
        [held((3, edges, channels), F32), held((rows, 3 * channels), F32)], own, radial_weight,
    )
    got_pair, part = lax.optimization_barrier((got_pair, part))
    joined = pl.pallas_call(
        join_kernel,
        out_shape=held((2 * ghosts, width), BF16),
        in_specs=[VMEM] * 2,
        out_specs=VMEM,
        compiler_params=params,
        name="join",
    )(*near(got_pair, got_other))
    joined_y = across(joined, half, slab_devices)
    hot_y, radial_y, lent_y, pulls, *later_weights = scales(
        partner_scale_kernel, plans[1], [held((rows, 3 * channels), BF16)],
        got_own, radial_weight, part,
    )
    blocks = spread({0: (own, joined), half: (got_own, joined_y)}, bits[1:], slab_devices)
    tables = [
        blocks[slot + upper][kind]
        for slot in range(half) for kind in range(2) for upper in (0, half)
    ]
    scratch = [pltpu.VMEM((rows, width), F32), pltpu.VMEM((2 * rows, width), BF16)]
    per_atom = edges // atoms
    fetched = dict(zip(plans[0] + plans[1], [*first_weights, *later_weights]))
    for layer in range(layers):
        now = [fetched[layer, which] for which in range(count)]
        if layer < layers - 1:
            last = layer == layers - 2
            wide = width + ((half + 1) // 2 * 3 * channels if last else 0)
            own, pair, other = pl.pallas_call(
                functools.partial(first_kernel, layer, last, degrees, channels, per_atom, len(tables)),
                out_shape=[
                    held((2 * atoms, wide), BF16), held((2 * ghosts, wide), BF16),
                    held((2 * ghosts, wide), BF16),
                ],
                in_specs=[VMEM] * (7 + len(tables) + count),
                out_specs=[VMEM] * 3,
                scratch_shapes=scratch,
                compiler_params=params,
                name="layer",
            )(*near(lent, hot, radial, lent_y, hot_y, radial_y, pulls, *tables, *now))
            got_other = toward(other, -1, slabs)
            got_pair = toward(pair, 1, slabs)
            blocks = spread({0: (own, got_pair, got_other)}, bits[1:], slab_devices)
            tables = [block for slot in range(half) for block in blocks[slot]]
        else:
            updated, forces = pl.pallas_call(
                functools.partial(
                    last_kernel, layer, degrees, channels, atoms, per_atom, len(tables)
                ),
                out_shape=[shape((coeffs, atoms, channels), BF16), shape((3, atoms), F32)],
                in_specs=[VMEM] * (6 + len(tables) + count),
                out_specs=[VMEM] * 2,
                scratch_shapes=scratch,
                compiler_params=params,
                name="last_layer",
            )(*near(rest, lent, hot, radial, dirs, vector, *tables, *now))
    return (updated.transpose(1, 0, 2), forces)


def solution(mesh):
    both = ("slab", "yz")
    in_specs = (P(both, None, None), *([P(both)] * 7), *([P()] * 7))
    out_specs = (P(both, None, None), P(None, both))
    return jax.shard_map(body, mesh=mesh, in_specs=in_specs, out_specs=out_specs, check_vma=False)
```

```python
import functools
import math

import jax
import jax.numpy as jnp
from jax import lax
from jax.experimental import pallas as pl
from jax.experimental.pallas import tpu as pltpu
from jax.sharding import PartitionSpec as P


HIGHEST = lax.Precision.HIGHEST
BF16 = jnp.bfloat16
F32 = jnp.float32
ORDERS = (1, 2)
DIGIT = 128
VMEM = pl.BlockSpec(memory_space=pltpu.VMEM)


def near(*arrays):
    return [pltpu.with_memory_space_constraint(array, pltpu.VMEM) for array in arrays]


def away(*arrays):
    return [pltpu.with_memory_space_constraint(array, pltpu.HBM) for array in arrays]


def slot_index(degree, azimuth_order):
    return degree * degree + degree + azimuth_order


def slot_groups(degrees):
    groups = [[slot_index(degree, 0) for degree in range(degrees)]]
    for order in ORDERS:
        groups.append([slot_index(degree, order) for degree in range(order, degrees)])
        groups.append([slot_index(degree, -order) for degree in range(order, degrees)])
    return groups


def slot_order(degrees):
    return [slot for group in slot_groups(degrees) for slot in group]


def unused_slots(coeffs):
    order = slot_order(math.isqrt(coeffs))
    return [slot for slot in range(coeffs) if slot not in order]


def odd_slab():
    return lax.axis_index("slab") % 2 == 1


def dot(left, right, contract=((1,), (0,)), precision=None):
    return lax.dot_general(
        left, right, (contract, ((), ())), precision=precision, preferred_element_type=F32
    )


def lent_picks(low_ref, high_ref):
    odd = odd_slab()
    low, high = low_ref[...], high_ref[...]
    return jnp.concatenate([jnp.where(odd, low, high), jnp.where(odd, high, low)], axis=1)


def lent_hot(picks, atoms):
    rows = lax.broadcasted_iota(jnp.int32, (atoms, picks.shape[1]), 0)
    return (rows == picks).astype(F32)


def lent_rows(hot, rows):
    return dot(hot.astype(BF16), rows, ((0,), (0,))).astype(BF16)


def thirds(value):
    parts = []
    for _ in range(3):
        part = value.astype(BF16).astype(F32)
        parts.append(part)
        value = value - part
    return parts


def pack_kernel(
    emb_ref, low_ref, high_ref, nbr_ref, valid_ref, dist_ref, azi_ref, pol_ref, rw_ref, readout_ref,
    own_ref, pair_ref, other_ref, rest_ref, scales_ref, vector_ref,
):
    coeffs, atoms, channels = emb_ref.shape
    ghosts = low_ref.shape[1]
    edges = nbr_ref.shape[1]
    order = slot_order(math.isqrt(coeffs))
    width = len(order) * channels
    for place, slot in enumerate(order):
        own_ref[:, place * channels : (place + 1) * channels] = emb_ref[slot]
    for place, slot in enumerate(unused_slots(coeffs)):
        rest_ref[place] = emb_ref[slot]
    picks = lent_picks(low_ref, high_ref)
    lent = lent_rows(lent_hot(picks, atoms), own_ref[:, :width])
    pair_ref[...] = lent[:ghosts]
    other_ref[...] = lent[ghosts:]
    nbr = nbr_ref[...]
    picks = jnp.concatenate(
        [picks, jnp.zeros((1, edges - 2 * ghosts), jnp.int32)], axis=1
    ).astype(F32)
    facts = [
        (nbr // DIGIT).astype(F32), (nbr % DIGIT).astype(F32), valid_ref[...].astype(F32), picks,
        *thirds(dist_ref[...]), *thirds(azi_ref[...]), *thirds(pol_ref[...]),
    ]
    facts.append(jnp.zeros((atoms - len(facts), edges), F32))
    own_ref[:, width:] = jnp.concatenate(facts, axis=0).astype(BF16)
    scales_ref[...] = rw_ref[...]
    vector_ref[...] = 0.125 * readout_ref[...]


def edge_facts(ref, edges):
    rows = ref[:, ref.shape[1] - edges :].astype(F32)
    row = lambda at: rows[at : at + 1]
    whole = lambda at: row(at) + row(at + 1) + row(at + 2)
    nbr = (row(0) * DIGIT + row(1)).astype(jnp.int32)
    return nbr, row(2), row(3).astype(jnp.int32), whole(4), whole(7), whole(10)


def start_fetch(far, near_refs, sems, plan):
    copies = [
        pltpu.make_async_copy(far[which].at[layer], near_refs[i], sems.at[i])
        for i, (layer, which) in enumerate(plan)
    ]
    for copy in copies:
        copy.start()
    return copies


def edge_scales(
    atoms, ghosts, slab_devices, facts_ref, rw_ref, hot_ref, radial_ref, lent_ref
):
    layers, centers = rw_ref.shape[0], rw_ref.shape[1]
    own_count, ghost_count = slab_devices * atoms, slab_devices * ghosts
    half = slab_devices // 2
    me = lax.axis_index("yz")
    odd = odd_slab()
    edges = hot_ref.shape[0]
    count = hot_ref.shape[1] // 2
    nbr, valid, picks, distance, _, _ = edge_facts(facts_ref, edges)
    is_own = nbr < own_count
    ghost = nbr - own_count
    below = ghost < ghost_count
    ghost = jnp.where(below, ghost, ghost - ghost_count)
    paired = jnp.where(odd, below.astype(jnp.int32), 1 - below.astype(jnp.int32))
    slot = jnp.where(is_own, nbr // atoms, ghost // ghosts) ^ me
    upper = slot // half
    inner = jnp.where(
        is_own,
        upper * atoms + nbr % atoms,
        2 * atoms + upper * (2 * ghosts) + (1 - paired) * ghosts + ghost % ghosts,
    )
    place = (slot % half) * (2 * atoms + 4 * ghosts) + inner
    rows = lax.broadcasted_iota(jnp.int32, (count, edges), 0)
    hot = jnp.where((rows == place) & (valid != 0.0), 1.0, 0.0).astype(F32)
    hot_cols = jnp.transpose(hot).astype(BF16)
    hot_ref[...] = jnp.concatenate([hot_cols, hot_cols], axis=1)
    middle = 1.0 + 0.5 * lax.broadcasted_iota(jnp.int32, (centers, edges), 0).astype(F32)
    basis = jnp.exp(-jnp.square((distance - middle) / 0.5))
    for layer in range(layers):
        scale = dot(basis, rw_ref[layer], ((0,), (0,)), HIGHEST)
        radial = scale / (1.0 + jnp.exp(-scale))
        radial_ref[layer] = radial
    lent_ref[...] = lent_hot(picks[:, : 2 * ghosts], atoms)
    return hot, radial


def pull_sums(facts_ref, hot, radial):
    _, _, _, _, azimuth, polar = edge_facts(facts_ref, hot.shape[1])
    sin_polar = jnp.sin(polar)
    dirs = [sin_polar * jnp.cos(azimuth), sin_polar * jnp.sin(azimuth), jnp.cos(polar)]
    count, channels = hot.shape[0], radial.shape[1]
    high = radial.astype(BF16)
    both = jnp.concatenate([high, (radial - high.astype(F32)).astype(BF16)], axis=1)
    pulls = []
    for axis in range(3):
        along = hot * dirs[axis]
        high = along.astype(BF16)
        low = (along - high.astype(F32)).astype(BF16)
        got = dot(jnp.concatenate([high, low], axis=0), both)
        pulls.append(got[:count, :channels] + got[:count, channels:] + got[count:, :channels])
    return dirs, jnp.concatenate(pulls, axis=1)


def own_scale_kernel(
    atoms, ghosts, slab_devices, facts_ref, rw_ref, hot_ref, radial_ref, lent_ref, flags_ref
):
    flags_ref[...], _ = edge_scales(
        atoms, ghosts, slab_devices, facts_ref, rw_ref, hot_ref, radial_ref, lent_ref
    )


def partner_scale_kernel(
    atoms, ghosts, slab_devices, count, plan,
    facts_ref, rw_ref, own_ref, own_radial_ref, flags_ref, *refs,
):
    far, (hot_ref, radial_ref, lent_ref, dirs_ref, pulls_ref), refs = (
        refs[:count], refs[count : count + 5], refs[count + 5 :]
    )
    copies = start_fetch(far, refs[:-1], refs[-1], plan)
    hot, radial = edge_scales(
        atoms, ghosts, slab_devices, facts_ref, rw_ref, hot_ref, radial_ref, lent_ref
    )
    _, pulls = pull_sums(facts_ref, hot, radial)
    dirs, own_pulls = pull_sums(own_ref, flags_ref[...], own_radial_ref[own_radial_ref.shape[0] - 1])
    pulls_ref[...] = (pulls + own_pulls).astype(BF16)
    columns = jnp.transpose(jnp.concatenate([*dirs, *dirs, *dirs[:2]], axis=0))
    for axis in range(3):
        dirs_ref[axis] = jnp.broadcast_to(columns[:, axis : axis + 1], dirs_ref.shape[1:])
    for copy in copies:
        copy.wait()


def fetch_kernel(count, plan, *refs):
    for copy in start_fetch(refs[:count], refs[count:-1], refs[-1], plan):
        copy.wait()


def join_kernel(pair_ref, other_ref, both_ref):
    ghosts = pair_ref.shape[0]
    both_ref[:ghosts] = pair_ref[...]
    both_ref[ghosts:] = other_ref[...]


def layer_sums(layer, degrees, channels, atoms, per_atom, tables, weights, hots, radials, scratch):
    joined, mixed = scratch
    groups = slot_groups(degrees)
    w_zero, w_one_re, w_one_im, w_two_re, w_two_im = (ref[...] for ref in weights)
    width = joined.shape[1]
    start = 0
    for ref, begin, end in tables:
        joined[start : start + end - begin] = ref[begin:end, :width].astype(F32)
        start += end - begin
    rows = start

    def put(column, value):
        high = value.astype(BF16)
        low = (value - high.astype(F32)).astype(BF16)
        mixed[:rows, column : column + value.shape[1]] = high
        mixed[rows:, column : column + value.shape[1]] = low

    span = len(groups[0]) * channels
    zero = dot(joined[:, :span].astype(BF16), w_zero)
    put(0, zero)
    column = span
    for index, (real, imag) in enumerate(((w_one_re, w_one_im), (w_two_re, w_two_im))):
        span = len(groups[2 * index + 1]) * channels
        both = jnp.concatenate(
            [joined[:, column : column + span], joined[:, column + span : column + 2 * span]], axis=0
        ).astype(BF16)
        by_real = dot(both, real)
        by_imag = dot(both, imag)
        put(column, by_real[:rows] - by_imag[rows:])
        put(column + span, by_imag[:rows] + by_real[rows:])
        column += 2 * span
    part = atoms // len(hots)
    sums = []
    first = None
    step = 2 * channels
    for begin in range(0, width, step):
        end = min(begin + step, width)
        pieces = []
        for hot_ref, radial_ref in zip(hots, radials):
            got = dot(hot_ref[...], mixed[:, begin:end])
            for inner in range(0, end - begin, channels):
                message = got[:, inner : inner + channels] * radial_ref[layer]
                if first is None:
                    first = message
                pieces.append(message.reshape(part, per_atom, channels).sum(axis=1))
        count = (end - begin) // channels
        for inner in range(count):
            sums.append(jnp.concatenate(pieces[inner::count], axis=0))
    return sums, first, zero


def first_kernel(
    layer, last, degrees, channels, per_atom, count,
    lent_ref, hot_ref, radial_ref, lent_y_ref, hot_y_ref, radial_y_ref, pulls_ref, *refs,
):
    tables, weights = refs[:count], refs[count : count + 5]
    own_ref, pair_ref, other_ref = refs[count + 5 : count + 8]
    scratch = refs[count + 8 :]
    joined = scratch[0]
    both = own_ref.shape[0]
    atoms, ghosts = both // 2, lent_ref.shape[1] // 2
    sums, _, _ = layer_sums(
        layer, degrees, channels, both, per_atom, [(ref, 0, ref.shape[0]) for ref in tables], weights,
        (hot_ref, hot_y_ref), (radial_ref, radial_y_ref), scratch,
    )
    width = len(sums) * channels
    for place, total in enumerate(sums):
        cols = slice(place * channels, (place + 1) * channels)
        own_ref[:, cols] = (joined[:both, cols] + 0.18 * total).astype(BF16)
    for side, hot in enumerate((lent_ref, lent_y_ref)):
        lent = lent_rows(hot[...], own_ref[side * atoms : (side + 1) * atoms, :width])
        pair_ref[side * ghosts : (side + 1) * ghosts, :width] = lent[:ghosts]
        other_ref[side * ghosts : (side + 1) * ghosts, :width] = lent[ghosts:]
    if last:
        part = pulls_ref.shape[1]
        block = 2 * atoms + 4 * ghosts
        for slot in range(pulls_ref.shape[0] // block):
            cols = slice(width + slot // 2 * part, width + (slot // 2 + 1) * part)
            at = slot * block
            for ref, size, gap in (
                (own_ref, atoms, 2 * atoms), (pair_ref, ghosts, ghosts), (other_ref, ghosts, 0)
            ):
                to = slot % 2 * size
                ref[to : to + size, cols] = pulls_ref[at : at + size]
                at += gap


def last_kernel(
    layer, degrees, channels, atoms, per_atom, count,
    rest_ref, lent_ref, hot_ref, radial_ref, dirs_ref, readout_ref, *refs,
):
    tables, weights = refs[:count], refs[count : count + 5]
    out_ref, force_ref = refs[count + 5 : count + 7]
    scratch = refs[count + 7 :]
    joined = scratch[0]
    ghosts = lent_ref.shape[1] // 2
    pieces = []
    for slot in range(count // 3):
        own_rows, pair_rows, other_rows = tables[3 * slot : 3 * slot + 3]
        pieces.append((own_rows, 0, 2 * atoms))
        for upper in range(2):
            span = (upper * ghosts, (upper + 1) * ghosts)
            pieces += [(pair_rows, *span), (other_rows, *span)]
    sums, first, zero = layer_sums(
        layer, degrees, channels, atoms, per_atom, pieces, weights, (hot_ref,), (radial_ref,), scratch
    )
    order = slot_order(degrees)
    for place, slot in enumerate(order):
        cols = slice(place * channels, (place + 1) * channels)
        out_ref[slot] = (joined[:atoms, cols] + 0.18 * sums[place]).astype(BF16)
    for place, slot in enumerate(unused_slots(degrees * degrees)):
        out_ref[slot] = rest_ref[place]

    width = len(sums) * channels
    part = 3 * channels
    own, lent = 0.0, []
    for slot in range(count // 3):
        cols = slice(width + slot // 2 * part, width + (slot // 2 + 1) * part)
        own_rows, *lent_blocks = (
            tables[3 * slot + kind][slot % 2 * size : (slot % 2 + 1) * size, cols].astype(F32)
            for kind, size in enumerate((atoms, ghosts, ghosts))
        )
        own += own_rows
        lent += lent_blocks
    hot = jnp.concatenate([lent_ref[...]] * (count // 3), axis=1).astype(BF16)
    pulls = own + dot(hot, jnp.concatenate(lent, axis=0).astype(BF16))
    readout = readout_ref[...]
    parts = []
    for axis in range(3):
        pull = (first * dirs_ref[axis]).reshape(atoms, per_atom, channels).sum(axis=1)
        back = zero[:atoms, :channels] * pulls[:, axis * channels : (axis + 1) * channels]
        parts.append((pull - back) * readout)
    ones = jnp.ones((8, channels), F32)
    total = dot(ones, jnp.concatenate(parts, axis=0), ((1,), (1,)), HIGHEST)
    for axis in range(3):
        force_ref[axis : axis + 1, :] = total[:1, axis * atoms : (axis + 1) * atoms]


def across(block, bit, slab_devices):
    return lax.ppermute(block, "yz", [(q, q ^ bit) for q in range(slab_devices)])


def toward(block, step, slabs):
    route = []
    for slab in range(slabs):
        to = slab + 1 if (slab % 2 == 0) == (step > 0) else slab - 1
        route.append((slab, to % slabs))
    return lax.ppermute(block, "slab", route)


def spread(held, bits, slab_devices):
    for bit in bits:
        for slot in sorted(held):
            got = []
            for block in held[slot]:
                got.append(across(block, bit, slab_devices))
            held[slot | bit] = tuple(got)
    return held


def order_bits(slab_devices):
    bits, bit = [], slab_devices // 2
    while bit:
        bits.append(bit)
        bit //= 2
    return bits


def body(
    embeddings, neighbours, valid, azimuth, polar, distance, send_low, send_high,
    w_zero, w_one_re, w_one_im, w_two_re, w_two_im, radial_weight, readout,
):
    atoms, coeffs, channels = embeddings.shape
    degrees = math.isqrt(coeffs)
    ghosts = send_low.shape[0]
    edges = neighbours.shape[0]
    layers = w_zero.shape[0]
    slabs, slab_devices = lax.axis_size("slab"), lax.axis_size("yz")
    rows = slab_devices * (atoms + 2 * ghosts)
    width = len(slot_order(degrees)) * channels
    low, high = send_low.reshape(1, -1), send_high.reshape(1, -1)
    held, shape = pltpu.VMEM, jax.ShapeDtypeStruct
    embeddings = embeddings.transpose(1, 0, 2)
    params = pltpu.CompilerParams(vmem_limit_bytes=24 * 2**20)
    row = lambda value: value.reshape(1, -1)
    far = pl.BlockSpec(memory_space=pl.ANY)

    half = slab_devices // 2
    bits = order_bits(slab_devices)
    own, pair, other, rest, radial_weight, vector = pl.pallas_call(
        pack_kernel,
        out_shape=[
            held((atoms, width + edges), BF16), held((ghosts, width), BF16),
            held((ghosts, width), BF16), held((len(unused_slots(coeffs)), atoms, channels), BF16),
            held(radial_weight.shape, F32), held((1, channels), F32),
        ],
        in_specs=[VMEM] * 10,
        out_specs=[VMEM] * 6,
        compiler_params=params,
        name="pack",
    )(*away(
        embeddings, low, high, *map(row, (neighbours, valid, distance, azimuth, polar)),
        radial_weight, row(readout),
    ))

    got_other = toward(other, -1, slabs)
    got_pair = toward(pair, 1, slabs)
    got_own = across(own, half, slab_devices)
    weights = (w_zero, w_one_re, w_one_im, w_two_re, w_two_im)
    count = len(weights)
    near_weights = [held(array.shape[1:], array.dtype) for array in weights]
    side_shapes = [
        held((edges, 2 * rows), BF16), held((layers, edges, channels), F32),
        held((atoms, 2 * ghosts), F32),
    ]
    plans = [[(layer, which) for which in range(count)] for layer in range(layers)]

    hot, radial, lent, flags = pl.pallas_call(
        functools.partial(own_scale_kernel, atoms, ghosts, slab_devices),
        out_shape=[*side_shapes, held((rows, edges), F32)],
        in_specs=[VMEM] * 2,
        out_specs=[VMEM] * 4,
        compiler_params=params,
        name="scales",
    )(*near(own, radial_weight))
    got_pair, flags = lax.optimization_barrier((got_pair, flags))
    joined = pl.pallas_call(
        join_kernel,
        out_shape=held((2 * ghosts, width), BF16),
        in_specs=[VMEM] * 2,
        out_specs=VMEM,
        compiler_params=params,
        name="join",
    )(*near(got_pair, got_other))
    joined_y = across(joined, half, slab_devices)
    hot_y, radial_y, lent_y, dirs, pulls, *now = pl.pallas_call(
        functools.partial(partner_scale_kernel, atoms, ghosts, slab_devices, count, plans[0]),
        out_shape=[
            *side_shapes, held((3, edges, channels), F32), held((rows, 3 * channels), BF16),
            *near_weights,
        ],
        in_specs=[VMEM] * 5 + [far] * count,
        out_specs=[VMEM] * (5 + count),
        scratch_shapes=[pltpu.SemaphoreType.DMA((count,))],
        compiler_params=params,
        name="scales_y",
    )(*near(got_own, radial_weight, own, radial, flags), *away(*weights))
    blocks = spread({0: (own, joined), half: (got_own, joined_y)}, bits[1:], slab_devices)
    tables = [
        blocks[slot + upper][kind]
        for slot in range(half) for kind in range(2) for upper in (0, half)
    ]
    scratch = [pltpu.VMEM((rows, width), F32), pltpu.VMEM((2 * rows, width), BF16)]
    per_atom = edges // atoms
    for layer in range(layers):
        if layer < layers - 1:
            last = layer == layers - 2
            wide = width + ((half + 1) // 2 * 3 * channels if last else 0)
            own, pair, other = pl.pallas_call(
                functools.partial(first_kernel, layer, last, degrees, channels, per_atom, len(tables)),
                out_shape=[
                    held((2 * atoms, wide), BF16), held((2 * ghosts, wide), BF16),
                    held((2 * ghosts, wide), BF16),
                ],
                in_specs=[VMEM] * (7 + len(tables) + count),
                out_specs=[VMEM] * 3,
                scratch_shapes=scratch,
                compiler_params=params,
                name="layer",
            )(*near(lent, hot, radial, lent_y, hot_y, radial_y, pulls, *tables, *now))
            got_other = toward(other, -1, slabs)
            got_pair = toward(pair, 1, slabs)
            now = pl.pallas_call(
                functools.partial(fetch_kernel, count, plans[layer + 1]),
                out_shape=near_weights,
                in_specs=[far] * count,
                out_specs=[VMEM] * count,
                scratch_shapes=[pltpu.SemaphoreType.DMA((count,))],
                compiler_params=params,
                name="fetch",
            )(*away(*weights))
            blocks = spread({0: (own, got_pair, got_other)}, bits[1:], slab_devices)
            tables = [block for slot in range(half) for block in blocks[slot]]
        else:
            updated, forces = pl.pallas_call(
                functools.partial(
                    last_kernel, layer, degrees, channels, atoms, per_atom, len(tables)
                ),
                out_shape=[shape((coeffs, atoms, channels), BF16), shape((3, atoms), F32)],
                in_specs=[VMEM] * (6 + len(tables) + count),
                out_specs=[VMEM] * 2,
                scratch_shapes=scratch,
                compiler_params=params,
                name="last_layer",
            )(*near(rest, lent, hot, radial, dirs, vector, *tables, *now))
    return (updated.transpose(1, 0, 2), forces)


def solution(mesh):
    both = ("slab", "yz")
    in_specs = (P(both, None, None), *([P(both)] * 7), *([P()] * 7))
    out_specs = (P(both, None, None), P(None, both))
    return jax.shard_map(body, mesh=mesh, in_specs=in_specs, out_specs=out_specs, check_vma=False)
```

```python
import functools
import math

import jax
import jax.numpy as jnp
from jax import lax
from jax.experimental import pallas as pl
from jax.experimental.pallas import tpu as pltpu
from jax.sharding import PartitionSpec as P


HIGHEST = lax.Precision.HIGHEST
BF16 = jnp.bfloat16
F32 = jnp.float32
ORDERS = (1, 2)
DIGIT = 128
VMEM = pl.BlockSpec(memory_space=pltpu.VMEM)


def near(*arrays):
    return [pltpu.with_memory_space_constraint(array, pltpu.VMEM) for array in arrays]


def away(*arrays):
    return [pltpu.with_memory_space_constraint(array, pltpu.HBM) for array in arrays]


def slot_index(degree, azimuth_order):
    return degree * degree + degree + azimuth_order


def slot_groups(degrees):
    groups = [[slot_index(degree, 0) for degree in range(degrees)]]
    for order in ORDERS:
        groups.append([slot_index(degree, order) for degree in range(order, degrees)])
        groups.append([slot_index(degree, -order) for degree in range(order, degrees)])
    return groups


def slot_order(degrees):
    return [slot for group in slot_groups(degrees) for slot in group]


def unused_slots(coeffs):
    order = slot_order(math.isqrt(coeffs))
    return [slot for slot in range(coeffs) if slot not in order]


def odd_slab():
    return lax.axis_index("slab") % 2 == 1


def dot(left, right, contract=((1,), (0,)), precision=None):
    return lax.dot_general(
        left, right, (contract, ((), ())), precision=precision, preferred_element_type=F32
    )


def lent_picks(low_ref, high_ref):
    odd = odd_slab()
    low, high = low_ref[...], high_ref[...]
    return jnp.concatenate([jnp.where(odd, low, high), jnp.where(odd, high, low)], axis=1)


def lent_hot(picks, atoms):
    rows = lax.broadcasted_iota(jnp.int32, (atoms, picks.shape[1]), 0)
    return (rows == picks).astype(F32)


def lent_rows(hot, rows):
    return dot(hot.astype(BF16), rows, ((0,), (0,))).astype(BF16)


def thirds(value):
    parts = []
    for _ in range(3):
        part = value.astype(BF16).astype(F32)
        parts.append(part)
        value = value - part
    return parts


def pack_kernel(
    emb_ref, low_ref, high_ref, nbr_ref, valid_ref, dist_ref, azi_ref, pol_ref, rw_ref, readout_ref,
    own_ref, pair_ref, other_ref, rest_ref, scales_ref, vector_ref,
):
    coeffs, atoms, channels = emb_ref.shape
    ghosts = low_ref.shape[1]
    edges = nbr_ref.shape[1]
    order = slot_order(math.isqrt(coeffs))
    width = len(order) * channels
    for place, slot in enumerate(order):
        own_ref[:, place * channels : (place + 1) * channels] = emb_ref[slot]
    for place, slot in enumerate(unused_slots(coeffs)):
        rest_ref[place] = emb_ref[slot]
    picks = lent_picks(low_ref, high_ref)
    lent = lent_rows(lent_hot(picks, atoms), own_ref[:, :width])
    pair_ref[...] = lent[:ghosts]
    other_ref[...] = lent[ghosts:]
    nbr = nbr_ref[...]
    picks = jnp.concatenate(
        [picks, jnp.zeros((1, edges - 2 * ghosts), jnp.int32)], axis=1
    ).astype(F32)
    facts = [
        (nbr // DIGIT).astype(F32), (nbr % DIGIT).astype(F32), valid_ref[...].astype(F32), picks,
        *thirds(dist_ref[...]), *thirds(azi_ref[...]), *thirds(pol_ref[...]),
    ]
    facts.append(jnp.zeros((atoms - len(facts), edges), F32))
    own_ref[:, width:] = jnp.concatenate(facts, axis=0).astype(BF16)
    scales_ref[...] = rw_ref[...]
    vector_ref[...] = 0.125 * readout_ref[...]


def edge_facts(ref, edges):
    rows = ref[:, ref.shape[1] - edges :].astype(F32)
    row = lambda at: rows[at : at + 1]
    whole = lambda at: row(at) + row(at + 1) + row(at + 2)
    nbr = (row(0) * DIGIT + row(1)).astype(jnp.int32)
    return nbr, row(2), row(3).astype(jnp.int32), whole(4), whole(7), whole(10)


def start_fetch(far, near_refs, sems, plan):
    copies = [
        pltpu.make_async_copy(far[which].at[layer], near_refs[i], sems.at[i])
        for i, (layer, which) in enumerate(plan)
    ]
    for copy in copies:
        copy.start()
    return copies


def edge_scales(
    atoms, ghosts, slab_devices, facts_ref, rw_ref, hot_ref, radial_ref, lent_ref
):
    layers, centers = rw_ref.shape[0], rw_ref.shape[1]
    own_count, ghost_count = slab_devices * atoms, slab_devices * ghosts
    half = slab_devices // 2
    me = lax.axis_index("yz")
    odd = odd_slab()
    edges = hot_ref.shape[0]
    count = hot_ref.shape[1] // 2
    nbr, valid, picks, distance, _, _ = edge_facts(facts_ref, edges)
    is_own = nbr < own_count
    ghost = nbr - own_count
    below = ghost < ghost_count
    ghost = jnp.where(below, ghost, ghost - ghost_count)
    paired = jnp.where(odd, below.astype(jnp.int32), 1 - below.astype(jnp.int32))
    slot = jnp.where(is_own, nbr // atoms, ghost // ghosts) ^ me
    upper = slot // half
    inner = jnp.where(
        is_own,
        upper * atoms + nbr % atoms,
        2 * atoms + upper * (2 * ghosts) + (1 - paired) * ghosts + ghost % ghosts,
    )
    place = (slot % half) * (2 * atoms + 4 * ghosts) + inner
    rows = lax.broadcasted_iota(jnp.int32, (count, edges), 0)
    hot = jnp.where((rows == place) & (valid != 0.0), 1.0, 0.0).astype(F32)
    hot_cols = jnp.transpose(hot).astype(BF16)
    hot_ref[...] = jnp.concatenate([hot_cols, hot_cols], axis=1)
    middle = 1.0 + 0.5 * lax.broadcasted_iota(jnp.int32, (centers, edges), 0).astype(F32)
    basis = jnp.exp(-jnp.square((distance - middle) / 0.5))
    for layer in range(layers):
        scale = dot(basis, rw_ref[layer], ((0,), (0,)), HIGHEST)
        radial = scale / (1.0 + jnp.exp(-scale))
        radial_ref[layer] = radial
    lent_ref[...] = lent_hot(picks[:, : 2 * ghosts], atoms)
    return hot, radial


def pull_sums(facts_ref, hot, radial):
    _, _, _, _, azimuth, polar = edge_facts(facts_ref, hot.shape[1])
    sin_polar = jnp.sin(polar)
    dirs = [sin_polar * jnp.cos(azimuth), sin_polar * jnp.sin(azimuth), jnp.cos(polar)]
    count, channels = hot.shape[0], radial.shape[1]
    high = radial.astype(BF16)
    both = jnp.concatenate([high, (radial - high.astype(F32)).astype(BF16)], axis=1)
    pulls = []
    for axis in range(3):
        along = hot * dirs[axis]
        high = along.astype(BF16)
        low = (along - high.astype(F32)).astype(BF16)
        got = dot(jnp.concatenate([high, low], axis=0), both)
        pulls.append(got[:count, :channels] + got[:count, channels:] + got[count:, :channels])
    return dirs, jnp.concatenate(pulls, axis=1)


def own_scale_kernel(
    atoms, ghosts, slab_devices,
    facts_ref, rw_ref, hot_ref, radial_ref, lent_ref, dirs_ref, part_ref,
):
    hot, radial = edge_scales(
        atoms, ghosts, slab_devices, facts_ref, rw_ref, hot_ref, radial_ref, lent_ref
    )
    dirs, part_ref[...] = pull_sums(facts_ref, hot, radial)
    columns = jnp.transpose(jnp.concatenate([*dirs, *dirs, *dirs[:2]], axis=0))
    for axis in range(3):
        dirs_ref[axis] = jnp.broadcast_to(columns[:, axis : axis + 1], dirs_ref.shape[1:])


def partner_scale_kernel(
    atoms, ghosts, slab_devices, count, plan, facts_ref, rw_ref, part_ref, *refs
):
    far, (hot_ref, radial_ref, lent_ref, pulls_ref), refs = (
        refs[:count], refs[count : count + 4], refs[count + 4 :]
    )
    copies = start_fetch(far, refs[:-1], refs[-1], plan)
    hot, radial = edge_scales(
        atoms, ghosts, slab_devices, facts_ref, rw_ref, hot_ref, radial_ref, lent_ref
    )
    _, pulls = pull_sums(facts_ref, hot, radial)
    pulls_ref[...] = (part_ref[...] + pulls).astype(BF16)
    for copy in copies:
        copy.wait()


def fetch_kernel(count, plan, *refs):
    for copy in start_fetch(refs[:count], refs[count:-1], refs[-1], plan):
        copy.wait()


def join_kernel(pair_ref, other_ref, both_ref):
    ghosts = pair_ref.shape[0]
    both_ref[:ghosts] = pair_ref[...]
    both_ref[ghosts:] = other_ref[...]


def layer_sums(layer, degrees, channels, atoms, per_atom, tables, weights, hots, radials, scratch):
    joined, mixed = scratch
    groups = slot_groups(degrees)
    w_zero, w_one_re, w_one_im, w_two_re, w_two_im = (ref[...] for ref in weights)
    width = joined.shape[1]
    start = 0
    for ref, begin, end in tables:
        joined[start : start + end - begin] = ref[begin:end, :width].astype(F32)
        start += end - begin
    rows = start

    def put(column, value):
        high = value.astype(BF16)
        low = (value - high.astype(F32)).astype(BF16)
        mixed[:rows, column : column + value.shape[1]] = high
        mixed[rows:, column : column + value.shape[1]] = low

    span = len(groups[0]) * channels
    zero = dot(joined[:, :span].astype(BF16), w_zero)
    put(0, zero)
    column = span
    for index, (real, imag) in enumerate(((w_one_re, w_one_im), (w_two_re, w_two_im))):
        span = len(groups[2 * index + 1]) * channels
        both = jnp.concatenate(
            [joined[:, column : column + span], joined[:, column + span : column + 2 * span]], axis=0
        ).astype(BF16)
        by_real = dot(both, real)
        by_imag = dot(both, imag)
        put(column, by_real[:rows] - by_imag[rows:])
        put(column + span, by_imag[:rows] + by_real[rows:])
        column += 2 * span
    part = atoms // len(hots)
    sums = []
    first = None
    step = 2 * channels
    for begin in range(0, width, step):
        end = min(begin + step, width)
        pieces = []
        for hot_ref, radial_ref in zip(hots, radials):
            got = dot(hot_ref[...], mixed[:, begin:end])
            for inner in range(0, end - begin, channels):
                message = got[:, inner : inner + channels] * radial_ref[layer]
                if first is None:
                    first = message
                pieces.append(message.reshape(part, per_atom, channels).sum(axis=1))
        count = (end - begin) // channels
        for inner in range(count):
            sums.append(jnp.concatenate(pieces[inner::count], axis=0))
    return sums, first, zero


def first_kernel(
    layer, last, degrees, channels, per_atom, count,
    lent_ref, hot_ref, radial_ref, lent_y_ref, hot_y_ref, radial_y_ref, pulls_ref, *refs,
):
    tables, weights = refs[:count], refs[count : count + 5]
    own_ref, pair_ref, other_ref = refs[count + 5 : count + 8]
    scratch = refs[count + 8 :]
    joined = scratch[0]
    both = own_ref.shape[0]
    atoms, ghosts = both // 2, lent_ref.shape[1] // 2
    sums, _, _ = layer_sums(
        layer, degrees, channels, both, per_atom, [(ref, 0, ref.shape[0]) for ref in tables], weights,
        (hot_ref, hot_y_ref), (radial_ref, radial_y_ref), scratch,
    )
    width = len(sums) * channels
    for place, total in enumerate(sums):
        cols = slice(place * channels, (place + 1) * channels)
        own_ref[:, cols] = (joined[:both, cols] + 0.18 * total).astype(BF16)
    for side, hot in enumerate((lent_ref, lent_y_ref)):
        lent = lent_rows(hot[...], own_ref[side * atoms : (side + 1) * atoms, :width])
        pair_ref[side * ghosts : (side + 1) * ghosts, :width] = lent[:ghosts]
        other_ref[side * ghosts : (side + 1) * ghosts, :width] = lent[ghosts:]
    if last:
        part = pulls_ref.shape[1]
        block = 2 * atoms + 4 * ghosts
        for slot in range(pulls_ref.shape[0] // block):
            cols = slice(width + slot // 2 * part, width + (slot // 2 + 1) * part)
            at = slot * block
            for ref, size, gap in (
                (own_ref, atoms, 2 * atoms), (pair_ref, ghosts, ghosts), (other_ref, ghosts, 0)
            ):
                to = slot % 2 * size
                ref[to : to + size, cols] = pulls_ref[at : at + size]
                at += gap


def last_kernel(
    layer, degrees, channels, atoms, per_atom, count,
    rest_ref, lent_ref, hot_ref, radial_ref, dirs_ref, readout_ref, *refs,
):
    tables, weights = refs[:count], refs[count : count + 5]
    out_ref, force_ref = refs[count + 5 : count + 7]
    scratch = refs[count + 7 :]
    joined = scratch[0]
    ghosts = lent_ref.shape[1] // 2
    pieces = []
    for slot in range(count // 3):
        own_rows, pair_rows, other_rows = tables[3 * slot : 3 * slot + 3]
        pieces.append((own_rows, 0, 2 * atoms))
        for upper in range(2):
            span = (upper * ghosts, (upper + 1) * ghosts)
            pieces += [(pair_rows, *span), (other_rows, *span)]
    sums, first, zero = layer_sums(
        layer, degrees, channels, atoms, per_atom, pieces, weights, (hot_ref,), (radial_ref,), scratch
    )
    order = slot_order(degrees)
    for place, slot in enumerate(order):
        cols = slice(place * channels, (place + 1) * channels)
        out_ref[slot] = (joined[:atoms, cols] + 0.18 * sums[place]).astype(BF16)
    for place, slot in enumerate(unused_slots(degrees * degrees)):
        out_ref[slot] = rest_ref[place]

    width = len(sums) * channels
    part = 3 * channels
    own, lent = 0.0, []
    for slot in range(count // 3):
        cols = slice(width + slot // 2 * part, width + (slot // 2 + 1) * part)
        own_rows, *lent_blocks = (
            tables[3 * slot + kind][slot % 2 * size : (slot % 2 + 1) * size, cols].astype(F32)
            for kind, size in enumerate((atoms, ghosts, ghosts))
        )
        own += own_rows
        lent += lent_blocks
    hot = jnp.concatenate([lent_ref[...]] * (count // 3), axis=1).astype(BF16)
    pulls = own + dot(hot, jnp.concatenate(lent, axis=0).astype(BF16))
    readout = readout_ref[...]
    parts = []
    for axis in range(3):
        pull = (first * dirs_ref[axis]).reshape(atoms, per_atom, channels).sum(axis=1)
        back = zero[:atoms, :channels] * pulls[:, axis * channels : (axis + 1) * channels]
        parts.append((pull - back) * readout)
    ones = jnp.ones((8, channels), F32)
    total = dot(ones, jnp.concatenate(parts, axis=0), ((1,), (1,)), HIGHEST)
    for axis in range(3):
        force_ref[axis : axis + 1, :] = total[:1, axis * atoms : (axis + 1) * atoms]


def across(block, bit, slab_devices):
    return lax.ppermute(block, "yz", [(q, q ^ bit) for q in range(slab_devices)])


def toward(block, step, slabs):
    route = []
    for slab in range(slabs):
        to = slab + 1 if (slab % 2 == 0) == (step > 0) else slab - 1
        route.append((slab, to % slabs))
    return lax.ppermute(block, "slab", route)


def spread(held, bits, slab_devices):
    for bit in bits:
        for slot in sorted(held):
            got = []
            for block in held[slot]:
                got.append(across(block, bit, slab_devices))
            held[slot | bit] = tuple(got)
    return held


def order_bits(slab_devices):
    bits, bit = [], slab_devices // 2
    while bit:
        bits.append(bit)
        bit //= 2
    return bits


def body(
    embeddings, neighbours, valid, azimuth, polar, distance, send_low, send_high,
    w_zero, w_one_re, w_one_im, w_two_re, w_two_im, radial_weight, readout,
):
    atoms, coeffs, channels = embeddings.shape
    degrees = math.isqrt(coeffs)
    ghosts = send_low.shape[0]
    edges = neighbours.shape[0]
    layers = w_zero.shape[0]
    slabs, slab_devices = lax.axis_size("slab"), lax.axis_size("yz")
    rows = slab_devices * (atoms + 2 * ghosts)
    width = len(slot_order(degrees)) * channels
    low, high = send_low.reshape(1, -1), send_high.reshape(1, -1)
    held, shape = pltpu.VMEM, jax.ShapeDtypeStruct
    embeddings = embeddings.transpose(1, 0, 2)
    params = pltpu.CompilerParams(vmem_limit_bytes=24 * 2**20)
    row = lambda value: value.reshape(1, -1)
    far = pl.BlockSpec(memory_space=pl.ANY)

    half = slab_devices // 2
    bits = order_bits(slab_devices)
    own, pair, other, rest, radial_weight, vector = pl.pallas_call(
        pack_kernel,
        out_shape=[
            held((atoms, width + edges), BF16), held((ghosts, width), BF16),
            held((ghosts, width), BF16), held((len(unused_slots(coeffs)), atoms, channels), BF16),
            held(radial_weight.shape, F32), held((1, channels), F32),
        ],
        in_specs=[VMEM] * 10,
        out_specs=[VMEM] * 6,
        compiler_params=params,
        name="pack",
    )(*away(
        embeddings, low, high, *map(row, (neighbours, valid, distance, azimuth, polar)),
        radial_weight, row(readout),
    ))

    got_other = toward(other, -1, slabs)
    got_pair = toward(pair, 1, slabs)
    got_own = across(own, half, slab_devices)
    weights = (w_zero, w_one_re, w_one_im, w_two_re, w_two_im)
    count = len(weights)
    near_weights = [held(array.shape[1:], array.dtype) for array in weights]
    side_shapes = [
        held((edges, 2 * rows), BF16), held((layers, edges, channels), F32),
        held((atoms, 2 * ghosts), F32),
    ]
    plans = [[(layer, which) for which in range(count)] for layer in range(layers)]

    hot, radial, lent, dirs, part = pl.pallas_call(
        functools.partial(own_scale_kernel, atoms, ghosts, slab_devices),
        out_shape=[*side_shapes, held((3, edges, channels), F32), held((rows, 3 * channels), F32)],
        in_specs=[VMEM] * 2,
        out_specs=[VMEM] * 5,
        compiler_params=params,
        name="scales",
    )(*near(own, radial_weight))
    got_pair, part = lax.optimization_barrier((got_pair, part))
    joined = pl.pallas_call(
        join_kernel,
        out_shape=held((2 * ghosts, width), BF16),
        in_specs=[VMEM] * 2,
        out_specs=VMEM,
        compiler_params=params,
        name="join",
    )(*near(got_pair, got_other))
    joined_y = across(joined, half, slab_devices)
    hot_y, radial_y, lent_y, pulls, *now = pl.pallas_call(
        functools.partial(partner_scale_kernel, atoms, ghosts, slab_devices, count, plans[0]),
        out_shape=[*side_shapes, held((rows, 3 * channels), BF16), *near_weights],
        in_specs=[VMEM] * 3 + [far] * count,
        out_specs=[VMEM] * (4 + count),
        scratch_shapes=[pltpu.SemaphoreType.DMA((count,))],
        compiler_params=params,
        name="scales_y",
    )(*near(got_own, radial_weight, part), *away(*weights))
    blocks = spread({0: (own, joined), half: (got_own, joined_y)}, bits[1:], slab_devices)
    tables = [
        blocks[slot + upper][kind]
        for slot in range(half) for kind in range(2) for upper in (0, half)
    ]
    scratch = [pltpu.VMEM((rows, width), F32), pltpu.VMEM((2 * rows, width), BF16)]
    per_atom = edges // atoms
    for layer in range(layers):
        if layer < layers - 1:
            last = layer == layers - 2
            wide = width + ((half + 1) // 2 * 3 * channels if last else 0)
            own, pair, other = pl.pallas_call(
                functools.partial(first_kernel, layer, last, degrees, channels, per_atom, len(tables)),
                out_shape=[
                    held((2 * atoms, wide), BF16), held((2 * ghosts, wide), BF16),
                    held((2 * ghosts, wide), BF16),
                ],
                in_specs=[VMEM] * (7 + len(tables) + count),
                out_specs=[VMEM] * 3,
                scratch_shapes=scratch,
                compiler_params=params,
                name="layer",
            )(*near(lent, hot, radial, lent_y, hot_y, radial_y, pulls, *tables, *now))
            got_other = toward(other, -1, slabs)
            got_pair = toward(pair, 1, slabs)
            now = pl.pallas_call(
                functools.partial(fetch_kernel, count, plans[layer + 1]),
                out_shape=near_weights,
                in_specs=[far] * count,
                out_specs=[VMEM] * count,
                scratch_shapes=[pltpu.SemaphoreType.DMA((count,))],
                compiler_params=params,
                name="fetch",
            )(*away(*weights))
            blocks = spread({0: (own, got_pair, got_other)}, bits[1:], slab_devices)
            tables = [block for slot in range(half) for block in blocks[slot]]
        else:
            updated, forces = pl.pallas_call(
                functools.partial(
                    last_kernel, layer, degrees, channels, atoms, per_atom, len(tables)
                ),
                out_shape=[shape((coeffs, atoms, channels), BF16), shape((3, atoms), F32)],
                in_specs=[VMEM] * (6 + len(tables) + count),
                out_specs=[VMEM] * 2,
                scratch_shapes=scratch,
                compiler_params=params,
                name="last_layer",
            )(*near(rest, lent, hot, radial, dirs, vector, *tables, *now))
    return (updated.transpose(1, 0, 2), forces)


def solution(mesh):
    both = ("slab", "yz")
    in_specs = (P(both, None, None), *([P(both)] * 7), *([P()] * 7))
    out_specs = (P(both, None, None), P(None, both))
    return jax.shard_map(body, mesh=mesh, in_specs=in_specs, out_specs=out_specs, check_vma=False)
```

```python
import functools
import math

import jax
import jax.numpy as jnp
from jax import lax
from jax.experimental import pallas as pl
from jax.experimental.pallas import tpu as pltpu
from jax.sharding import PartitionSpec as P


HIGHEST = lax.Precision.HIGHEST
BF16 = jnp.bfloat16
F32 = jnp.float32
ORDERS = (1, 2)
DIGIT = 128
VMEM = pl.BlockSpec(memory_space=pltpu.VMEM)


def near(*arrays):
    return [pltpu.with_memory_space_constraint(array, pltpu.VMEM) for array in arrays]


def away(*arrays):
    return [pltpu.with_memory_space_constraint(array, pltpu.HBM) for array in arrays]


def slot_index(degree, azimuth_order):
    return degree * degree + degree + azimuth_order


def slot_groups(degrees):
    groups = [[slot_index(degree, 0) for degree in range(degrees)]]
    for order in ORDERS:
        groups.append([slot_index(degree, order) for degree in range(order, degrees)])
        groups.append([slot_index(degree, -order) for degree in range(order, degrees)])
    return groups


def slot_order(degrees):
    return [slot for group in slot_groups(degrees) for slot in group]


def unused_slots(coeffs):
    order = slot_order(math.isqrt(coeffs))
    return [slot for slot in range(coeffs) if slot not in order]


def odd_slab():
    return lax.axis_index("slab") % 2 == 1


def dot(left, right, contract=((1,), (0,)), precision=None):
    return lax.dot_general(
        left, right, (contract, ((), ())), precision=precision, preferred_element_type=F32
    )


def lent_picks(low_ref, high_ref):
    odd = odd_slab()
    low, high = low_ref[...], high_ref[...]
    return jnp.concatenate([jnp.where(odd, low, high), jnp.where(odd, high, low)], axis=1)


def lent_hot(picks, atoms):
    rows = lax.broadcasted_iota(jnp.int32, (atoms, picks.shape[1]), 0)
    return (rows == picks).astype(F32)


def lent_rows(hot, rows):
    return dot(hot.astype(BF16), rows, ((0,), (0,))).astype(BF16)


def thirds(value):
    parts = []
    for _ in range(3):
        part = value.astype(BF16).astype(F32)
        parts.append(part)
        value = value - part
    return parts


def pack_kernel(
    emb_ref, low_ref, high_ref, nbr_ref, valid_ref, dist_ref, azi_ref, pol_ref, rw_ref, readout_ref,
    own_ref, pair_ref, other_ref, rest_ref, scales_ref, vector_ref,
):
    coeffs, atoms, channels = emb_ref.shape
    ghosts = low_ref.shape[1]
    edges = nbr_ref.shape[1]
    order = slot_order(math.isqrt(coeffs))
    width = len(order) * channels
    for place, slot in enumerate(order):
        own_ref[:, place * channels : (place + 1) * channels] = emb_ref[slot]
    for place, slot in enumerate(unused_slots(coeffs)):
        rest_ref[place] = emb_ref[slot]
    picks = lent_picks(low_ref, high_ref)
    lent = lent_rows(lent_hot(picks, atoms), own_ref[:, :width])
    pair_ref[...] = lent[:ghosts]
    other_ref[...] = lent[ghosts:]
    nbr = nbr_ref[...]
    picks = jnp.concatenate(
        [picks, jnp.zeros((1, edges - 2 * ghosts), jnp.int32)], axis=1
    ).astype(F32)
    facts = [
        (nbr // DIGIT).astype(F32), (nbr % DIGIT).astype(F32), valid_ref[...].astype(F32), picks,
        *thirds(dist_ref[...]), *thirds(azi_ref[...]), *thirds(pol_ref[...]),
    ]
    facts.append(jnp.zeros((atoms - len(facts), edges), F32))
    own_ref[:, width:] = jnp.concatenate(facts, axis=0).astype(BF16)
    scales_ref[...] = rw_ref[...]
    vector_ref[...] = 0.125 * readout_ref[...]


def edge_facts(ref, edges):
    rows = ref[:, ref.shape[1] - edges :].astype(F32)
    row = lambda at: rows[at : at + 1]
    whole = lambda at: row(at) + row(at + 1) + row(at + 2)
    nbr = (row(0) * DIGIT + row(1)).astype(jnp.int32)
    return nbr, row(2), row(3).astype(jnp.int32), whole(4), whole(7), whole(10)


def start_fetch(far, near_refs, sems, plan):
    copies = [
        pltpu.make_async_copy(far[which].at[layer], near_refs[i], sems.at[i])
        for i, (layer, which) in enumerate(plan)
    ]
    for copy in copies:
        copy.start()
    return copies


def edge_scales(
    atoms, ghosts, slab_devices, facts_ref, rw_ref, hot_ref, radial_ref, lent_ref
):
    layers, centers = rw_ref.shape[0], rw_ref.shape[1]
    own_count, ghost_count = slab_devices * atoms, slab_devices * ghosts
    half = slab_devices // 2
    me = lax.axis_index("yz")
    odd = odd_slab()
    edges = hot_ref.shape[0]
    count = hot_ref.shape[1] // 2
    nbr, valid, picks, distance, _, _ = edge_facts(facts_ref, edges)
    is_own = nbr < own_count
    ghost = nbr - own_count
    below = ghost < ghost_count
    ghost = jnp.where(below, ghost, ghost - ghost_count)
    paired = jnp.where(odd, below.astype(jnp.int32), 1 - below.astype(jnp.int32))
    slot = jnp.where(is_own, nbr // atoms, ghost // ghosts) ^ me
    upper = slot // half
    inner = jnp.where(
        is_own,
        upper * atoms + nbr % atoms,
        2 * atoms + upper * (2 * ghosts) + (1 - paired) * ghosts + ghost % ghosts,
    )
    place = (slot % half) * (2 * atoms + 4 * ghosts) + inner
    rows = lax.broadcasted_iota(jnp.int32, (count, edges), 0)
    hot = jnp.where((rows == place) & (valid != 0.0), 1.0, 0.0).astype(F32)
    hot_cols = jnp.transpose(hot).astype(BF16)
    hot_ref[...] = jnp.concatenate([hot_cols, hot_cols], axis=1)
    middle = 1.0 + 0.5 * lax.broadcasted_iota(jnp.int32, (centers, edges), 0).astype(F32)
    basis = jnp.exp(-jnp.square((distance - middle) / 0.5))
    for layer in range(layers):
        scale = dot(basis, rw_ref[layer], ((0,), (0,)), HIGHEST)
        radial = scale / (1.0 + jnp.exp(-scale))
        radial_ref[layer] = radial
    lent_ref[...] = lent_hot(picks[:, : 2 * ghosts], atoms)
    return hot, radial


def pull_sums(facts_ref, hot, radial):
    _, _, _, _, azimuth, polar = edge_facts(facts_ref, hot.shape[1])
    sin_polar = jnp.sin(polar)
    dirs = [sin_polar * jnp.cos(azimuth), sin_polar * jnp.sin(azimuth), jnp.cos(polar)]
    count, channels = hot.shape[0], radial.shape[1]
    high = radial.astype(BF16)
    both = jnp.concatenate([high, (radial - high.astype(F32)).astype(BF16)], axis=1)
    pulls = []
    for axis in range(3):
        along = hot * dirs[axis]
        high = along.astype(BF16)
        low = (along - high.astype(F32)).astype(BF16)
        got = dot(jnp.concatenate([high, low], axis=0), both)
        pulls.append(got[:count, :channels] + got[:count, channels:] + got[count:, :channels])
    return dirs, jnp.concatenate(pulls, axis=1)


def own_scale_kernel(
    atoms, ghosts, slab_devices,
    facts_ref, rw_ref, hot_ref, radial_ref, lent_ref, dirs_ref, part_ref,
):
    hot, radial = edge_scales(
        atoms, ghosts, slab_devices, facts_ref, rw_ref, hot_ref, radial_ref, lent_ref
    )
    dirs, part_ref[...] = pull_sums(facts_ref, hot, radial)
    columns = jnp.transpose(jnp.concatenate([*dirs, *dirs, *dirs[:2]], axis=0))
    for axis in range(3):
        dirs_ref[axis] = jnp.broadcast_to(columns[:, axis : axis + 1], dirs_ref.shape[1:])


def partner_scale_kernel(
    atoms, ghosts, slab_devices, count, plan, facts_ref, rw_ref, part_ref, *refs
):
    far, (hot_ref, radial_ref, lent_ref, pulls_ref), refs = (
        refs[:count], refs[count : count + 4], refs[count + 4 :]
    )
    copies = start_fetch(far, refs[:-1], refs[-1], plan)
    hot, radial = edge_scales(
        atoms, ghosts, slab_devices, facts_ref, rw_ref, hot_ref, radial_ref, lent_ref
    )
    _, pulls = pull_sums(facts_ref, hot, radial)
    pulls_ref[...] = (part_ref[...] + pulls).astype(BF16)
    for copy in copies:
        copy.wait()


def fetch_kernel(count, plan, *refs):
    for copy in start_fetch(refs[:count], refs[count:-1], refs[-1], plan):
        copy.wait()


def join_kernel(pair_ref, other_ref, both_ref):
    ghosts = pair_ref.shape[0]
    both_ref[:ghosts] = pair_ref[...]
    both_ref[ghosts:] = other_ref[...]


def mix_rows(pieces, degrees, channels, weights, mixed_ref, joined):
    groups = slot_groups(degrees)
    w_zero, w_one_re, w_one_im, w_two_re, w_two_im = (ref[...] for ref in weights)
    rows, width = mixed_ref.shape[0] // 2, mixed_ref.shape[1]
    runs, count = [], 0
    for ref, begin, end, to in pieces:
        size = end - begin
        joined[count : count + size] = ref[begin:end, :width].astype(F32)
        if runs and runs[-1][2] + runs[-1][1] == to:
            runs[-1][1] += size
        else:
            runs.append([count, size, to])
        count += size

    def put(column, value):
        high = value.astype(BF16)
        low = (value - high.astype(F32)).astype(BF16)
        cols = slice(column, column + value.shape[1])
        for start, size, to in runs:
            mixed_ref[to : to + size, cols] = high[start : start + size]
            mixed_ref[rows + to : rows + to + size, cols] = low[start : start + size]

    span = len(groups[0]) * channels
    put(0, dot(joined[:, :span].astype(BF16), w_zero))
    column = span
    for index, (real, imag) in enumerate(((w_one_re, w_one_im), (w_two_re, w_two_im))):
        span = len(groups[2 * index + 1]) * channels
        both = jnp.concatenate(
            [joined[:, column : column + span], joined[:, column + span : column + 2 * span]], axis=0
        ).astype(BF16)
        by_real = dot(both, real)
        by_imag = dot(both, imag)
        put(column, by_real[:count] - by_imag[count:])
        put(column + span, by_imag[:count] + by_real[count:])
        column += 2 * span


def early_kernel(degrees, channels, pieces, count, *refs):
    tables, weights, (mixed_ref, joined) = refs[:count], refs[count : count + 5], refs[count + 5 :]
    mix_rows(
        [(tables[at], *rest) for at, *rest in pieces], degrees, channels, weights, mixed_ref, joined
    )


def layer_sums(layer, channels, atoms, per_atom, mixed_ref, hots, radials):
    width = mixed_ref.shape[1]
    part = atoms // len(hots)
    sums = []
    first = None
    step = 4 * channels
    for begin in range(0, width, step):
        end = min(begin + step, width)
        pieces = []
        for hot_ref, radial_ref in zip(hots, radials):
            got = dot(hot_ref[...], mixed_ref[:, begin:end])
            for inner in range(0, end - begin, channels):
                message = got[:, inner : inner + channels] * radial_ref[layer]
                if first is None:
                    first = message
                pieces.append(message.reshape(part, per_atom, channels).sum(axis=1))
        count = (end - begin) // channels
        for inner in range(count):
            sums.append(jnp.concatenate(pieces[inner::count], axis=0))
    return sums, first


def first_kernel(
    layer, last, degrees, channels, per_atom, late, count,
    lent_ref, hot_ref, radial_ref, lent_y_ref, hot_y_ref, radial_y_ref, pulls_ref, _, *refs,
):
    tables, weights = refs[:count], refs[count : count + 5]
    mixed_ref, own_ref, pair_ref, other_ref, joined = refs[count + 5 :]
    both = own_ref.shape[0]
    atoms, ghosts = both // 2, lent_ref.shape[1] // 2
    mix_rows(
        [(tables[at], *rest) for at, *rest in late], degrees, channels, weights, mixed_ref, joined
    )
    sums, _ = layer_sums(
        layer, channels, both, per_atom, mixed_ref, (hot_ref, hot_y_ref), (radial_ref, radial_y_ref)
    )
    old = [ref for ref in tables if ref.shape[0] in (atoms, both)][: 2 if layer == 0 else 1]
    width = len(sums) * channels
    for place, total in enumerate(sums):
        cols = slice(place * channels, (place + 1) * channels)
        before = jnp.concatenate([ref[:, cols].astype(F32) for ref in old], axis=0)
        own_ref[:, cols] = (before + 0.18 * total).astype(BF16)
    for side, hot in enumerate((lent_ref, lent_y_ref)):
        lent = lent_rows(hot[...], own_ref[side * atoms : (side + 1) * atoms, :width])
        pair_ref[side * ghosts : (side + 1) * ghosts, :width] = lent[:ghosts]
        other_ref[side * ghosts : (side + 1) * ghosts, :width] = lent[ghosts:]
    if last:
        part = pulls_ref.shape[1]
        block = 2 * atoms + 4 * ghosts
        for slot in range(pulls_ref.shape[0] // block):
            cols = slice(width + slot // 2 * part, width + (slot // 2 + 1) * part)
            at = slot * block
            for ref, size, gap in (
                (own_ref, atoms, 2 * atoms), (pair_ref, ghosts, ghosts), (other_ref, ghosts, 0)
            ):
                to = slot % 2 * size
                ref[to : to + size, cols] = pulls_ref[at : at + size]
                at += gap


def last_kernel(
    layer, degrees, channels, atoms, per_atom, late, count,
    rest_ref, lent_ref, hot_ref, radial_ref, dirs_ref, readout_ref, _, *refs,
):
    tables, weights = refs[:count], refs[count : count + 5]
    mixed_ref, out_ref, force_ref, joined = refs[count + 5 :]
    ghosts = lent_ref.shape[1] // 2
    mix_rows(
        [(tables[at], *rest) for at, *rest in late], degrees, channels, weights, mixed_ref, joined
    )
    sums, first = layer_sums(
        layer, channels, atoms, per_atom, mixed_ref, (hot_ref,), (radial_ref,)
    )
    rows = mixed_ref.shape[0] // 2
    zero = mixed_ref[:atoms, :channels].astype(F32)
    zero += mixed_ref[rows : rows + atoms, :channels].astype(F32)
    order = slot_order(degrees)
    for place, slot in enumerate(order):
        cols = slice(place * channels, (place + 1) * channels)
        out_ref[slot] = (tables[0][:atoms, cols].astype(F32) + 0.18 * sums[place]).astype(BF16)
    for place, slot in enumerate(unused_slots(degrees * degrees)):
        out_ref[slot] = rest_ref[place]

    width = len(sums) * channels
    part = 3 * channels
    own, lent = 0.0, []
    for slot in range(count // 3):
        cols = slice(width + slot // 2 * part, width + (slot // 2 + 1) * part)
        own_rows, *lent_blocks = (
            tables[3 * slot + kind][slot % 2 * size : (slot % 2 + 1) * size, cols].astype(F32)
            for kind, size in enumerate((atoms, ghosts, ghosts))
        )
        own += own_rows
        lent += lent_blocks
    hot = jnp.concatenate([lent_ref[...]] * (count // 3), axis=1).astype(BF16)
    pulls = own + dot(hot, jnp.concatenate(lent, axis=0).astype(BF16))
    readout = readout_ref[...]
    parts = []
    for axis in range(3):
        pull = (first * dirs_ref[axis]).reshape(atoms, per_atom, channels).sum(axis=1)
        back = zero * pulls[:, axis * channels : (axis + 1) * channels]
        parts.append((pull - back) * readout)
    ones = jnp.ones((8, channels), F32)
    total = dot(ones, jnp.concatenate(parts, axis=0), ((1,), (1,)), HIGHEST)
    for axis in range(3):
        force_ref[axis : axis + 1, :] = total[:1, axis * atoms : (axis + 1) * atoms]


def across(block, bit, slab_devices):
    return lax.ppermute(block, "yz", [(q, q ^ bit) for q in range(slab_devices)])


def toward(block, step, slabs):
    route = []
    for slab in range(slabs):
        to = slab + 1 if (slab % 2 == 0) == (step > 0) else slab - 1
        route.append((slab, to % slabs))
    return lax.ppermute(block, "slab", route)


def spread(held, bits, slab_devices):
    for bit in bits:
        for slot in sorted(held):
            got = []
            for block in held[slot]:
                got.append(across(block, bit, slab_devices))
            held[slot | bit] = tuple(got)
    return held


def order_bits(slab_devices):
    bits, bit = [], slab_devices // 2
    while bit:
        bits.append(bit)
        bit //= 2
    return bits


def body(
    embeddings, neighbours, valid, azimuth, polar, distance, send_low, send_high,
    w_zero, w_one_re, w_one_im, w_two_re, w_two_im, radial_weight, readout,
):
    atoms, coeffs, channels = embeddings.shape
    degrees = math.isqrt(coeffs)
    ghosts = send_low.shape[0]
    edges = neighbours.shape[0]
    layers = w_zero.shape[0]
    slabs, slab_devices = lax.axis_size("slab"), lax.axis_size("yz")
    rows = slab_devices * (atoms + 2 * ghosts)
    width = len(slot_order(degrees)) * channels
    low, high = send_low.reshape(1, -1), send_high.reshape(1, -1)
    held, shape = pltpu.VMEM, jax.ShapeDtypeStruct
    embeddings = embeddings.transpose(1, 0, 2)
    params = pltpu.CompilerParams(vmem_limit_bytes=24 * 2**20)
    row = lambda value: value.reshape(1, -1)
    far = pl.BlockSpec(memory_space=pl.ANY)

    half = slab_devices // 2
    bits = order_bits(slab_devices)
    own, pair, other, rest, radial_weight, vector = pl.pallas_call(
        pack_kernel,
        out_shape=[
            held((atoms, width + edges), BF16), held((ghosts, width), BF16),
            held((ghosts, width), BF16), held((len(unused_slots(coeffs)), atoms, channels), BF16),
            held(radial_weight.shape, F32), held((1, channels), F32),
        ],
        in_specs=[VMEM] * 10,
        out_specs=[VMEM] * 6,
        compiler_params=params,
        name="pack",
    )(*away(
        embeddings, low, high, *map(row, (neighbours, valid, distance, azimuth, polar)),
        radial_weight, row(readout),
    ))

    got_other = toward(other, -1, slabs)
    got_pair = toward(pair, 1, slabs)
    got_own = across(own, half, slab_devices)
    weights = (w_zero, w_one_re, w_one_im, w_two_re, w_two_im)
    count = len(weights)
    near_weights = [held(array.shape[1:], array.dtype) for array in weights]
    side_shapes = [
        held((edges, 2 * rows), BF16), held((layers, edges, channels), F32),
        held((atoms, 2 * ghosts), F32),
    ]
    plans = [[(layer, which) for which in range(count)] for layer in range(layers)]

    hot, radial, lent, dirs, part = pl.pallas_call(
        functools.partial(own_scale_kernel, atoms, ghosts, slab_devices),
        out_shape=[*side_shapes, held((3, edges, channels), F32), held((rows, 3 * channels), F32)],
        in_specs=[VMEM] * 2,
        out_specs=[VMEM] * 5,
        compiler_params=params,
        name="scales",
    )(*near(own, radial_weight))
    got_pair, part = lax.optimization_barrier((got_pair, part))
    joined = pl.pallas_call(
        join_kernel,
        out_shape=held((2 * ghosts, width), BF16),
        in_specs=[VMEM] * 2,
        out_specs=VMEM,
        compiler_params=params,
        name="join",
    )(*near(got_pair, got_other))
    joined_y = across(joined, half, slab_devices)
    hot_y, radial_y, lent_y, pulls, *now = pl.pallas_call(
        functools.partial(partner_scale_kernel, atoms, ghosts, slab_devices, count, plans[0]),
        out_shape=[*side_shapes, held((rows, 3 * channels), BF16), *near_weights],
        in_specs=[VMEM] * 3 + [far] * count,
        out_specs=[VMEM] * (4 + count),
        scratch_shapes=[pltpu.SemaphoreType.DMA((count,))],
        compiler_params=params,
        name="scales_y",
    )(*near(got_own, radial_weight, part), *away(*weights))
    blocks = spread({0: (own, joined), half: (got_own, joined_y)}, bits[1:], slab_devices)
    tables = [
        blocks[slot + upper][kind]
        for slot in range(half) for kind in range(2) for upper in (0, half)
    ]

    def sizes(pieces):
        return sum(end - begin for _, begin, end, _ in pieces)

    def mix_early(pieces):
        used = sorted({piece[0] for piece in pieces})
        pieces = [(used.index(piece[0]), *piece[1:]) for piece in pieces]
        return pl.pallas_call(
            functools.partial(early_kernel, degrees, channels, pieces, len(used)),
            out_shape=held((2 * rows, width), BF16),
            in_specs=[VMEM] * (len(used) + count),
            out_specs=VMEM,
            scratch_shapes=[pltpu.VMEM((sizes(pieces), width), F32)],
            compiler_params=params,
            name="early",
        )(*near(*(tables[at] for at in used), *now))

    pieces, at = [], 0
    for index, block in enumerate(tables):
        pieces.append((index, 0, block.shape[0], at))
        at += block.shape[0]
    early, late = pieces[:-1], pieces[-1:]
    per_atom = edges // atoms
    for layer in range(layers):
        mixed = mix_early(early)
        if layer < layers - 1:
            last = layer == layers - 2
            wide = width + ((half + 1) // 2 * 3 * channels if last else 0)
            _, own, pair, other = pl.pallas_call(
                functools.partial(
                    first_kernel, layer, last, degrees, channels, per_atom, late, len(tables)
                ),
                out_shape=[
                    held((2 * rows, width), BF16), held((2 * atoms, wide), BF16), held((2 * ghosts, wide), BF16),
                    held((2 * ghosts, wide), BF16),
                ],
                in_specs=[VMEM] * (8 + len(tables) + count),
                out_specs=[VMEM] * 4,
                input_output_aliases={7: 0},
                scratch_shapes=[pltpu.VMEM((sizes(late), width), F32)],
                compiler_params=params,
                name="layer",
            )(*near(lent, hot, radial, lent_y, hot_y, radial_y, pulls, mixed, *tables, *now))
            got_other = toward(other, -1, slabs)
            got_pair = toward(pair, 1, slabs)
            now = pl.pallas_call(
                functools.partial(fetch_kernel, count, plans[layer + 1]),
                out_shape=near_weights,
                in_specs=[far] * count,
                out_specs=[VMEM] * count,
                scratch_shapes=[pltpu.SemaphoreType.DMA((count,))],
                compiler_params=params,
                name="fetch",
            )(*away(*weights))
            blocks = spread({0: (own, got_pair, got_other)}, bits[1:], slab_devices)
            tables = [block for slot in range(half) for block in blocks[slot]]
            early, late = [], []
            for slot in range(half):
                at = slot * (2 * atoms + 4 * ghosts)
                early.append((3 * slot, 0, 2 * atoms, at))
                at += 2 * atoms
                for upper in range(2):
                    for kind in (1, 2):
                        waits = slot == half - 1
                        span = (upper * ghosts, (upper + 1) * ghosts)
                        (late if waits else early).append((3 * slot + kind, *span, at))
                        at += ghosts
        else:
            _, updated, forces = pl.pallas_call(
                functools.partial(
                    last_kernel, layer, degrees, channels, atoms, per_atom, late, len(tables)
                ),
                out_shape=[
                    held((2 * rows, width), BF16), shape((coeffs, atoms, channels), BF16),
                    shape((3, atoms), F32),
                ],
                in_specs=[VMEM] * (7 + len(tables) + count),
                out_specs=[VMEM] * 3,
                input_output_aliases={6: 0},
                scratch_shapes=[pltpu.VMEM((sizes(late), width), F32)],
                compiler_params=params,
                name="last_layer",
            )(*near(rest, lent, hot, radial, dirs, vector, mixed, *tables, *now))
    return (updated.transpose(1, 0, 2), forces)


def solution(mesh):
    both = ("slab", "yz")
    in_specs = (P(both, None, None), *([P(both)] * 7), *([P()] * 7))
    out_specs = (P(both, None, None), P(None, both))
    return jax.shard_map(body, mesh=mesh, in_specs=in_specs, out_specs=out_specs, check_vma=False)
```
